8 devices in a mesh: pairs: 2 (over z, y), rows: 4 (over x, core).
Axes of the slice: x: 2, y: 2, z: 1, core: 2. Of those that a mesh axis runs over, the one named last changes fastest.
Arguments:
- cost_src: float32 [4096, 2048], P(('pairs', 'rows')), parts along dimension 0
- cost_tgt: float32 [2048, 1024], P(('pairs', 'rows')), parts along dimension 0
- plan_init: float32 [4096, 1024], P(('pairs', 'rows')), parts along dimension 0
- mass_src: float32 [4096], P(('pairs', 'rows')), parts along dimension 0
- mass_tgt: float32 [2048], P('pairs'), parts along dimension 0
- feat_src: float32 [4096, 256], P(('pairs', 'rows')), parts along dimension 0
- feat_tgt: float32 [2048, 256], P(('pairs', 'rows')), parts along dimension 0
- epsilon: float32 [], replicated
Outputs:
- output: float32 [4096, 1024], P(('pairs', 'rows')), parts along dimension 0
There are 2 independent parts. The reference program is written for one: setup_inputs(seed, part) draws one part's arguments, and reference() takes and returns one part's arrays. A program takes and returns all parts, laid end to end along the dimension named above; an argument that names none is the same for every part.
All inputs are finite; a program needn't handle non-finite values.
Results may differ from the reference program's by a relative error of at most 0.001.
Values are sent between devices in bfloat16 or wider.
A program may use at most 1 GiB of HBM per device.

```python
import jax
import jax.numpy as jnp
from jax import lax

N = 2048
M = 1024
D = 256
OUTER_STEPS = 2
SWEEPS = 10
ALPHA = 0.5


def point_costs(key_pts, num_points):
    key_centers, key_labels, key_noise = jax.random.split(key_pts, 3)
    centers = 1.5 * jax.random.normal(key_centers, (8, 3), jnp.float32)
    labels = jax.random.randint(key_labels, (num_points,), 0, 8)
    points = centers[labels] + 0.4 * jax.random.normal(key_noise, (num_points, 3), jnp.float32)
    sq_dist = jnp.zeros((num_points, num_points), jnp.float32)
    for dim_index in range(3):
        column_vals = points[:, dim_index]
        coord_diff = column_vals[:, None] - column_vals[None, :]
        sq_dist = sq_dist + coord_diff * coord_diff
    return sq_dist / jnp.max(sq_dist), labels


def marginal(key_mass, num_points):
    weights = jnp.exp(0.5 * jax.random.normal(key_mass, (num_points,), jnp.float32))
    return weights / jnp.sum(weights)


def setup_inputs(seed: int = 0, part: int = 0) -> dict:
    base_key, shared_key = jax.random.split(jax.random.key(seed))
    sub_keys = jax.random.split(jax.random.fold_in(base_key, part), 7)
    cost_src, labels_src = point_costs(sub_keys[0], N)
    cost_tgt, labels_tgt = point_costs(sub_keys[1], M)
    mass_src = marginal(sub_keys[2], N)
    mass_tgt = marginal(sub_keys[3], M)
    block_logits = 3.0 * jax.random.normal(sub_keys[4], (8, 8), jnp.float32)
    plan_init = mass_src[:, None] * mass_tgt[None, :] * jnp.exp(block_logits[labels_src][:, labels_tgt])
    plan_init = plan_init / jnp.sum(plan_init)
    feat_scale = 0.125 * D ** -0.25
    feat_src = feat_scale * jax.random.normal(sub_keys[5], (N, D), jnp.float32)
    feat_tgt = feat_scale * jax.random.normal(sub_keys[6], (M, D), jnp.float32)
    epsilon = jax.random.uniform(shared_key, (), jnp.float32, 0.04, 0.08)
    return {"cost_src": cost_src, "cost_tgt": cost_tgt, "plan_init": plan_init, "mass_src": mass_src, "mass_tgt": mass_tgt, "feat_src": feat_src, "feat_tgt": feat_tgt, "epsilon": epsilon}


def reference(cost_src, cost_tgt, plan_init, mass_src, mass_tgt, feat_src, feat_tgt, epsilon):
    src_half = cost_src.astype(jnp.bfloat16)
    tgt_half = cost_tgt.astype(jnp.bfloat16)
    cross_term = jnp.dot(feat_src.astype(jnp.bfloat16), feat_tgt.astype(jnp.bfloat16).T, preferred_element_type=jnp.float32)
    feat_cost = (-2.0 * ALPHA) * cross_term

    def outer_step(step_index, transport):
        prod_a = jnp.dot(src_half, transport.astype(jnp.bfloat16), preferred_element_type=jnp.float32)
        prod_b = jnp.dot(prod_a.astype(jnp.bfloat16), tgt_half, preferred_element_type=jnp.float32)
        step_cost = feat_cost - (2.0 * (1.0 - ALPHA)) * prod_b
        kernel = jnp.exp(-(step_cost - jnp.min(step_cost, axis=1, keepdims=True)) / epsilon)

        def sinkhorn_sweep(sweep_index, scales):
            row_scale = mass_src / jnp.sum(kernel * scales[1][None, :], axis=1)
            return row_scale, mass_tgt / jnp.sum(kernel * row_scale[:, None], axis=0)

        start_scales = (jnp.ones_like(mass_src), jnp.ones_like(mass_tgt))
        row_scale, col_scale = lax.fori_loop(0, SWEEPS, sinkhorn_sweep, start_scales)
        return row_scale[:, None] * kernel * col_scale[None, :]

    return lax.fori_loop(0, OUTER_STEPS, outer_step, plan_init)
```

```python
import jax
import jax.numpy as jnp
from jax import lax
from jax.experimental import pallas as pl
from jax.experimental.pallas import tpu as pltpu
from jax.sharding import PartitionSpec as P

ALPHA = 0.5
OUTER_STEPS = 2
SWEEPS = 10
LOG2E = 1.4426950408889634

N = 2048
M = 1024
D = 256
NB = 512
MB = 256
F32 = jnp.float32
BF16 = jnp.bfloat16
LANES = 128

T_CHUNKS = 4
C1_CHUNKS = 2
TR = NB // T_CHUNKS
CR = NB // C1_CHUNKS
K_CHUNKS = 4
KR = 2 * NB // K_CHUNKS

S_T = 0
S_C2 = S_T + T_CHUNKS
S_Y = S_C2 + 1
S_P = S_Y + 1
S_X = S_P + 1
S_C1 = S_X + 1
ICI_SLOTS = S_C1 + C1_CHUNKS
F_T = S_P + 1
F_C2 = F_T + T_CHUNKS
F_Y = F_C2 + 1
F_P = F_Y + 1
S_C1P = F_P + 1
S_K1 = S_C1P + 1
S_K2 = S_K1 + K_CHUNKS
D2D_SLOTS = S_K2 + K_CHUNKS


def hint(value, multiple):
    return pl.multiple_of(value, multiple)


def sinkhorn(kern, plan_b, u_b, v_ref, q_ref):
    rb = 128
    blocks = N // rb
    cols = M // LANES

    def load(i, j):
        k = kern[pl.ds(hint(i * rb, rb), rb), j * LANES:(j + 1) * LANES]
        return k.reshape(rb // 8, 8, LANES)

    v_ref[...] = jnp.ones_like(v_ref)

    def sweep(_, carry):
        v = [v_ref[:, j * LANES:(j + 1) * LANES] for j in range(cols)]

        def row_sums(i):
            part = load(i, 0) * v[0][None]
            for j in range(1, cols):
                part = part + load(i, j) * v[j][None]
            return jnp.sum(part, axis=-1, keepdims=True)

        def accumulate(i, sums, acc):
            rows = pl.ds(hint(i * rb, rb), rb)
            u = plan_b[rows, :].reshape(rb // 8, 8, LANES) / sums
            u_b[rows, :] = u.reshape(rb, LANES)
            return tuple(acc[j] + jnp.sum(load(i, j) * u, axis=0) for j in range(cols))

        def body(i, state):
            sums, acc = state
            following = row_sums(i + 1)
            return following, accumulate(i, sums, acc)

        zero = tuple(jnp.zeros((8, LANES), F32) for _ in range(cols))
        sums, acc = lax.fori_loop(0, blocks - 1, body, (row_sums(0), zero))
        acc = accumulate(blocks - 1, sums, acc)
        for j in range(cols):
            col_sum = jnp.sum(acc[j], axis=0, keepdims=True)
            v_new = q_ref[:, j * LANES:(j + 1) * LANES] / col_sum
            v_ref[:, j * LANES:(j + 1) * LANES] = jnp.broadcast_to(v_new, (8, LANES))
        return carry

    lax.fori_loop(0, SWEEPS, sweep, 0)


def scaled_rows(kern, u_b, v_ref, row, count):
    parts = []
    u = u_b[pl.ds(row, count), :].reshape(count // 8, 8, LANES)
    for j in range(M // LANES):
        k = kern[pl.ds(row, count), j * LANES:(j + 1) * LANES].reshape(count // 8, 8, LANES)
        t = u * k * v_ref[:, j * LANES:(j + 1) * LANES][None]
        parts.append(t.reshape(count, LANES))
    return parts


def kernel(c1_hbm, c2_hbm, t0_hbm, p_hbm, q_ref, x_hbm, y_hbm, eps_ref, out_ref,
           c1_st, c2_st, t_st, x_st, y_st,
           t_all, c1_rows, c1_side, c2_all, y_all, x_rows, g_rows, a_buf,
           kern1, kern2, p_all, p_b, u_b, v_ref,
           load_sem, ici_send, ici_recv, d2d_send, d2d_recv):
    me = lax.axis_index("rows")
    chip = me // 2
    core = me % 2
    partner = chip * 2 + (1 - core)
    far = (1 - chip) * 2 + core
    far_partner = (1 - chip) * 2 + (1 - core)

    loads = [pltpu.make_async_copy(src, dst, load_sem.at[i]) for i, (src, dst) in enumerate((
        (t0_hbm, t_st), (c2_hbm, c2_st), (y_hbm, y_st), (p_hbm, p_all.at[me]), (x_hbm, x_st), (c1_hbm, c1_st)))]
    for copy in loads:
        copy.start()

    barrier = pltpu.get_barrier_semaphore()
    for peer in (partner, far):
        pl.semaphore_signal(barrier, inc=1, device_id={"rows": peer}, device_id_type=pl.DeviceIdType.MESH)
    pl.semaphore_wait(barrier, 2)

    def to_far(src, dst, slot):
        return pltpu.make_async_remote_copy(
            src_ref=src, dst_ref=dst, send_sem=ici_send.at[slot], recv_sem=ici_recv.at[slot],
            device_id={"rows": far}, device_id_type=pl.DeviceIdType.MESH)

    def to_partner(src, dst, slot):
        return pltpu.make_async_remote_copy(
            src_ref=src, dst_ref=dst, send_sem=d2d_send.at[slot], recv_sem=d2d_recv.at[slot],
            device_id={"rows": partner}, device_id_type=pl.DeviceIdType.MESH)

    def t_rows(owner, k):
        return t_all.at[pl.ds(hint(owner * NB + k * TR, TR), TR), :]

    def c2_diag(owner, owner_chip):
        return c2_all.at[pl.ds(hint(owner * MB, MB), MB), pl.ds(hint(owner_chip * 2 * MB, 2 * MB), 2 * MB)]

    def c2_full(owner):
        return c2_all.at[pl.ds(hint(owner * MB, MB), MB), :]

    def y_rows(owner):
        return y_all.at[pl.ds(hint(owner * MB, MB), MB), :]

    sends = []

    def go(copy):
        copy.start()
        sends.append(copy)

    loads[0].wait()
    for k in range(T_CHUNKS):
        t_all[pl.ds(hint(me * NB + k * TR, TR), TR), :] = t_st[k * TR:(k + 1) * TR, :].astype(BF16)
    for k in range(T_CHUNKS):
        go(to_far(t_rows(me, k), t_rows(me, k), S_T + k))
        go(to_partner(t_rows(me, k), t_rows(me, k), S_T + k))
    for copy in loads[1:5]:
        copy.wait()
    c2_all[pl.ds(hint(me * MB, MB), MB), :] = c2_st[...].astype(BF16)
    y_all[pl.ds(hint(me * MB, MB), MB), :] = y_st[...].astype(BF16)
    x_rows[:NB, :] = x_st[...].astype(BF16)
    loads[5].wait()
    c1_rows[:NB, :] = c1_st[...].astype(BF16)
    go(to_far(c2_diag(me, chip), c2_diag(me, chip), S_C2))
    go(to_far(y_rows(me), y_rows(me), S_Y))
    go(to_far(p_all.at[me], p_all.at[me], S_P))
    go(to_far(x_rows.at[:NB], x_rows.at[NB:], S_X))
    for k in range(C1_CHUNKS):
        cols = pl.ds(hint(chip * 2 * NB, 2 * NB), 2 * NB)
        go(to_far(c1_rows.at[k * CR:(k + 1) * CR, cols], c1_rows.at[NB + k * CR:NB + (k + 1) * CR, cols], S_C1 + k))
    go(to_partner(c2_full(me), c2_full(me), S_C2))
    go(to_partner(y_rows(me), y_rows(me), S_Y))
    go(to_partner(p_all.at[me], p_all.at[me], S_P))
    go(to_partner(c1_rows.at[:NB, pl.ds(hint(far_partner * NB, NB), NB)], c1_side, S_C1P))

    def mirror(src, src_row, src_col, dst, dst_row, dst_col, size):
        for i in range(size // LANES):
            for j in range(size // LANES):
                tile = src[pl.ds(hint(src_row + i * LANES, LANES), LANES), pl.ds(hint(src_col + j * LANES, LANES), LANES)]
                dst[pl.ds(hint(dst_row + j * LANES, LANES), LANES), pl.ds(hint(dst_col + i * LANES, LANES), LANES)] = (
                    tile.astype(F32).T.astype(BF16))

    mirror(c1_rows, 0, far * NB, c1_rows, NB, me * NB, NB)
    to_partner(c1_side, c1_side, S_C1P).wait_recv()
    mirror(c1_side, 0, 0, c1_rows, NB, partner * NB, NB)
    to_partner(c2_full(me), c2_full(partner), S_C2).wait_recv()
    mirror(c2_all, chip * 2 * MB, (1 - chip) * 2 * MB, c2_all, (1 - chip) * 2 * MB, chip * 2 * MB, 2 * MB)
    for k in range(T_CHUNKS):
        to_partner(t_rows(me, k), t_rows(partner, k), S_T + k).wait_recv()
    to_partner(y_rows(me), y_rows(partner), S_Y).wait_recv()
    to_partner(p_all.at[me], p_all.at[partner], S_P).wait_recv()

    for k in range(T_CHUNKS):
        to_far(t_rows(me, k), t_rows(far, k), S_T + k).wait_recv()
        go(to_partner(t_rows(far, k), t_rows(far, k), F_T + k))
    to_far(c2_diag(me, chip), c2_diag(far, 1 - chip), S_C2).wait_recv()
    go(to_partner(c2_diag(far, 1 - chip), c2_diag(far, 1 - chip), F_C2))
    to_far(y_rows(me), y_rows(far), S_Y).wait_recv()
    go(to_partner(y_rows(far), y_rows(far), F_Y))
    to_far(p_all.at[me], p_all.at[far], S_P).wait_recv()
    go(to_partner(p_all.at[far], p_all.at[far], F_P))
    to_far(x_rows.at[:NB], x_rows.at[NB:], S_X).wait_recv()
    for k in range(T_CHUNKS):
        to_partner(t_rows(far, k), t_rows(far_partner, k), F_T + k).wait_recv()
    to_partner(c2_diag(far, 1 - chip), c2_diag(far_partner, 1 - chip), F_C2).wait_recv()
    to_partner(y_rows(far), y_rows(far_partner), F_Y).wait_recv()
    to_partner(p_all.at[far], p_all.at[far_partner], F_P).wait_recv()

    for owner in range(4):
        for i in range(NB // LANES):
            block = jnp.broadcast_to(p_all[owner, i:i + 1, :], (LANES, LANES))
            p_b[owner * NB + i * LANES:owner * NB + (i + 1) * LANES, :] = block.T

    for h in range(2):
        for n in range(4):
            g = lax.dot_general(x_rows[h * NB:(h + 1) * NB, :], y_all[n * 256:(n + 1) * 256, :],
                                (((1,), (1,)), ((), ())), preferred_element_type=F32)
            g_rows[h * NB:(h + 1) * NB, n * 256:(n + 1) * 256] = (2.0 * ALPHA) * g

    scale = LOG2E / eps_ref[0, 0]

    def global_row(k):
        local = k * KR
        return jnp.where(local < NB, me * NB + local, far * NB + local - NB)

    def kernel_rows(kern, k):
        rows = pl.ds(hint(k * KR, KR), KR)
        for n in range(4):
            a_buf[:, n * 256:(n + 1) * 256] = jnp.dot(
                c1_rows[rows, :], t_all[:, n * 256:(n + 1) * 256], preferred_element_type=F32).astype(BF16)
        top = hint(global_row(k), KR)
        gain = []
        for n in range(4):
            b = jnp.dot(a_buf[...], c2_all[:, n * 256:(n + 1) * 256], preferred_element_type=F32)
            s = g_rows[rows, n * 256:(n + 1) * 256] + (2.0 * (1.0 - ALPHA)) * b
            kern[pl.ds(top, KR), n * 256:(n + 1) * 256] = s
            gain.append(jnp.max(s, axis=1, keepdims=True))
        peak = jnp.maximum(jnp.maximum(gain[0], gain[1]), jnp.maximum(gain[2], gain[3]))
        for n in range(4):
            s = kern[pl.ds(top, KR), n * 256:(n + 1) * 256]
            kern[pl.ds(top, KR), n * 256:(n + 1) * 256] = jnp.exp2((s - peak) * scale)

    def kern_slice(kern, base):
        return kern.at[pl.ds(hint(base, KR), KR), :]

    def share_rows(kern, k, slot):
        rows = kern_slice(kern, global_row(k))
        return to_partner(rows, rows, slot + k)

    def receive_rows(kern, k, slot):
        local = k * KR
        base = jnp.where(local < NB, partner * NB + local, far_partner * NB + local - NB)
        to_partner(kern_slice(kern, base), kern_slice(kern, base), slot + k).wait_recv()

    for step, (kern, slot) in enumerate(((kern1, S_K1), (kern2, S_K2))):
        def chunk(k, carry):
            kernel_rows(kern, k)
            share_rows(kern, k, slot).start()
            return carry
        if step == 0:
            lax.fori_loop(0, K_CHUNKS // 2, chunk, 0)
            for k in range(C1_CHUNKS):
                cols = pl.ds(hint((1 - chip) * 2 * NB, 2 * NB), 2 * NB)
                part = c1_rows.at[NB + k * CR:NB + (k + 1) * CR, cols]
                to_far(part, part, S_C1 + k).wait_recv()
            lax.fori_loop(K_CHUNKS // 2, K_CHUNKS, chunk, 0)
        else:
            lax.fori_loop(0, K_CHUNKS, chunk, 0)
        for k in range(K_CHUNKS):
            receive_rows(kern, k, slot)
        sinkhorn(kern, p_b, u_b, v_ref, q_ref)
        if step == 0:
            def next_plan(i, carry):
                row = hint(i * 64, 64)
                for j, t in enumerate(scaled_rows(kern, u_b, v_ref, row, 64)):
                    t_all[pl.ds(row, 64), j * LANES:(j + 1) * LANES] = t.astype(BF16)
                return carry
            for copy in sends:
                copy.wait_send()
            lax.fori_loop(0, N // 64, next_plan, 0)

    def result(i, carry):
        row = hint(i * 64, 64)
        for j, t in enumerate(scaled_rows(kern2, u_b, v_ref, hint(me * NB + row, 64), 64)):
            out_ref[pl.ds(row, 64), j * LANES:(j + 1) * LANES] = t
        return carry
    lax.fori_loop(0, NB // 64, result, 0)
    for kern, slot in ((kern1, S_K1), (kern2, S_K2)):
        for k in range(K_CHUNKS):
            share_rows(kern, k, slot).wait_send()


def solution(mesh):
    vmem = pl.BlockSpec(memory_space=pltpu.VMEM)
    hbm = pl.BlockSpec(memory_space=pl.ANY)
    smem = pl.BlockSpec(memory_space=pltpu.SMEM)

    def local_fgw(cost_src, cost_tgt, plan_init, mass_src, mass_tgt, feat_src, feat_tgt, epsilon):
        return pl.pallas_call(
            kernel,
            out_shape=jax.ShapeDtypeStruct((NB, M), F32),
            in_specs=[hbm, hbm, hbm, hbm, vmem, hbm, hbm, smem],
            out_specs=vmem,
            scratch_shapes=[
                pltpu.VMEM((NB, N), F32),
                pltpu.VMEM((MB, M), F32),
                pltpu.VMEM((NB, M), F32),
                pltpu.VMEM((NB, D), F32),
                pltpu.VMEM((MB, D), F32),
                pltpu.VMEM((N, M), BF16),
                pltpu.VMEM((2 * NB, N), BF16),
                pltpu.VMEM((NB, NB), BF16),
                pltpu.VMEM((M, M), BF16),
                pltpu.VMEM((M, D), BF16),
                pltpu.VMEM((2 * NB, D), BF16),
                pltpu.VMEM((2 * NB, M), F32),
                pltpu.VMEM((KR, M), BF16),
                pltpu.VMEM((N, M), F32),
                pltpu.VMEM((N, M), F32),
                pltpu.VMEM((4, NB // LANES, LANES), F32),
                pltpu.VMEM((N, LANES), F32),
                pltpu.VMEM((N, LANES), F32),
                pltpu.VMEM((8, M), F32),
                pltpu.SemaphoreType.DMA((6,)),
                pltpu.SemaphoreType.DMA((ICI_SLOTS,)),
                pltpu.SemaphoreType.DMA((ICI_SLOTS,)),
                pltpu.SemaphoreType.DMA((D2D_SLOTS,)),
                pltpu.SemaphoreType.DMA((D2D_SLOTS,)),
            ],
            compiler_params=pltpu.CompilerParams(
                collective_id=0, has_side_effects=True, vmem_limit_bytes=60000 * 1024),
        )(cost_src, cost_tgt, plan_init, mass_src.reshape(NB // LANES, LANES), mass_tgt.reshape(1, M),
          feat_src, feat_tgt, epsilon.reshape(1, 1))

    row_spec = P(('pairs', 'rows'), None)
    vec_spec = P(('pairs', 'rows'))
    in_specs = (row_spec, row_spec, row_spec, vec_spec, P('pairs'), row_spec, row_spec, P())
    return jax.shard_map(local_fgw, mesh=mesh, in_specs=in_specs, out_specs=row_spec, check_vma=False)
```

```python
import jax
import jax.numpy as jnp
from jax import lax
from jax.experimental import pallas as pl
from jax.experimental.pallas import tpu as pltpu
from jax.sharding import PartitionSpec as P

ALPHA = 0.5
OUTER_STEPS = 2
SWEEPS = 10
LOG2E = 1.4426950408889634

N = 2048
M = 1024
D = 256
NB = 512
MB = 256
F32 = jnp.float32
BF16 = jnp.bfloat16
LANES = 128

T_CHUNKS = 4
C1_CHUNKS = 2
TR = NB // T_CHUNKS
CR = NB // C1_CHUNKS
K_CHUNKS = 4
KR = 2 * NB // K_CHUNKS

S_T = 0
S_C2 = S_T + T_CHUNKS
S_Y = S_C2 + 1
S_P = S_Y + 1
S_X = S_P + 1
S_C1 = S_X + 1
ICI_SLOTS = S_C1 + C1_CHUNKS
F_T = S_P + 1
F_C2 = F_T + T_CHUNKS
F_Y = F_C2 + 1
F_P = F_Y + 1
S_C1P = F_P + 1
S_K1 = S_C1P + 1
S_K2 = S_K1 + K_CHUNKS
D2D_SLOTS = S_K2 + K_CHUNKS


def hint(value, multiple):
    return pl.multiple_of(value, multiple)


def sinkhorn(kern, plan_b, u_b, v_ref, q_ref):
    lead = 128
    cols = M // LANES

    def col(j):
        return slice(j * LANES, (j + 1) * LANES)

    v_ref[...] = jnp.ones_like(v_ref)

    def sweep(_, carry):
        v = [v_ref[:, col(j)] for j in range(cols)]

        def row_scale(row):
            rows = slice(row, row + 8)
            part = [kern[rows, col(j)] * v[j] for j in range(cols)]
            while len(part) > 1:
                part = [part[i] + part[i + 1] for i in range(0, len(part), 2)]
            u_b[rows, :] = plan_b[rows, :] / jnp.sum(part[0], axis=1, keepdims=True)

        acc = [jnp.zeros((8, LANES), F32) for _ in range(cols)]
        for row in range(-lead, N, 8):
            if row + lead < N:
                row_scale(row + lead)
            if row >= 0:
                u = u_b[row:row + 8, :]
                acc = [acc[j] + kern[row:row + 8, col(j)] * u for j in range(cols)]
        for j in range(cols):
            col_sum = jnp.sum(acc[j], axis=0, keepdims=True)
            v_ref[:, col(j)] = jnp.broadcast_to(q_ref[:, col(j)] / col_sum, (8, LANES))
        return carry

    lax.fori_loop(0, SWEEPS, sweep, 0)


def scaled_rows(kern, u_b, v_ref, row, count):
    parts = []
    u = u_b[pl.ds(row, count), :].reshape(count // 8, 8, LANES)
    for j in range(M // LANES):
        k = kern[pl.ds(row, count), j * LANES:(j + 1) * LANES].reshape(count // 8, 8, LANES)
        t = u * k * v_ref[:, j * LANES:(j + 1) * LANES][None]
        parts.append(t.reshape(count, LANES))
    return parts


def kernel(c1_hbm, c2_hbm, t0_hbm, p_hbm, q_ref, x_hbm, y_hbm, eps_ref, out_ref,
           c1_st, c2_st, t_st, x_st, y_st,
           t_all, c1_rows, c1_side, c2_all, y_all, x_rows, g_rows, a_buf,
           kern1, kern2, p_all, p_b, u_b, v_ref,
           load_sem, ici_send, ici_recv, d2d_send, d2d_recv):
    current = [None]

    def mark(name):
        if current[0] is not None:
            current[0].__exit__(None, None, None)
            current[0] = None
        if name:
            current[0] = jax.named_scope(name)
            current[0].__enter__()
    me = lax.axis_index("rows")
    chip = me // 2
    core = me % 2
    partner = chip * 2 + (1 - core)
    far = (1 - chip) * 2 + core
    far_partner = (1 - chip) * 2 + (1 - core)

    loads = [pltpu.make_async_copy(src, dst, load_sem.at[i]) for i, (src, dst) in enumerate((
        (t0_hbm, t_st), (c2_hbm, c2_st), (y_hbm, y_st), (p_hbm, p_all.at[me]), (x_hbm, x_st), (c1_hbm, c1_st)))]
    for copy in loads:
        copy.start()

    mark('barrier')
    barrier = pltpu.get_barrier_semaphore()
    for peer in (partner, far):
        pl.semaphore_signal(barrier, inc=1, device_id={"rows": peer}, device_id_type=pl.DeviceIdType.MESH)
    pl.semaphore_wait(barrier, 2)

    def to_far(src, dst, slot):
        return pltpu.make_async_remote_copy(
            src_ref=src, dst_ref=dst, send_sem=ici_send.at[slot], recv_sem=ici_recv.at[slot],
            device_id={"rows": far}, device_id_type=pl.DeviceIdType.MESH)

    def to_partner(src, dst, slot):
        return pltpu.make_async_remote_copy(
            src_ref=src, dst_ref=dst, send_sem=d2d_send.at[slot], recv_sem=d2d_recv.at[slot],
            device_id={"rows": partner}, device_id_type=pl.DeviceIdType.MESH)

    def t_rows(owner, k):
        return t_all.at[pl.ds(hint(owner * NB + k * TR, TR), TR), :]

    def c2_diag(owner, owner_chip):
        return c2_all.at[pl.ds(hint(owner * MB, MB), MB), pl.ds(hint(owner_chip * 2 * MB, 2 * MB), 2 * MB)]

    def c2_full(owner):
        return c2_all.at[pl.ds(hint(owner * MB, MB), MB), :]

    def y_rows(owner):
        return y_all.at[pl.ds(hint(owner * MB, MB), MB), :]

    sends = []

    def go(copy):
        copy.start()
        sends.append(copy)

    mark('cast_t')
    loads[0].wait()
    for k in range(T_CHUNKS):
        t_all[pl.ds(hint(me * NB + k * TR, TR), TR), :] = t_st[k * TR:(k + 1) * TR, :].astype(BF16)
    for k in range(T_CHUNKS):
        go(to_far(t_rows(me, k), t_rows(me, k), S_T + k))
        go(to_partner(t_rows(me, k), t_rows(me, k), S_T + k))
    mark('cast_rest')
    for copy in loads[1:5]:
        copy.wait()
    c2_all[pl.ds(hint(me * MB, MB), MB), :] = c2_st[...].astype(BF16)
    y_all[pl.ds(hint(me * MB, MB), MB), :] = y_st[...].astype(BF16)
    x_rows[:NB, :] = x_st[...].astype(BF16)
    loads[5].wait()
    c1_rows[:NB, :] = c1_st[...].astype(BF16)
    go(to_far(c2_diag(me, chip), c2_diag(me, chip), S_C2))
    go(to_far(y_rows(me), y_rows(me), S_Y))
    go(to_far(p_all.at[me], p_all.at[me], S_P))
    go(to_far(x_rows.at[:NB], x_rows.at[NB:], S_X))
    for k in range(C1_CHUNKS):
        cols = pl.ds(hint(chip * 2 * NB, 2 * NB), 2 * NB)
        go(to_far(c1_rows.at[k * CR:(k + 1) * CR, cols], c1_rows.at[NB + k * CR:NB + (k + 1) * CR, cols], S_C1 + k))
    go(to_partner(c2_full(me), c2_full(me), S_C2))
    go(to_partner(y_rows(me), y_rows(me), S_Y))
    go(to_partner(p_all.at[me], p_all.at[me], S_P))
    go(to_partner(c1_rows.at[:NB, pl.ds(hint(far_partner * NB, NB), NB)], c1_side, S_C1P))

    def mirror(src, src_row, src_col, dst, dst_row, dst_col, size):
        for i in range(size // LANES):
            for j in range(size // LANES):
                tile = src[pl.ds(hint(src_row + i * LANES, LANES), LANES), pl.ds(hint(src_col + j * LANES, LANES), LANES)]
                dst[pl.ds(hint(dst_row + j * LANES, LANES), LANES), pl.ds(hint(dst_col + i * LANES, LANES), LANES)] = (
                    tile.astype(F32).T.astype(BF16))

    mark('mirrors')
    mirror(c1_rows, 0, far * NB, c1_rows, NB, me * NB, NB)
    to_partner(c1_side, c1_side, S_C1P).wait_recv()
    mirror(c1_side, 0, 0, c1_rows, NB, partner * NB, NB)
    to_partner(c2_full(me), c2_full(partner), S_C2).wait_recv()
    mirror(c2_all, chip * 2 * MB, (1 - chip) * 2 * MB, c2_all, (1 - chip) * 2 * MB, chip * 2 * MB, 2 * MB)
    mark('wait_partner')
    for k in range(T_CHUNKS):
        to_partner(t_rows(me, k), t_rows(partner, k), S_T + k).wait_recv()
    to_partner(y_rows(me), y_rows(partner), S_Y).wait_recv()
    to_partner(p_all.at[me], p_all.at[partner], S_P).wait_recv()

    mark('wait_t')
    for k in range(T_CHUNKS):
        to_far(t_rows(me, k), t_rows(far, k), S_T + k).wait_recv()
        go(to_partner(t_rows(far, k), t_rows(far, k), F_T + k))
    mark('wait_c2yx')
    to_far(c2_diag(me, chip), c2_diag(far, 1 - chip), S_C2).wait_recv()
    go(to_partner(c2_diag(far, 1 - chip), c2_diag(far, 1 - chip), F_C2))
    to_far(y_rows(me), y_rows(far), S_Y).wait_recv()
    go(to_partner(y_rows(far), y_rows(far), F_Y))
    to_far(p_all.at[me], p_all.at[far], S_P).wait_recv()
    go(to_partner(p_all.at[far], p_all.at[far], F_P))
    to_far(x_rows.at[:NB], x_rows.at[NB:], S_X).wait_recv()
    for k in range(T_CHUNKS):
        to_partner(t_rows(far, k), t_rows(far_partner, k), F_T + k).wait_recv()
    to_partner(c2_diag(far, 1 - chip), c2_diag(far_partner, 1 - chip), F_C2).wait_recv()
    to_partner(y_rows(far), y_rows(far_partner), F_Y).wait_recv()
    to_partner(p_all.at[far], p_all.at[far_partner], F_P).wait_recv()

    mark('p_b')
    for owner in range(4):
        for i in range(NB // LANES):
            block = jnp.broadcast_to(p_all[owner, i:i + 1, :], (LANES, LANES))
            p_b[owner * NB + i * LANES:owner * NB + (i + 1) * LANES, :] = block.T

    mark('gram')
    for h in range(2):
        for n in range(4):
            g = lax.dot_general(x_rows[h * NB:(h + 1) * NB, :], y_all[n * 256:(n + 1) * 256, :],
                                (((1,), (1,)), ((), ())), preferred_element_type=F32)
            g_rows[h * NB:(h + 1) * NB, n * 256:(n + 1) * 256] = (2.0 * ALPHA) * g

    mark('steps')
    scale = LOG2E / eps_ref[0, 0]

    def global_row(k):
        local = k * KR
        return jnp.where(local < NB, me * NB + local, far * NB + local - NB)

    def kernel_rows(kern, k):
        rows = pl.ds(hint(k * KR, KR), KR)
        for n in range(4):
            a_buf[:, n * 256:(n + 1) * 256] = jnp.dot(
                c1_rows[rows, :], t_all[:, n * 256:(n + 1) * 256], preferred_element_type=F32).astype(BF16)
        top = hint(global_row(k), KR)
        gain = []
        for n in range(4):
            b = jnp.dot(a_buf[...], c2_all[:, n * 256:(n + 1) * 256], preferred_element_type=F32)
            s = g_rows[rows, n * 256:(n + 1) * 256] + (2.0 * (1.0 - ALPHA)) * b
            kern[pl.ds(top, KR), n * 256:(n + 1) * 256] = s
            gain.append(jnp.max(s, axis=1, keepdims=True))
        peak = jnp.maximum(jnp.maximum(gain[0], gain[1]), jnp.maximum(gain[2], gain[3]))
        for n in range(4):
            s = kern[pl.ds(top, KR), n * 256:(n + 1) * 256]
            kern[pl.ds(top, KR), n * 256:(n + 1) * 256] = jnp.exp2((s - peak) * scale)

    def kern_slice(kern, base):
        return kern.at[pl.ds(hint(base, KR), KR), :]

    def share_rows(kern, k, slot):
        rows = kern_slice(kern, global_row(k))
        return to_partner(rows, rows, slot + k)

    def receive_rows(kern, k, slot):
        local = k * KR
        base = jnp.where(local < NB, partner * NB + local, far_partner * NB + local - NB)
        to_partner(kern_slice(kern, base), kern_slice(kern, base), slot + k).wait_recv()

    for step, (kern, slot) in enumerate(((kern1, S_K1), (kern2, S_K2))):
        def chunk(k, carry):
            kernel_rows(kern, k)
            share_rows(kern, k, slot).start()
            return carry
        if step == 0:
            mark('own_rows')
            lax.fori_loop(0, K_CHUNKS // 2, chunk, 0)
            mark('wait_c1')
            for k in range(C1_CHUNKS):
                cols = pl.ds(hint((1 - chip) * 2 * NB, 2 * NB), 2 * NB)
                part = c1_rows.at[NB + k * CR:NB + (k + 1) * CR, cols]
                to_far(part, part, S_C1 + k).wait_recv()
            mark('far_rows')
            lax.fori_loop(K_CHUNKS // 2, K_CHUNKS, chunk, 0)
        else:
            mark('rows_2')
            lax.fori_loop(0, K_CHUNKS, chunk, 0)
        mark('receive')
        for k in range(K_CHUNKS):
            receive_rows(kern, k, slot)
        mark('sinkhorn')
        sinkhorn(kern, p_b, u_b, v_ref, q_ref)
        mark('next_plan')
        if step == 0:
            def next_plan(i, carry):
                row = hint(i * 64, 64)
                for j, t in enumerate(scaled_rows(kern, u_b, v_ref, row, 64)):
                    t_all[pl.ds(row, 64), j * LANES:(j + 1) * LANES] = t.astype(BF16)
                return carry
            for copy in sends:
                copy.wait_send()
            lax.fori_loop(0, N // 64, next_plan, 0)

    mark('result')

    def result(i, carry):
        row = hint(i * 64, 64)
        for j, t in enumerate(scaled_rows(kern2, u_b, v_ref, hint(me * NB + row, 64), 64)):
            out_ref[pl.ds(row, 64), j * LANES:(j + 1) * LANES] = t
        return carry
    lax.fori_loop(0, NB // 64, result, 0)
    for kern, slot in ((kern1, S_K1), (kern2, S_K2)):
        for k in range(K_CHUNKS):
            share_rows(kern, k, slot).wait_send()
    mark(None)


def solution(mesh):
    vmem = pl.BlockSpec(memory_space=pltpu.VMEM)
    hbm = pl.BlockSpec(memory_space=pl.ANY)
    smem = pl.BlockSpec(memory_space=pltpu.SMEM)

    def local_fgw(cost_src, cost_tgt, plan_init, mass_src, mass_tgt, feat_src, feat_tgt, epsilon):
        return pl.pallas_call(
            kernel,
            out_shape=jax.ShapeDtypeStruct((NB, M), F32),
            in_specs=[hbm, hbm, hbm, hbm, vmem, hbm, hbm, smem],
            out_specs=vmem,
            scratch_shapes=[
                pltpu.VMEM((NB, N), F32),
                pltpu.VMEM((MB, M), F32),
                pltpu.VMEM((NB, M), F32),
                pltpu.VMEM((NB, D), F32),
                pltpu.VMEM((MB, D), F32),
                pltpu.VMEM((N, M), BF16),
                pltpu.VMEM((2 * NB, N), BF16),
                pltpu.VMEM((NB, NB), BF16),
                pltpu.VMEM((M, M), BF16),
                pltpu.VMEM((M, D), BF16),
                pltpu.VMEM((2 * NB, D), BF16),
                pltpu.VMEM((2 * NB, M), F32),
                pltpu.VMEM((KR, M), BF16),
                pltpu.VMEM((N, M), F32),
                pltpu.VMEM((N, M), F32),
                pltpu.VMEM((4, NB // LANES, LANES), F32),
                pltpu.VMEM((N, LANES), F32),
                pltpu.VMEM((N, LANES), F32),
                pltpu.VMEM((8, M), F32),
                pltpu.SemaphoreType.DMA((6,)),
                pltpu.SemaphoreType.DMA((ICI_SLOTS,)),
                pltpu.SemaphoreType.DMA((ICI_SLOTS,)),
                pltpu.SemaphoreType.DMA((D2D_SLOTS,)),
                pltpu.SemaphoreType.DMA((D2D_SLOTS,)),
            ],
            compiler_params=pltpu.CompilerParams(
                collective_id=0, has_side_effects=True, vmem_limit_bytes=60000 * 1024),
        )(cost_src, cost_tgt, plan_init, mass_src.reshape(NB // LANES, LANES), mass_tgt.reshape(1, M),
          feat_src, feat_tgt, epsilon.reshape(1, 1))

    row_spec = P(('pairs', 'rows'), None)
    vec_spec = P(('pairs', 'rows'))
    in_specs = (row_spec, row_spec, row_spec, vec_spec, P('pairs'), row_spec, row_spec, P())
    return jax.shard_map(local_fgw, mesh=mesh, in_specs=in_specs, out_specs=row_spec, check_vma=False)
```

```python
import jax
import jax.numpy as jnp
from jax import lax
from jax.experimental import pallas as pl
from jax.experimental.pallas import tpu as pltpu
from jax.sharding import PartitionSpec as P

ALPHA = 0.5
OUTER_STEPS = 2
SWEEPS = 10
LOG2E = 1.4426950408889634

N = 2048
M = 1024
D = 256
NB = 512
MB = 256
F32 = jnp.float32
BF16 = jnp.bfloat16
LANES = 128
COLS = M // LANES

T_CHUNKS = 4
TR = NB // T_CHUNKS
CH = 256
HALF = NB // 2
SWEEP_GROUP = 32
FORM_GROUP = 32


class Slots:
    def __init__(self):
        self.names = {}

    def __call__(self, name):
        return self.names.setdefault(name, len(self.names))


LINK = Slots()
SIDE = Slots()
for k in range(T_CHUNKS):
    LINK(("t", k)), SIDE(("t", k)), SIDE(("far t", k))
for k in range(4):
    LINK(("c2", k)), SIDE(("far c2", k)), LINK(("c1 strip", k))
for name in ("a1", "a2"):
    for k in range(4):
        SIDE((name, k))
for k in range(2):
    LINK(("c1 quad", k)), SIDE(("c1 quad", k))
for name in ("y", "x", "p"):
    LINK(name), SIDE(name), SIDE("far " + name)
SIDE("c2"), SIDE("c1")


def hint(value, multiple):
    return value if isinstance(value, int) else pl.multiple_of(value, multiple)


def span(start, size):
    return pl.ds(hint(start, size), size)


def col(j):
    return slice(j * LANES, (j + 1) * LANES)


def tree(op, parts):
    while len(parts) > 1:
        parts = [op(parts[i], parts[i + 1]) for i in range(0, len(parts), 2)]
    return parts[0]


def store_col_scale(acc, v_ref, q_ref):
    for j in range(COLS):
        col_sum = jnp.sum(acc[j], axis=0, keepdims=True)
        v_ref[:, col(j)] = jnp.broadcast_to(q_ref[:, col(j)] / col_sum, (8, LANES))


def sweeps(count, kern, plan_b, u_b, v_ref, q_ref):
    lead = 128
    group = SWEEP_GROUP
    shape = (group // 8, 8, LANES)

    def sweep(_, carry):
        v = [v_ref[:, col(j)][None] for j in range(COLS)]

        def tile(row, j):
            return kern[row:row + group, col(j)].reshape(shape)

        acc = [jnp.zeros((8, LANES), F32) for _ in range(COLS)]
        for row in range(-lead, N, group):
            top = row + lead
            if top < N:
                total = tree(jnp.add, [tile(top, j) * v[j] for j in range(COLS)])
                u = plan_b[top:top + group, :].reshape(shape) / jnp.sum(total, axis=2, keepdims=True)
                u_b[top:top + group, :] = u.reshape(group, LANES)
            if row >= 0:
                u = u_b[row:row + group, :].reshape(shape)
                acc = [acc[j] + jnp.sum(tile(row, j) * u, axis=0) for j in range(COLS)]
        store_col_scale(acc, v_ref, q_ref)
        return carry

    lax.fori_loop(0, count, sweep, 0)


def scaled_rows(kern, u_b, v_ref, row, count):
    u = u_b[pl.ds(row, count), :].reshape(count // 8, 8, LANES)
    for j in range(COLS):
        k = kern[pl.ds(row, count), col(j)].reshape(count // 8, 8, LANES)
        yield j, (u * k * v_ref[:, col(j)][None]).reshape(count, LANES)


def kernel(c1_hbm, c2_hbm, t0_hbm, p_hbm, q_ref, x_hbm, y_hbm, eps_ref, out_ref,
           c1_st, c2_st, t_st, x_st, y_st,
           t_all, c1_rows, c1_side, quad_side, c2_all, y_all, x_all, g_all, a1_all, a2_all,
           kern, p_all, p_b, u_b, peak_b, first_b, acc_ref, v_ref,
           load_sem, link_send, link_recv, side_send, side_recv):
    raw0, raw1 = 0, CH
    current = [None]

    def mark(name):
        if current[0] is not None:
            current[0].__exit__(None, None, None)
            current[0] = None
        if name:
            current[0] = jax.named_scope(name)
            current[0].__enter__()

    me = lax.axis_index("rows")
    chip = me // 2
    core = me % 2
    partner = chip * 2 + (1 - core)
    far = (1 - chip) * 2 + core
    far_partner = (1 - chip) * 2 + (1 - core)

    loads = [pltpu.make_async_copy(src, dst, load_sem.at[i]) for i, (src, dst) in enumerate((
        (t0_hbm, t_st), (c2_hbm, c2_st), (y_hbm, y_st), (p_hbm, p_all.at[me]), (x_hbm, x_st), (c1_hbm, c1_st)))]
    for copy in loads:
        copy.start()

    mark("barrier")
    barrier = pltpu.get_barrier_semaphore()
    for peer in (partner, far):
        pl.semaphore_signal(barrier, inc=1, device_id={"rows": peer}, device_id_type=pl.DeviceIdType.MESH)
    pl.semaphore_wait(barrier, 2)

    def to_far(src, dst, name):
        slot = LINK.names[name]
        return pltpu.make_async_remote_copy(
            src_ref=src, dst_ref=dst, send_sem=link_send.at[slot], recv_sem=link_recv.at[slot],
            device_id={"rows": far}, device_id_type=pl.DeviceIdType.MESH)

    def to_partner(src, dst, name):
        slot = SIDE.names[name]
        return pltpu.make_async_remote_copy(
            src_ref=src, dst_ref=dst, send_sem=side_send.at[slot], recv_sem=side_recv.at[slot],
            device_id={"rows": partner}, device_id_type=pl.DeviceIdType.MESH)

    sends = []

    def go(copy):
        copy.start()
        sends.append(copy)

    def far_arrived(ref, name):
        to_far(ref, ref, name).wait_recv()

    def partner_arrived(ref, name):
        to_partner(ref, ref, name).wait_recv()

    def t_rows(owner, k):
        return t_all.at[span(owner * NB + k * TR, TR), :]

    def c2_rows(owner):
        return c2_all.at[span(owner * MB, MB), :]

    def c2_pieces(owner, other, which):
        return (
            c2_all.at[span(owner * MB + 128, 128), span(other * MB, 128)],
            c2_all.at[span(owner * MB + which * 128, 128), span(other * MB + which * 128, 128)],
            c2_all.at[span(owner * MB, 128), span(owner * MB, MB)],
            c2_all.at[span(owner * MB + 128, 128), span(owner * MB + 128, 128)])

    def y_rows(owner):
        return y_all.at[span(owner * MB, MB), :]

    def x_rows(owner):
        return x_all.at[span(owner * NB, NB), :]

    def c1_quads(base, other, which):
        return (c1_rows.at[base + HALF:base + NB, span(other * NB, HALF)],
                c1_rows.at[span(base + which * HALF, HALF), span(other * NB + which * HALF, HALF)])

    def c1_strip(base, owner, k):
        return c1_rows.at[base + k * 128:base + (k + 1) * 128, pl.ds(hint(owner * NB + k * 128, 128), NB - k * 128)]

    mark("cast_t")
    loads[0].wait()
    for k in range(T_CHUNKS):
        t_all[span(me * NB + k * TR, TR), :] = t_st[k * TR:(k + 1) * TR, :].astype(BF16)
    for k in range(T_CHUNKS):
        go(to_far(t_rows(me, k), t_rows(me, k), ("t", k)))
        go(to_partner(t_rows(me, k), t_rows(me, k), ("t", k)))
    mark("cast_rest")
    for copy in loads[1:]:
        copy.wait()
    c2_all[span(me * MB, MB), :] = c2_st[...].astype(BF16)
    y_all[span(me * MB, MB), :] = y_st[...].astype(BF16)
    x_all[span(me * NB, NB), :] = x_st[...].astype(BF16)
    c1_rows[:NB, :] = c1_st[...].astype(BF16)
    for k, piece in enumerate(c2_pieces(me, partner, core)):
        go(to_far(piece, piece, ("c2", k)))
    go(to_far(y_rows(me), y_rows(me), "y"))
    go(to_far(p_all.at[me], p_all.at[me], "p"))
    go(to_far(x_rows(me), x_rows(me), "x"))
    for k, (src, dst) in enumerate(zip(c1_quads(0, partner, core), c1_quads(NB, partner, core))):
        go(to_far(src, dst, ("c1 quad", k)))
    for k in range(4):
        go(to_far(c1_strip(0, me, k), c1_strip(NB, me, k), ("c1 strip", k)))
    go(to_partner(c2_rows(me), c2_rows(me), "c2"))
    go(to_partner(y_rows(me), y_rows(me), "y"))
    go(to_partner(p_all.at[me], p_all.at[me], "p"))
    go(to_partner(x_rows(me), x_rows(me), "x"))
    go(to_partner(c1_rows.at[:NB, span(far_partner * NB, NB)], c1_side, "c1"))

    def mirror(src, src_row, src_col, dst, dst_row, dst_col, size):
        for i in range(size // LANES):
            for j in range(size // LANES):
                tile = src[span(src_row + i * LANES, LANES), span(src_col + j * LANES, LANES)]
                dst[span(dst_row + j * LANES, LANES), span(dst_col + i * LANES, LANES)] = (
                    tile.astype(F32).T.astype(BF16))

    mark("mirrors")
    mirror(c1_rows, 0, far * NB, c1_rows, NB, me * NB, NB)
    partner_arrived(c1_side, "c1")
    mirror(c1_side, 0, 0, c1_rows, NB, partner * NB, NB)
    partner_arrived(c2_rows(partner), "c2")
    mirror(c2_all, chip * 2 * MB, (1 - chip) * 2 * MB, c2_all, (1 - chip) * 2 * MB, chip * 2 * MB, 2 * MB)
    for k in range(T_CHUNKS):
        partner_arrived(t_rows(partner, k), ("t", k))
    partner_arrived(y_rows(partner), "y")
    partner_arrived(p_all.at[partner], "p")
    partner_arrived(x_rows(partner), "x")

    mark("wait_t")
    for k in range(T_CHUNKS):
        far_arrived(t_rows(far, k), ("t", k))
        go(to_partner(t_rows(far, k), t_rows(far, k), ("far t", k)))
    mark("wait_c2yx")
    for k, piece in enumerate(c2_pieces(far, far_partner, core)):
        far_arrived(piece, ("c2", k))
        go(to_partner(piece, piece, ("far c2", k)))
    for name, ref in (("y", y_rows(far)), ("p", p_all.at[far]), ("x", x_rows(far))):
        far_arrived(ref, name)
        go(to_partner(ref, ref, "far " + name))
    for k in range(T_CHUNKS):
        partner_arrived(t_rows(far_partner, k), ("far t", k))
    for k, piece in enumerate(c2_pieces(far_partner, far, 1 - core)):
        partner_arrived(piece, ("far c2", k))
    for name, ref in (("y", y_rows(far_partner)), ("p", p_all.at[far_partner]), ("x", x_rows(far_partner))):
        partner_arrived(ref, "far " + name)

    mark("c2_mirror")
    first = (1 - chip) * 2 * MB
    second = first + MB
    for base in (first, second):
        mirror(c2_all, base, base + 128, c2_all, base + 128, base, 128)
    mirror(c2_all, second + 128, first, c2_all, first, second + 128, 128)
    mirror(c2_all, second + 128, first + 128, c2_all, first + 128, second + 128, 128)
    mirror(c2_all, first, second, c2_all, second, first, 128)
    mirror(c2_all, first + 128, second, c2_all, second, first + 128, 128)

    mark("p_b")
    for owner in range(4):
        for i in range(NB // LANES):
            block = jnp.broadcast_to(p_all[owner, i:i + 1, :], (LANES, LANES))
            p_b[owner * NB + i * LANES:owner * NB + (i + 1) * LANES, :] = block.T

    mark("gram")

    def gram(h, carry):
        for n in range(4):
            g = lax.dot_general(x_all[span(h * NB, NB), :], y_all[n * 256:(n + 1) * 256, :],
                                (((1,), (1,)), ((), ())), preferred_element_type=F32)
            g_all[span(h * NB, NB), n * 256:(n + 1) * 256] = (2.0 * ALPHA) * g
        return carry
    lax.fori_loop(0, 4, gram, 0)

    scale = LOG2E / eps_ref[0, 0]

    def a_rows(a_all, local, base):
        for n in range(4):
            a_all[span(base, CH), n * 256:(n + 1) * 256] = jnp.dot(
                c1_rows[span(local, CH), :], t_all[:, n * 256:(n + 1) * 256], preferred_element_type=F32).astype(BF16)

    def scores(a_all, base, raw):
        for n in range(4):
            b = jnp.dot(a_all[span(base, CH), :], c2_all[:, n * 256:(n + 1) * 256], preferred_element_type=F32)
            t_st[raw:raw + CH, n * 256:(n + 1) * 256] = g_all[span(base, CH), n * 256:(n + 1) * 256] + (2.0 * (1.0 - ALPHA)) * b

    def form(base, raw):
        acc = [acc_ref[:, col(j)] for j in range(COLS)]
        lead = 64
        group = FORM_GROUP
        shape = (group // 8, 8, LANES)
        for row in range(-2 * lead, CH, group):
            top = row + 2 * lead
            if top < CH:
                peak = tree(jnp.maximum, [t_st[raw + top:raw + top + group, col(j)] for j in range(COLS)])
                peak_b[top:top + group, :] = jnp.broadcast_to(jnp.max(peak, axis=1, keepdims=True), (group, LANES))
            mid = row + lead
            if 0 <= mid < CH:
                here = pl.ds(hint(base + mid, group), group)
                peak = peak_b[mid:mid + group, :]
                vals = [jnp.exp2((t_st[raw + mid:raw + mid + group, col(j)] - peak) * scale) for j in range(COLS)]
                for j in range(COLS):
                    kern[here, col(j)] = vals[j]
                total = jnp.sum(tree(jnp.add, vals), axis=1, keepdims=True)
                first_b[mid:mid + group, :] = p_b[here, :] / total
            if row >= 0:
                here = pl.ds(hint(base + row, group), group)
                u = first_b[row:row + group, :].reshape(shape)
                acc = [acc[j] + jnp.sum(kern[here, col(j)].reshape(shape) * u, axis=0) for j in range(COLS)]
        for j in range(COLS):
            acc_ref[:, col(j)] = acc[j]

    def b_rows(a_all, bases):
        raws = (raw0, raw1)
        for i, base in enumerate(bases):
            scores(a_all, base, raws[i % 2])
            if i:
                form(bases[i - 1], raws[(i - 1) % 2])
        form(bases[-1], raws[(len(bases) - 1) % 2])

    def b_loop(a_all, count, base_of):
        scores(a_all, base_of(0), raw0)

        def pair(i, carry):
            scores(a_all, base_of(2 * i + 1), raw1)
            form(base_of(2 * i), raw0)
            scores(a_all, base_of(2 * i + 2), raw0)
            form(base_of(2 * i + 1), raw1)
            return carry
        lax.fori_loop(0, count // 2 - 1, pair, 0)
        scores(a_all, base_of(count - 1), raw1)
        form(base_of(count - 2), raw0)
        form(base_of(count - 1), raw1)

    def a_slice(a_all, base):
        return a_all.at[span(base, CH), :]

    def my_base(i):
        return jnp.where(i < 2, me * NB + i * CH, far * NB + (i - 2) * CH)

    def their_base(i):
        return jnp.where(i < 2, partner * NB + i * CH, far_partner * NB + (i - 2) * CH)

    mine = [my_base(i) for i in range(4)]
    theirs = [their_base(i) for i in range(4)]

    def share(a_all, name, start, stop):
        slot = SIDE.names[(name, 0)]

        def piece(i):
            ref = a_slice(a_all, my_base(i))
            return pltpu.make_async_remote_copy(
                src_ref=ref, dst_ref=ref, send_sem=side_send.at[slot + i], recv_sem=side_recv.at[slot + i],
                device_id={"rows": partner}, device_id_type=pl.DeviceIdType.MESH)

        def step(i, carry):
            a_rows(a_all, i * CH, my_base(i))
            piece(i).start()
            return carry
        if stop - start == 1:
            step(start, 0)
        else:
            lax.fori_loop(start, stop, step, 0)
        for i in range(start, stop):
            sends.append(piece(i))

    acc_ref[...] = jnp.zeros_like(acc_ref)
    mark("a_own")
    share(a1_all, "a1", 0, 2)
    for i in range(2):
        partner_arrived(a_slice(a1_all, theirs[i]), ("a1", i))
    mark("b_own")
    b_rows(a1_all, [mine[0], mine[1], theirs[0], theirs[1]])
    mark("wait_quads")
    for k, piece in enumerate(c1_quads(NB, far_partner, core)):
        far_arrived(piece, ("c1 quad", k))
        go(to_partner(piece, quad_side.at[k * HALF:(k + 1) * HALF, :], ("c1 quad", k)))
    for k in range(2):
        partner_arrived(quad_side.at[k * HALF:(k + 1) * HALF, :], ("c1 quad", k))
    mark("quad_mirror")
    mirror(quad_side, 0, 0, c1_rows, NB, far_partner * NB + HALF, HALF)
    mirror(quad_side, HALF, 0, c1_rows, NB + (1 - core) * HALF, far_partner * NB + (1 - core) * HALF, HALF)
    for i in range(2):
        mark("wait_strips%d" % i)
        for k in (2 * i, 2 * i + 1):
            far_arrived(c1_strip(NB, far, k), ("c1 strip", k))
            for below in range(k + 1, 4):
                mirror(c1_rows, NB + k * 128, far * NB + below * 128, c1_rows, NB + below * 128, far * NB + k * 128, 128)
        mark("a_far%d" % i)
        share(a1_all, "a1", 2 + i, 3 + i)
    mark("b_far")
    partner_arrived(a_slice(a1_all, theirs[2]), ("a1", 2))
    partner_arrived(a_slice(a1_all, theirs[3]), ("a1", 3))
    b_rows(a1_all, [mine[2], theirs[2], mine[3], theirs[3]])
    store_col_scale([acc_ref[:, col(j)] for j in range(COLS)], v_ref, q_ref)
    mark("sweeps")
    sweeps(SWEEPS - 1, kern, p_b, u_b, v_ref, q_ref)

    mark("next_plan")
    for copy in sends:
        copy.wait_send()
    sends.clear()

    def next_plan(i, carry):
        row = hint(i * 64, 64)
        for j, t in scaled_rows(kern, u_b, v_ref, row, 64):
            t_all[pl.ds(row, 64), col(j)] = t.astype(BF16)
        return carry
    lax.fori_loop(0, N // 64, next_plan, 0)

    acc_ref[...] = jnp.zeros_like(acc_ref)
    mark("a_2")
    share(a2_all, "a2", 0, 4)
    mark("wait_a2")
    for i in range(4):
        partner_arrived(a_slice(a2_all, theirs[i]), ("a2", i))
    mark("b_2")
    b_loop(a2_all, 8, lambda i: jnp.where(i < 4, my_base(i), their_base(i - 4)))
    store_col_scale([acc_ref[:, col(j)] for j in range(COLS)], v_ref, q_ref)
    mark("sweeps")
    sweeps(SWEEPS - 1, kern, p_b, u_b, v_ref, q_ref)

    mark("result")

    def result(i, carry):
        row = hint(i * 64, 64)
        for j, t in scaled_rows(kern, u_b, v_ref, hint(me * NB + row, 64), 64):
            out_ref[pl.ds(row, 64), col(j)] = t
        return carry
    lax.fori_loop(0, NB // 64, result, 0)
    for copy in sends:
        copy.wait_send()
    mark(None)


def solution(mesh):
    vmem = pl.BlockSpec(memory_space=pltpu.VMEM)
    hbm = pl.BlockSpec(memory_space=pl.ANY)
    smem = pl.BlockSpec(memory_space=pltpu.SMEM)

    def local_fgw(cost_src, cost_tgt, plan_init, mass_src, mass_tgt, feat_src, feat_tgt, epsilon):
        return pl.pallas_call(
            kernel,
            out_shape=jax.ShapeDtypeStruct((NB, M), F32),
            in_specs=[hbm, hbm, hbm, hbm, vmem, hbm, hbm, smem],
            out_specs=vmem,
            scratch_shapes=[
                pltpu.VMEM((NB, N), F32),
                pltpu.VMEM((MB, M), F32),
                pltpu.VMEM((NB, M), F32),
                pltpu.VMEM((NB, D), F32),
                pltpu.VMEM((MB, D), F32),
                pltpu.VMEM((N, M), BF16),
                pltpu.VMEM((2 * NB, N), BF16),
                pltpu.VMEM((NB, NB), BF16),
                pltpu.VMEM((2 * HALF, HALF), BF16),
                pltpu.VMEM((M, M), BF16),
                pltpu.VMEM((M, D), BF16),
                pltpu.VMEM((N, D), BF16),
                pltpu.VMEM((N, M), F32),
                pltpu.VMEM((N, M), BF16),
                pltpu.VMEM((N, M), BF16),
                pltpu.VMEM((N, M), F32),
                pltpu.VMEM((4, NB // LANES, LANES), F32),
                pltpu.VMEM((N, LANES), F32),
                pltpu.VMEM((N, LANES), F32),
                pltpu.VMEM((CH, LANES), F32),
                pltpu.VMEM((CH, LANES), F32),
                pltpu.VMEM((8, M), F32),
                pltpu.VMEM((8, M), F32),
                pltpu.SemaphoreType.DMA((6,)),
                pltpu.SemaphoreType.DMA((len(LINK.names),)),
                pltpu.SemaphoreType.DMA((len(LINK.names),)),
                pltpu.SemaphoreType.DMA((len(SIDE.names),)),
                pltpu.SemaphoreType.DMA((len(SIDE.names),)),
            ],
            compiler_params=pltpu.CompilerParams(
                collective_id=0, has_side_effects=True, vmem_limit_bytes=56000 * 1024),
        )(cost_src, cost_tgt, plan_init, mass_src.reshape(NB // LANES, LANES), mass_tgt.reshape(1, M),
          feat_src, feat_tgt, epsilon.reshape(1, 1))

    row_spec = P(('pairs', 'rows'), None)
    vec_spec = P(('pairs', 'rows'))
    in_specs = (row_spec, row_spec, row_spec, vec_spec, P('pairs'), row_spec, row_spec, P())
    return jax.shard_map(local_fgw, mesh=mesh, in_specs=in_specs, out_specs=row_spec, check_vma=False)
```

```python
import jax
import jax.numpy as jnp
from jax import lax
from jax.experimental import pallas as pl
from jax.experimental.pallas import tpu as pltpu
from jax.sharding import PartitionSpec as P

ALPHA = 0.5
OUTER_STEPS = 2
SWEEPS = 10
LOG2E = 1.4426950408889634

N = 2048
M = 1024
D = 256
NB = 512
MB = 256
F32 = jnp.float32
BF16 = jnp.bfloat16
LANES = 128
COLS = M // LANES

T_CHUNKS = 4
TR = NB // T_CHUNKS
CH = 256
HALF = NB // 2
SWEEP_GROUP = 32
FORM_GROUP = 32


class Slots:
    def __init__(self):
        self.names = {}

    def __call__(self, name):
        return self.names.setdefault(name, len(self.names))


LINK = Slots()
SIDE = Slots()
for k in range(T_CHUNKS):
    LINK(("t", k)), SIDE(("t", k)), SIDE(("far t", k))
for k in range(4):
    LINK(("c2", k)), SIDE(("far c2", k)), LINK(("c1 strip", k))
for name in ("a1", "a2"):
    for k in range(4):
        SIDE((name, k))
for k in range(2):
    LINK(("c1 quad", k)), SIDE(("c1 quad", k))
for name in ("y", "x", "p"):
    LINK(name), SIDE(name), SIDE("far " + name)
SIDE("c2"), SIDE("c1")


def hint(value, multiple):
    return value if isinstance(value, int) else pl.multiple_of(value, multiple)


def span(start, size):
    return pl.ds(hint(start, size), size)


def col(j):
    return slice(j * LANES, (j + 1) * LANES)


def tree(op, parts):
    while len(parts) > 1:
        parts = [op(parts[i], parts[i + 1]) for i in range(0, len(parts), 2)]
    return parts[0]


def store_col_scale(acc, v_ref, q_ref):
    for j in range(COLS):
        col_sum = jnp.sum(acc[j], axis=0, keepdims=True)
        v_ref[:, col(j)] = jnp.broadcast_to(q_ref[:, col(j)] / col_sum, (8, LANES))


def sweeps(count, kern, plan_b, u_b, v_ref, q_ref):
    lead = 128
    group = SWEEP_GROUP
    shape = (group // 8, 8, LANES)

    def sweep(_, carry):
        v = [v_ref[:, col(j)][None] for j in range(COLS)]

        def tile(row, j):
            return kern[row:row + group, col(j)].reshape(shape)

        acc = [jnp.zeros((8, LANES), F32) for _ in range(COLS)]
        for row in range(-lead, N, group):
            top = row + lead
            if top < N:
                total = tree(jnp.add, [tile(top, j) * v[j] for j in range(COLS)])
                u = plan_b[top:top + group, :].reshape(shape) / jnp.sum(total, axis=2, keepdims=True)
                u_b[top:top + group, :] = u.reshape(group, LANES)
            if row >= 0:
                u = u_b[row:row + group, :].reshape(shape)
                acc = [acc[j] + jnp.sum(tile(row, j) * u, axis=0) for j in range(COLS)]
        store_col_scale(acc, v_ref, q_ref)
        return carry

    lax.fori_loop(0, count, sweep, 0)


def scaled_rows(kern, u_b, v_ref, row, count):
    u = u_b[pl.ds(row, count), :].reshape(count // 8, 8, LANES)
    for j in range(COLS):
        k = kern[pl.ds(row, count), col(j)].reshape(count // 8, 8, LANES)
        yield j, (u * k * v_ref[:, col(j)][None]).reshape(count, LANES)


def kernel(c1_hbm, c2_ref, t0_hbm, p_ref, q_ref, x_ref, y_ref, eps_ref, out_ref,
           t_st, t_all, c1_rows, c1_side, quad_side, c2_all, y_all, x_all, g_all, a1_all, a2_all,
           kern, p_all, p_b, u_b, peak_b, first_b, acc_ref, v_ref,
           load_sem, link_send, link_recv, side_send, side_recv):
    raw0, raw1 = 0, CH
    current = [None]

    def mark(name):
        if current[0] is not None:
            current[0].__exit__(None, None, None)
            current[0] = None
        if name:
            current[0] = jax.named_scope(name)
            current[0].__enter__()

    me = lax.axis_index("rows")
    chip = me // 2
    core = me % 2
    partner = chip * 2 + (1 - core)
    far = (1 - chip) * 2 + core
    far_partner = (1 - chip) * 2 + (1 - core)

    loads = [pltpu.make_async_copy(src, dst, load_sem.at[i]) for i, (src, dst) in enumerate((
        (t0_hbm, t_st), (c1_hbm.at[:, :M], g_all.at[:NB]), (c1_hbm.at[:, M:], g_all.at[NB:2 * NB])))]
    for copy in loads:
        copy.start()

    mark("barrier")
    barrier = pltpu.get_barrier_semaphore()
    for peer in (partner, far):
        pl.semaphore_signal(barrier, inc=1, device_id={"rows": peer}, device_id_type=pl.DeviceIdType.MESH)
    pl.semaphore_wait(barrier, 2)

    def to_far(src, dst, name):
        slot = LINK.names[name]
        return pltpu.make_async_remote_copy(
            src_ref=src, dst_ref=dst, send_sem=link_send.at[slot], recv_sem=link_recv.at[slot],
            device_id={"rows": far}, device_id_type=pl.DeviceIdType.MESH)

    def to_partner(src, dst, name):
        slot = SIDE.names[name]
        return pltpu.make_async_remote_copy(
            src_ref=src, dst_ref=dst, send_sem=side_send.at[slot], recv_sem=side_recv.at[slot],
            device_id={"rows": partner}, device_id_type=pl.DeviceIdType.MESH)

    sends = []

    def go(copy):
        copy.start()
        sends.append(copy)

    def far_arrived(ref, name):
        to_far(ref, ref, name).wait_recv()

    def partner_arrived(ref, name):
        to_partner(ref, ref, name).wait_recv()

    def t_rows(owner, k):
        return t_all.at[span(owner * NB + k * TR, TR), :]

    def c2_rows(owner):
        return c2_all.at[span(owner * MB, MB), :]

    def c2_pieces(owner, other, which):
        return (
            c2_all.at[span(owner * MB + 128, 128), span(other * MB, 128)],
            c2_all.at[span(owner * MB + which * 128, 128), span(other * MB + which * 128, 128)],
            c2_all.at[span(owner * MB, 128), span(owner * MB, MB)],
            c2_all.at[span(owner * MB + 128, 128), span(owner * MB + 128, 128)])

    def y_rows(owner):
        return y_all.at[span(owner * MB, MB), :]

    def x_rows(owner):
        return x_all.at[span(owner * NB, NB), :]

    def c1_quads(base, other, which):
        return (c1_rows.at[base + HALF:base + NB, span(other * NB, HALF)],
                c1_rows.at[span(base + which * HALF, HALF), span(other * NB + which * HALF, HALF)])

    def c1_strip(base, owner, k):
        return c1_rows.at[base + k * 128:base + (k + 1) * 128, pl.ds(hint(owner * NB + k * 128, 128), NB - k * 128)]

    mark("cast_y")
    y_all[span(me * MB, MB), :] = y_ref[...].astype(BF16)
    p_all[me] = p_ref[...]
    mark("cast_t")
    loads[0].wait()
    for k in range(T_CHUNKS):
        t_all[span(me * NB + k * TR, TR), :] = t_st[k * TR:(k + 1) * TR, :].astype(BF16)
    go(to_far(y_rows(me), y_rows(me), "y"))
    go(to_far(p_all.at[me], p_all.at[me], "p"))
    for k in range(T_CHUNKS):
        go(to_far(t_rows(me, k), t_rows(me, k), ("t", k)))
    go(to_partner(y_rows(me), y_rows(me), "y"))
    go(to_partner(p_all.at[me], p_all.at[me], "p"))
    for k in range(T_CHUNKS):
        go(to_partner(t_rows(me, k), t_rows(me, k), ("t", k)))
    mark("cast_rest")
    c2_all[span(me * MB, MB), :] = c2_ref[...].astype(BF16)
    x_all[span(me * NB, NB), :] = x_ref[...].astype(BF16)
    loads[1].wait()
    loads[2].wait()
    c1_rows[:NB, :M] = g_all[:NB, :].astype(BF16)
    c1_rows[:NB, M:] = g_all[NB:2 * NB, :].astype(BF16)
    for k, piece in enumerate(c2_pieces(me, partner, core)):
        go(to_far(piece, piece, ("c2", k)))
    go(to_far(x_rows(me), x_rows(me), "x"))
    for k, (src, dst) in enumerate(zip(c1_quads(0, partner, core), c1_quads(NB, partner, core))):
        go(to_far(src, dst, ("c1 quad", k)))
    for k in range(4):
        go(to_far(c1_strip(0, me, k), c1_strip(NB, me, k), ("c1 strip", k)))
    go(to_partner(c2_rows(me), c2_rows(me), "c2"))
    go(to_partner(x_rows(me), x_rows(me), "x"))
    go(to_partner(c1_rows.at[:NB, span(far_partner * NB, NB)], c1_side, "c1"))

    def mirror(src, src_row, src_col, dst, dst_row, dst_col, size):
        for i in range(size // LANES):
            for j in range(size // LANES):
                tile = src[span(src_row + i * LANES, LANES), span(src_col + j * LANES, LANES)]
                dst[span(dst_row + j * LANES, LANES), span(dst_col + i * LANES, LANES)] = (
                    tile.astype(F32).T.astype(BF16))

    mark("mirrors")
    mirror(c1_rows, 0, far * NB, c1_rows, NB, me * NB, NB)
    partner_arrived(c1_side, "c1")
    mirror(c1_side, 0, 0, c1_rows, NB, partner * NB, NB)
    partner_arrived(c2_rows(partner), "c2")
    mirror(c2_all, chip * 2 * MB, (1 - chip) * 2 * MB, c2_all, (1 - chip) * 2 * MB, chip * 2 * MB, 2 * MB)
    partner_arrived(y_rows(partner), "y")
    partner_arrived(p_all.at[partner], "p")
    partner_arrived(x_rows(partner), "x")

    def forward(ref, name):
        far_arrived(ref, name)
        go(to_partner(ref, ref, ("far " + name[0], name[1]) if isinstance(name, tuple) else "far " + name))

    def gram(owner):
        for n in range(4):
            g = lax.dot_general(x_all[span(owner * NB, NB), :], y_all[n * 256:(n + 1) * 256, :],
                                (((1,), (1,)), ((), ())), preferred_element_type=F32)
            g_all[span(owner * NB, NB), n * 256:(n + 1) * 256] = (2.0 * ALPHA) * g

    def grams(first, second):
        def one(i, carry):
            gram(first + i * (second - first))
            return carry
        lax.fori_loop(0, 2, one, 0)

    mark("wait_y")
    forward(y_rows(far), "y")
    forward(p_all.at[far], "p")
    partner_arrived(y_rows(far_partner), "far y")
    partner_arrived(p_all.at[far_partner], "far p")
    mark("p_b_gram")
    for owner in range(4):
        for i in range(NB // LANES):
            block = jnp.broadcast_to(p_all[owner, i:i + 1, :], (LANES, LANES))
            p_b[owner * NB + i * LANES:owner * NB + (i + 1) * LANES, :] = block.T
    grams(me, partner)
    mark("wait_t")
    for k in range(T_CHUNKS):
        partner_arrived(t_rows(partner, k), ("t", k))
    for k in range(T_CHUNKS):
        forward(t_rows(far, k), ("t", k))
    for k in range(T_CHUNKS):
        partner_arrived(t_rows(far_partner, k), ("far t", k))

    scale = LOG2E / eps_ref[0, 0]

    def a_rows(a_all, local, base):
        for n in range(4):
            a_all[span(base, CH), n * 256:(n + 1) * 256] = jnp.dot(
                c1_rows[span(local, CH), :], t_all[:, n * 256:(n + 1) * 256], preferred_element_type=F32).astype(BF16)

    def scores(a_all, base, raw):
        for n in range(4):
            b = jnp.dot(a_all[span(base, CH), :], c2_all[:, n * 256:(n + 1) * 256], preferred_element_type=F32)
            t_st[raw:raw + CH, n * 256:(n + 1) * 256] = g_all[span(base, CH), n * 256:(n + 1) * 256] + (2.0 * (1.0 - ALPHA)) * b

    def form(base, raw):
        acc = [acc_ref[:, col(j)] for j in range(COLS)]
        lead = 64
        group = FORM_GROUP
        shape = (group // 8, 8, LANES)
        for row in range(-2 * lead, CH, group):
            top = row + 2 * lead
            if top < CH:
                peak = tree(jnp.maximum, [t_st[raw + top:raw + top + group, col(j)] for j in range(COLS)])
                peak_b[top:top + group, :] = jnp.broadcast_to(jnp.max(peak, axis=1, keepdims=True), (group, LANES))
            mid = row + lead
            if 0 <= mid < CH:
                here = pl.ds(hint(base + mid, group), group)
                peak = peak_b[mid:mid + group, :]
                vals = [jnp.exp2((t_st[raw + mid:raw + mid + group, col(j)] - peak) * scale) for j in range(COLS)]
                for j in range(COLS):
                    kern[here, col(j)] = vals[j]
                total = jnp.sum(tree(jnp.add, vals), axis=1, keepdims=True)
                first_b[mid:mid + group, :] = p_b[here, :] / total
            if row >= 0:
                here = pl.ds(hint(base + row, group), group)
                u = first_b[row:row + group, :].reshape(shape)
                acc = [acc[j] + jnp.sum(kern[here, col(j)].reshape(shape) * u, axis=0) for j in range(COLS)]
        for j in range(COLS):
            acc_ref[:, col(j)] = acc[j]

    def b_rows(a_all, bases, ready=None):
        raws = (raw0, raw1)
        for i, base in enumerate(bases):
            if ready and ready[i]:
                ready[i]()
            scores(a_all, base, raws[i % 2])
            if i:
                form(bases[i - 1], raws[(i - 1) % 2])
        form(bases[-1], raws[(len(bases) - 1) % 2])

    def a_slice(a_all, base):
        return a_all.at[span(base, CH), :]

    def my_base(i):
        return jnp.where(i < 2, me * NB + i * CH, far * NB + (i - 2) * CH)

    def their_base(i):
        return jnp.where(i < 2, partner * NB + i * CH, far_partner * NB + (i - 2) * CH)

    mine = [my_base(i) for i in range(4)]
    theirs = [their_base(i) for i in range(4)]

    def share(a_all, name, start, stop):
        slot = SIDE.names[(name, 0)]

        def piece(i):
            ref = a_slice(a_all, my_base(i))
            return pltpu.make_async_remote_copy(
                src_ref=ref, dst_ref=ref, send_sem=side_send.at[slot + i], recv_sem=side_recv.at[slot + i],
                device_id={"rows": partner}, device_id_type=pl.DeviceIdType.MESH)

        def step(i, carry):
            a_rows(a_all, i * CH, my_base(i))
            piece(i).start()
            return carry
        if stop - start == 1:
            step(start, 0)
        else:
            lax.fori_loop(start, stop, step, 0)
        for i in range(start, stop):
            sends.append(piece(i))

    def b_groups(a_all, name, count):
        def group(g, carry):
            @pl.when(g == 1)
            def _():
                for i in range(count):
                    partner_arrived(a_slice(a_all, theirs[i]), (name, i))
            b_rows(a_all, [jnp.where(g == 0, mine[i], theirs[i]) for i in range(count)])
            return carry
        lax.fori_loop(0, 2, group, 0)

    acc_ref[...] = jnp.zeros_like(acc_ref)
    mark("a_own")
    share(a1_all, "a1", 0, 2)
    mark("wait_c2")
    for k, piece in enumerate(c2_pieces(far, far_partner, core)):
        forward(piece, ("c2", k))
    for k, piece in enumerate(c2_pieces(far_partner, far, 1 - core)):
        partner_arrived(piece, ("far c2", k))
    mark("c2_mirror")
    first = (1 - chip) * 2 * MB
    second = first + MB
    for base in (first, second):
        mirror(c2_all, base, base + 128, c2_all, base + 128, base, 128)
    mirror(c2_all, second + 128, first, c2_all, first, second + 128, 128)
    mirror(c2_all, second + 128, first + 128, c2_all, first + 128, second + 128, 128)
    mirror(c2_all, first, second, c2_all, second, first, 128)
    mirror(c2_all, first + 128, second, c2_all, second, first + 128, 128)
    mark("b_own")
    b_groups(a1_all, "a1", 2)
    mark("wait_x")
    forward(x_rows(far), "x")
    partner_arrived(x_rows(far_partner), "far x")
    mark("gram_far")
    grams(far, far_partner)
    mark("wait_quads")
    for k, piece in enumerate(c1_quads(NB, far_partner, core)):
        far_arrived(piece, ("c1 quad", k))
        go(to_partner(piece, quad_side.at[k * HALF:(k + 1) * HALF, :], ("c1 quad", k)))
    for k in range(2):
        partner_arrived(quad_side.at[k * HALF:(k + 1) * HALF, :], ("c1 quad", k))
    mark("quad_mirror")
    mirror(quad_side, 0, 0, c1_rows, NB, far_partner * NB + HALF, HALF)
    mirror(quad_side, HALF, 0, c1_rows, NB + (1 - core) * HALF, far_partner * NB + (1 - core) * HALF, HALF)
    for i in range(2):
        mark("wait_strips%d" % i)
        for k in (2 * i, 2 * i + 1):
            far_arrived(c1_strip(NB, far, k), ("c1 strip", k))
            for below in range(k + 1, 4):
                mirror(c1_rows, NB + k * 128, far * NB + below * 128, c1_rows, NB + below * 128, far * NB + k * 128, 128)
        mark("a_far%d" % i)
        share(a1_all, "a1", 2 + i, 3 + i)
        if i == 0:
            mark("b_far0")
            b_rows(a1_all, [mine[2]])
    mark("b_far1")
    b_rows(a1_all, [theirs[2], mine[3], theirs[3]],
           [lambda: partner_arrived(a_slice(a1_all, theirs[2]), ("a1", 2)), None,
            lambda: partner_arrived(a_slice(a1_all, theirs[3]), ("a1", 3))])
    store_col_scale([acc_ref[:, col(j)] for j in range(COLS)], v_ref, q_ref)
    mark("sweeps")
    sweeps(SWEEPS - 1, kern, p_b, u_b, v_ref, q_ref)

    mark("next_plan")
    for copy in sends:
        copy.wait_send()
    sends.clear()

    def next_plan(i, carry):
        row = hint(i * 256, 256)
        for j, t in scaled_rows(kern, u_b, v_ref, row, 256):
            t_all[pl.ds(row, 256), col(j)] = t.astype(BF16)
        return carry
    lax.fori_loop(0, N // 256, next_plan, 0)

    acc_ref[...] = jnp.zeros_like(acc_ref)
    mark("a_2")
    share(a2_all, "a2", 0, 4)
    mark("b_2")
    b_groups(a2_all, "a2", 4)
    store_col_scale([acc_ref[:, col(j)] for j in range(COLS)], v_ref, q_ref)
    mark("sweeps")
    sweeps(SWEEPS - 1, kern, p_b, u_b, v_ref, q_ref)

    mark("result")

    def result(i, carry):
        row = hint(i * 64, 64)
        for j, t in scaled_rows(kern, u_b, v_ref, hint(me * NB + row, 64), 64):
            out_ref[pl.ds(row, 64), col(j)] = t
        return carry
    lax.fori_loop(0, NB // 64, result, 0)
    for copy in sends:
        copy.wait_send()
    mark(None)


def solution(mesh):
    vmem = pl.BlockSpec(memory_space=pltpu.VMEM)
    hbm = pl.BlockSpec(memory_space=pl.ANY)
    smem = pl.BlockSpec(memory_space=pltpu.SMEM)

    def local_fgw(cost_src, cost_tgt, plan_init, mass_src, mass_tgt, feat_src, feat_tgt, epsilon):
        return pl.pallas_call(
            kernel,
            out_shape=jax.ShapeDtypeStruct((NB, M), F32),
            in_specs=[hbm, vmem, hbm, vmem, vmem, vmem, vmem, smem],
            out_specs=vmem,
            scratch_shapes=[
                pltpu.VMEM((NB, M), F32),
                pltpu.VMEM((N, M), BF16),
                pltpu.VMEM((2 * NB, N), BF16),
                pltpu.VMEM((NB, NB), BF16),
                pltpu.VMEM((2 * HALF, HALF), BF16),
                pltpu.VMEM((M, M), BF16),
                pltpu.VMEM((M, D), BF16),
                pltpu.VMEM((N, D), BF16),
                pltpu.VMEM((N, M), F32),
                pltpu.VMEM((N, M), BF16),
                pltpu.VMEM((N, M), BF16),
                pltpu.VMEM((N, M), F32),
                pltpu.VMEM((4, NB // LANES, LANES), F32),
                pltpu.VMEM((N, LANES), F32),
                pltpu.VMEM((N, LANES), F32),
                pltpu.VMEM((CH, LANES), F32),
                pltpu.VMEM((CH, LANES), F32),
                pltpu.VMEM((8, M), F32),
                pltpu.VMEM((8, M), F32),
                pltpu.SemaphoreType.DMA((3,)),
                pltpu.SemaphoreType.DMA((len(LINK.names),)),
                pltpu.SemaphoreType.DMA((len(LINK.names),)),
                pltpu.SemaphoreType.DMA((len(SIDE.names),)),
                pltpu.SemaphoreType.DMA((len(SIDE.names),)),
            ],
            compiler_params=pltpu.CompilerParams(
                collective_id=0, has_side_effects=True, vmem_limit_bytes=50000 * 1024),
        )(cost_src, cost_tgt, plan_init, mass_src.reshape(NB // LANES, LANES), mass_tgt.reshape(1, M),
          feat_src, feat_tgt, epsilon.reshape(1, 1))

    row_spec = P(('pairs', 'rows'), None)
    vec_spec = P(('pairs', 'rows'))
    in_specs = (row_spec, row_spec, row_spec, vec_spec, P('pairs'), row_spec, row_spec, P())
    return jax.shard_map(local_fgw, mesh=mesh, in_specs=in_specs, out_specs=row_spec, check_vma=False)
```

```python
import jax
import jax.numpy as jnp
from jax import lax
from jax.experimental import pallas as pl
from jax.experimental.pallas import tpu as pltpu
from jax.sharding import PartitionSpec as P

ALPHA = 0.5
OUTER_STEPS = 2
SWEEPS = 10
LOG2E = 1.4426950408889634

N = 2048
M = 1024
D = 256
NB = 512
MB = 256
F32 = jnp.float32
BF16 = jnp.bfloat16
LANES = 128
COLS = M // LANES

T_CHUNKS = 4
TR = NB // T_CHUNKS
CH = 256
HALF = NB // 2
SWEEP_GROUP = 16
FORM_GROUP = 32


class Slots:
    def __init__(self):
        self.names = {}

    def __call__(self, name):
        return self.names.setdefault(name, len(self.names))


LINK = Slots()
SIDE = Slots()
for k in range(T_CHUNKS):
    LINK(("t", k)), SIDE(("t", k)), SIDE(("far t", k))
for k in range(4):
    LINK(("c2", k)), SIDE(("far c2", k)), LINK(("c1 strip", k))
for k in range(4):
    SIDE(("a1", k))
for k in range(2):
    SIDE(("a2", k))
for k in range(2):
    LINK(("c1 quad", k)), SIDE(("c1 quad", k))
for name in ("y", "x", "p"):
    LINK(name), SIDE(name), SIDE("far " + name)
SIDE("c2"), SIDE("c1")


def hint(value, multiple):
    return value if isinstance(value, int) else pl.multiple_of(value, multiple)


def span(start, size):
    return pl.ds(hint(start, size), size)


def col(j):
    return slice(j * LANES, (j + 1) * LANES)


def tree(op, parts):
    while len(parts) > 1:
        parts = [op(parts[i], parts[i + 1]) for i in range(0, len(parts), 2)]
    return parts[0]


def store_col_scale(acc, v_ref, q_ref):
    for j in range(COLS):
        col_sum = jnp.sum(acc[j], axis=0, keepdims=True)
        v_ref[:, col(j)] = jnp.broadcast_to(q_ref[:, col(j)] / col_sum, (8, LANES))


def sweeps(count, kern, plan_b, u_b, v_ref, q_ref):
    lead = 128
    group = SWEEP_GROUP
    shape = (group // 8, 8, LANES)

    def sweep(_, carry):
        v = [v_ref[:, col(j)][None] for j in range(COLS)]

        def tile(row, j):
            return kern[row:row + group, col(j)].reshape(shape)

        acc = [jnp.zeros((8, LANES), F32) for _ in range(COLS)]
        for row in range(-lead, N, group):
            top = row + lead
            if top < N:
                total = tree(jnp.add, [tile(top, j) * v[j] for j in range(COLS)])
                u = plan_b[top:top + group, :].reshape(shape) / jnp.sum(total, axis=2, keepdims=True)
                u_b[top:top + group, :] = u.reshape(group, LANES)
            if row >= 0:
                u = u_b[row:row + group, :].reshape(shape)
                acc = [acc[j] + jnp.sum(tile(row, j) * u, axis=0) for j in range(COLS)]
        store_col_scale(acc, v_ref, q_ref)
        return carry

    lax.fori_loop(0, count, sweep, 0)


def scaled_rows(kern, u_b, v_ref, row, count):
    u = u_b[pl.ds(row, count), :].reshape(count // 8, 8, LANES)
    for j in range(COLS):
        k = kern[pl.ds(row, count), col(j)].reshape(count // 8, 8, LANES)
        yield j, (u * k * v_ref[:, col(j)][None]).reshape(count, LANES)


def kernel(c1_hbm, c2_hbm, t0_hbm, p_hbm, q_hbm, x_hbm, y_hbm, eps_ref, out_ref,
           q_ref, t_st, t_all, c1_rows, c1_side, quad_side, c2_all, y_all, x_all, g_all, a1_all, a2_all,
           kern, p_all, p_b, u_b, peak_b, first_b, acc_ref, v_ref,
           load_sem, link_send, link_recv, side_send, side_recv):
    raw0, raw1 = 0, CH
    current = [None]

    def mark(name):
        if current[0] is not None:
            current[0].__exit__(None, None, None)
            current[0] = None
        if name:
            current[0] = jax.named_scope(name)
            current[0].__enter__()

    me = lax.axis_index("rows")
    chip = me // 2
    core = me % 2
    partner = chip * 2 + (1 - core)
    far = (1 - chip) * 2 + core
    far_partner = (1 - chip) * 2 + (1 - core)

    y_st, x_st, c2_st = kern.at[:MB, :D], kern.at[MB:MB + NB, :D], kern.at[MB + NB:2 * MB + NB, :]
    loads = {}
    for i, (name, src, dst) in enumerate((
            ("y", y_hbm, y_st), ("p", p_hbm, p_all.at[me]), ("t", t0_hbm, t_st), ("c2", c2_hbm, c2_st), ("x", x_hbm, x_st),
            ("left", c1_hbm.at[:, :M], g_all.at[:NB]), ("right", c1_hbm.at[:, M:], g_all.at[NB:2 * NB]), ("q", q_hbm, q_ref))):
        loads[name] = pltpu.make_async_copy(src, dst, load_sem.at[i])
        loads[name].start()

    mark("barrier")
    barrier = pltpu.get_barrier_semaphore()
    for peer in (partner, far):
        pl.semaphore_signal(barrier, inc=1, device_id={"rows": peer}, device_id_type=pl.DeviceIdType.MESH)
    pl.semaphore_wait(barrier, 2)

    def to_far(src, dst, name):
        slot = LINK.names[name]
        return pltpu.make_async_remote_copy(
            src_ref=src, dst_ref=dst, send_sem=link_send.at[slot], recv_sem=link_recv.at[slot],
            device_id={"rows": far}, device_id_type=pl.DeviceIdType.MESH)

    def to_partner(src, dst, name):
        slot = SIDE.names[name]
        return pltpu.make_async_remote_copy(
            src_ref=src, dst_ref=dst, send_sem=side_send.at[slot], recv_sem=side_recv.at[slot],
            device_id={"rows": partner}, device_id_type=pl.DeviceIdType.MESH)

    sends = []

    def go(copy):
        copy.start()
        sends.append(copy)

    def far_arrived(ref, name):
        to_far(ref, ref, name).wait_recv()

    def partner_arrived(ref, name):
        to_partner(ref, ref, name).wait_recv()

    def t_rows(owner, k):
        return t_all.at[span(owner * NB + k * TR, TR), :]

    def c2_rows(owner):
        return c2_all.at[span(owner * MB, MB), :]

    def c2_pieces(owner, other, which):
        return (
            c2_all.at[span(owner * MB + 128, 128), span(other * MB, 128)],
            c2_all.at[span(owner * MB + which * 128, 128), span(other * MB + which * 128, 128)],
            c2_all.at[span(owner * MB, 128), span(owner * MB, MB)],
            c2_all.at[span(owner * MB + 128, 128), span(owner * MB + 128, 128)])

    def y_rows(owner):
        return y_all.at[span(owner * MB, MB), :]

    def x_rows(owner):
        return x_all.at[span(owner * NB, NB), :]

    def c1_quads(base, other, which):
        return (c1_rows.at[base + HALF:base + NB, span(other * NB, HALF)],
                c1_rows.at[span(base + which * HALF, HALF), span(other * NB + which * HALF, HALF)])

    def c1_strip(base, owner, k):
        return c1_rows.at[base + k * 128:base + (k + 1) * 128, pl.ds(hint(owner * NB + k * 128, 128), NB - k * 128)]

    mark("cast_y")
    loads["y"].wait()
    y_all[span(me * MB, MB), :] = kern[:MB, :D].astype(BF16)
    loads["p"].wait()
    mark("cast_t")
    loads["t"].wait()
    for k in range(T_CHUNKS):
        t_all[span(me * NB + k * TR, TR), :] = t_st[k * TR:(k + 1) * TR, :].astype(BF16)
    go(to_far(y_rows(me), y_rows(me), "y"))
    go(to_far(p_all.at[me], p_all.at[me], "p"))
    for k in range(T_CHUNKS):
        go(to_far(t_rows(me, k), t_rows(me, k), ("t", k)))
    go(to_partner(y_rows(me), y_rows(me), "y"))
    go(to_partner(p_all.at[me], p_all.at[me], "p"))
    for k in range(T_CHUNKS):
        go(to_partner(t_rows(me, k), t_rows(me, k), ("t", k)))
    mark("cast_rest")
    for name in ("c2", "x", "left", "right", "q"):
        loads[name].wait()
    c2_all[span(me * MB, MB), :] = kern[MB + NB:2 * MB + NB, :].astype(BF16)
    x_all[span(me * NB, NB), :] = kern[MB:MB + NB, :D].astype(BF16)
    c1_rows[:NB, :M] = g_all[:NB, :].astype(BF16)
    c1_rows[:NB, M:] = g_all[NB:2 * NB, :].astype(BF16)
    for k, piece in enumerate(c2_pieces(me, partner, core)):
        go(to_far(piece, piece, ("c2", k)))
    go(to_far(x_rows(me), x_rows(me), "x"))
    for k, (src, dst) in enumerate(zip(c1_quads(0, partner, core), c1_quads(NB, partner, core))):
        go(to_far(src, dst, ("c1 quad", k)))
    for k in range(4):
        go(to_far(c1_strip(0, me, k), c1_strip(NB, me, k), ("c1 strip", k)))
    go(to_partner(c2_rows(me), c2_rows(me), "c2"))
    go(to_partner(x_rows(me), x_rows(me), "x"))
    go(to_partner(c1_rows.at[:NB, span(far_partner * NB, NB)], c1_side, "c1"))

    def mirror(src, src_row, src_col, dst, dst_row, dst_col, size):
        for i in range(size // LANES):
            for j in range(size // LANES):
                tile = src[span(src_row + i * LANES, LANES), span(src_col + j * LANES, LANES)]
                dst[span(dst_row + j * LANES, LANES), span(dst_col + i * LANES, LANES)] = (
                    tile.astype(F32).T.astype(BF16))

    mark("mirrors")
    mirror(c1_rows, 0, far * NB, c1_rows, NB, me * NB, NB)
    partner_arrived(c1_side, "c1")
    mirror(c1_side, 0, 0, c1_rows, NB, partner * NB, NB)
    partner_arrived(c2_rows(partner), "c2")
    mirror(c2_all, chip * 2 * MB, (1 - chip) * 2 * MB, c2_all, (1 - chip) * 2 * MB, chip * 2 * MB, 2 * MB)
    partner_arrived(y_rows(partner), "y")
    partner_arrived(p_all.at[partner], "p")
    partner_arrived(x_rows(partner), "x")

    def forward(ref, name):
        far_arrived(ref, name)
        go(to_partner(ref, ref, ("far " + name[0], name[1]) if isinstance(name, tuple) else "far " + name))

    def gram(owner):
        for n in range(4):
            g = lax.dot_general(x_all[span(owner * NB, NB), :], y_all[n * 256:(n + 1) * 256, :],
                                (((1,), (1,)), ((), ())), preferred_element_type=F32)
            g_all[span(owner * NB, NB), n * 256:(n + 1) * 256] = (2.0 * ALPHA) * g

    def grams(first, second):
        def one(i, carry):
            gram(first + i * (second - first))
            return carry
        lax.fori_loop(0, 2, one, 0)

    mark("wait_y")
    forward(y_rows(far), "y")
    forward(p_all.at[far], "p")
    partner_arrived(y_rows(far_partner), "far y")
    partner_arrived(p_all.at[far_partner], "far p")
    mark("p_b_gram")
    for owner in range(4):
        for i in range(NB // LANES):
            block = jnp.broadcast_to(p_all[owner, i:i + 1, :], (LANES, LANES))
            p_b[owner * NB + i * LANES:owner * NB + (i + 1) * LANES, :] = block.T
    grams(me, partner)
    mark("wait_t")
    for k in range(T_CHUNKS):
        partner_arrived(t_rows(partner, k), ("t", k))
    for k in range(T_CHUNKS):
        forward(t_rows(far, k), ("t", k))
    for k in range(T_CHUNKS):
        partner_arrived(t_rows(far_partner, k), ("far t", k))

    scale = LOG2E / eps_ref[0, 0]

    def a_rows(a_all, local, base, rows=CH):
        for n in range(4):
            a_all[span(base, rows), n * 256:(n + 1) * 256] = jnp.dot(
                c1_rows[span(local, rows), :], t_all[:, n * 256:(n + 1) * 256], preferred_element_type=F32).astype(BF16)

    def scores(a_all, base, raw):
        for n in range(4):
            b = jnp.dot(a_all[span(base, CH), :], c2_all[:, n * 256:(n + 1) * 256], preferred_element_type=F32)
            t_st[raw:raw + CH, n * 256:(n + 1) * 256] = g_all[span(base, CH), n * 256:(n + 1) * 256] + (2.0 * (1.0 - ALPHA)) * b

    def form(base, raw):
        acc = [acc_ref[:, col(j)] for j in range(COLS)]
        lead = 64
        group = FORM_GROUP
        shape = (group // 8, 8, LANES)
        for row in range(-2 * lead, CH, group):
            top = row + 2 * lead
            if top < CH:
                peak = tree(jnp.maximum, [t_st[raw + top:raw + top + group, col(j)] for j in range(COLS)])
                peak_b[top:top + group, :] = jnp.broadcast_to(jnp.max(peak, axis=1, keepdims=True), (group, LANES))
            mid = row + lead
            if 0 <= mid < CH:
                here = pl.ds(hint(base + mid, group), group)
                peak = peak_b[mid:mid + group, :]
                vals = [jnp.exp2((t_st[raw + mid:raw + mid + group, col(j)] - peak) * scale) for j in range(COLS)]
                for j in range(COLS):
                    kern[here, col(j)] = vals[j]
                total = jnp.sum(tree(jnp.add, vals), axis=1, keepdims=True)
                first_b[mid:mid + group, :] = p_b[here, :] / total
            if row >= 0:
                here = pl.ds(hint(base + row, group), group)
                u = first_b[row:row + group, :].reshape(shape)
                acc = [acc[j] + jnp.sum(kern[here, col(j)].reshape(shape) * u, axis=0) for j in range(COLS)]
        for j in range(COLS):
            acc_ref[:, col(j)] = acc[j]

    def b_rows(a_all, bases, ready=None):
        raws = (raw0, raw1)
        for i, base in enumerate(bases):
            if ready and ready[i]:
                ready[i]()
            scores(a_all, base, raws[i % 2])
            if i:
                form(bases[i - 1], raws[(i - 1) % 2])
        form(bases[-1], raws[(len(bases) - 1) % 2])

    def a_slice(a_all, base):
        return a_all.at[span(base, CH), :]

    def my_base(i):
        return jnp.where(i < 2, me * NB + i * CH, far * NB + (i - 2) * CH)

    def their_base(i):
        return jnp.where(i < 2, partner * NB + i * CH, far_partner * NB + (i - 2) * CH)

    mine = [my_base(i) for i in range(4)]
    theirs = [their_base(i) for i in range(4)]

    def share(a_all, name, start, stop):
        slot = SIDE.names[(name, 0)]

        def piece(i):
            ref = a_slice(a_all, my_base(i))
            return pltpu.make_async_remote_copy(
                src_ref=ref, dst_ref=ref, send_sem=side_send.at[slot + i], recv_sem=side_recv.at[slot + i],
                device_id={"rows": partner}, device_id_type=pl.DeviceIdType.MESH)

        def step(i, carry):
            a_rows(a_all, i * CH, my_base(i))
            piece(i).start()
            return carry
        if stop - start == 1:
            step(start, 0)
        else:
            lax.fori_loop(start, stop, step, 0)
        for i in range(start, stop):
            sends.append(piece(i))

    def b_groups(a_all, count, arrived):
        def group(g, carry):
            @pl.when(g == 1)
            def _():
                arrived()
            b_rows(a_all, [jnp.where(g == 0, mine[i], theirs[i]) for i in range(count)])
            return carry
        lax.fori_loop(0, 2, group, 0)

    acc_ref[...] = jnp.zeros_like(acc_ref)
    mark("a_own")
    share(a1_all, "a1", 0, 2)
    mark("wait_c2")
    for k, piece in enumerate(c2_pieces(far, far_partner, core)):
        forward(piece, ("c2", k))
    for k, piece in enumerate(c2_pieces(far_partner, far, 1 - core)):
        partner_arrived(piece, ("far c2", k))
    mark("c2_mirror")
    first = (1 - chip) * 2 * MB
    second = first + MB
    for base in (first, second):
        mirror(c2_all, base, base + 128, c2_all, base + 128, base, 128)
    mirror(c2_all, second + 128, first, c2_all, first, second + 128, 128)
    mirror(c2_all, second + 128, first + 128, c2_all, first + 128, second + 128, 128)
    mirror(c2_all, first, second, c2_all, second, first, 128)
    mirror(c2_all, first + 128, second, c2_all, second, first + 128, 128)
    mark("b_own")

    def a1_arrived():
        for i in range(2):
            partner_arrived(a_slice(a1_all, theirs[i]), ("a1", i))
    b_groups(a1_all, 2, a1_arrived)
    mark("wait_x")
    forward(x_rows(far), "x")
    partner_arrived(x_rows(far_partner), "far x")
    mark("gram_far")
    grams(far, far_partner)
    mark("wait_quads")
    for k, piece in enumerate(c1_quads(NB, far_partner, core)):
        far_arrived(piece, ("c1 quad", k))
        go(to_partner(piece, quad_side.at[k * HALF:(k + 1) * HALF, :], ("c1 quad", k)))
    for k in range(2):
        partner_arrived(quad_side.at[k * HALF:(k + 1) * HALF, :], ("c1 quad", k))
    mark("quad_mirror")
    mirror(quad_side, 0, 0, c1_rows, NB, far_partner * NB + HALF, HALF)
    mirror(quad_side, HALF, 0, c1_rows, NB + (1 - core) * HALF, far_partner * NB + (1 - core) * HALF, HALF)
    for i in range(2):
        mark("wait_strips%d" % i)
        for k in (2 * i, 2 * i + 1):
            far_arrived(c1_strip(NB, far, k), ("c1 strip", k))
            for below in range(k + 1, 4):
                mirror(c1_rows, NB + k * 128, far * NB + below * 128, c1_rows, NB + below * 128, far * NB + k * 128, 128)
        mark("a_far%d" % i)
        share(a1_all, "a1", 2 + i, 3 + i)
        if i == 0:
            mark("b_far0")
            b_rows(a1_all, [mine[2]])
    mark("b_far1")
    b_rows(a1_all, [theirs[2], mine[3], theirs[3]],
           [lambda: partner_arrived(a_slice(a1_all, theirs[2]), ("a1", 2)), None,
            lambda: partner_arrived(a_slice(a1_all, theirs[3]), ("a1", 3))])
    store_col_scale([acc_ref[:, col(j)] for j in range(COLS)], v_ref, q_ref)
    mark("sweeps")
    sweeps(SWEEPS - 1, kern, p_b, u_b, v_ref, q_ref)

    mark("next_plan")
    for copy in sends:
        copy.wait_send()
    sends.clear()

    def next_plan(i, carry):
        row = hint(i * 64, 64)
        for j, t in scaled_rows(kern, u_b, v_ref, row, 64):
            t_all[pl.ds(row, 64), col(j)] = t.astype(BF16)
        return carry
    lax.fori_loop(0, N // 64, next_plan, 0)

    acc_ref[...] = jnp.zeros_like(acc_ref)
    mark("a_2")
    first_slot = SIDE.names[("a2", 0)]

    def a2_piece(i):
        ref = a2_all.at[span(jnp.where(i == 0, me, far) * NB, NB), :]
        return pltpu.make_async_remote_copy(
            src_ref=ref, dst_ref=ref, send_sem=side_send.at[first_slot + i], recv_sem=side_recv.at[first_slot + i],
            device_id={"rows": partner}, device_id_type=pl.DeviceIdType.MESH)

    def a2_step(i, carry):
        a_rows(a2_all, i * NB, jnp.where(i == 0, me, far) * NB, NB)
        a2_piece(i).start()
        return carry
    lax.fori_loop(0, 2, a2_step, 0)
    sends.extend((a2_piece(0), a2_piece(1)))
    mark("b_2")

    def a2_arrived():
        for i in range(2):
            a2_piece(i).wait_recv()
    b_groups(a2_all, 4, a2_arrived)
    store_col_scale([acc_ref[:, col(j)] for j in range(COLS)], v_ref, q_ref)
    mark("sweeps")
    sweeps(SWEEPS - 1, kern, p_b, u_b, v_ref, q_ref)

    mark("result")

    def result(i, carry):
        row = hint(i * 64, 64)
        for j, t in scaled_rows(kern, u_b, v_ref, hint(me * NB + row, 64), 64):
            out_ref[pl.ds(row, 64), col(j)] = t
        return carry
    lax.fori_loop(0, NB // 64, result, 0)
    for copy in sends:
        copy.wait_send()
    mark(None)


def solution(mesh):
    vmem = pl.BlockSpec(memory_space=pltpu.VMEM)
    hbm = pl.BlockSpec(memory_space=pl.ANY)
    smem = pl.BlockSpec(memory_space=pltpu.SMEM)

    def local_fgw(cost_src, cost_tgt, plan_init, mass_src, mass_tgt, feat_src, feat_tgt, epsilon):
        return pl.pallas_call(
            kernel,
            out_shape=pltpu.VMEM((NB, M), F32),
            in_specs=[hbm] * 7 + [smem],
            out_specs=vmem,
            scratch_shapes=[
                pltpu.VMEM((1, M), F32),
                pltpu.VMEM((NB, M), F32),
                pltpu.VMEM((N, M), BF16),
                pltpu.VMEM((2 * NB, N), BF16),
                pltpu.VMEM((NB, NB), BF16),
                pltpu.VMEM((2 * HALF, HALF), BF16),
                pltpu.VMEM((M, M), BF16),
                pltpu.VMEM((M, D), BF16),
                pltpu.VMEM((N, D), BF16),
                pltpu.VMEM((N, M), F32),
                pltpu.VMEM((N, M), BF16),
                pltpu.VMEM((N, M), BF16),
                pltpu.VMEM((N, M), F32),
                pltpu.VMEM((4, NB // LANES, LANES), F32),
                pltpu.VMEM((N, LANES), F32),
                pltpu.VMEM((N, LANES), F32),
                pltpu.VMEM((CH, LANES), F32),
                pltpu.VMEM((CH, LANES), F32),
                pltpu.VMEM((8, M), F32),
                pltpu.VMEM((8, M), F32),
                pltpu.SemaphoreType.DMA((8,)),
                pltpu.SemaphoreType.DMA((len(LINK.names),)),
                pltpu.SemaphoreType.DMA((len(LINK.names),)),
                pltpu.SemaphoreType.DMA((len(SIDE.names),)),
                pltpu.SemaphoreType.DMA((len(SIDE.names),)),
            ],
            compiler_params=pltpu.CompilerParams(
                collective_id=0, has_side_effects=True, vmem_limit_bytes=54000 * 1024),
        )(*(pltpu.with_memory_space_constraint(x, pltpu.HBM) for x in (
            cost_src, cost_tgt, plan_init, mass_src.reshape(NB // LANES, LANES), mass_tgt.reshape(1, M),
            feat_src, feat_tgt)), epsilon.reshape(1, 1))

    row_spec = P(('pairs', 'rows'), None)
    vec_spec = P(('pairs', 'rows'))
    in_specs = (row_spec, row_spec, row_spec, vec_spec, P('pairs'), row_spec, row_spec, P())
    return jax.shard_map(local_fgw, mesh=mesh, in_specs=in_specs, out_specs=row_spec, check_vma=False)
```

```python
import jax
import jax.numpy as jnp
from jax import lax
from jax.experimental import pallas as pl
from jax.experimental.pallas import tpu as pltpu
from jax.sharding import PartitionSpec as P

ALPHA = 0.5
OUTER_STEPS = 2
SWEEPS = 10
LOG2E = 1.4426950408889634

N = 2048
M = 1024
D = 256
NB = 512
MB = 256
F32 = jnp.float32
BF16 = jnp.bfloat16
LANES = 128
COLS = M // LANES

T_CHUNKS = 4
TR = NB // T_CHUNKS
CH = 256
HALF = NB // 2
SWEEP_GROUP = 16
FORM_GROUP = 32


class Slots:
    def __init__(self):
        self.names = {}

    def __call__(self, name):
        return self.names.setdefault(name, len(self.names))


LINK = Slots()
SIDE = Slots()
for k in range(T_CHUNKS):
    LINK(("t", k)), SIDE(("t", k)), SIDE(("far t", k))
for k in range(4):
    LINK(("c2", k)), SIDE(("far c2", k)), LINK(("c1 strip", k))
for k in range(4):
    SIDE(("a1", k))
for k in range(2):
    SIDE(("a2", k))
for k in range(2):
    LINK(("c1 quad", k)), SIDE(("c1 quad", k))
for k in range(2):
    LINK(("x", k)), SIDE(("far x", k))
for name in ("y", "p"):
    LINK(name), SIDE(name), SIDE("far " + name)
SIDE("c2"), SIDE("c1"), SIDE("x")


def hint(value, multiple):
    return value if isinstance(value, int) else pl.multiple_of(value, multiple)


def span(start, size):
    return pl.ds(hint(start, size), size)


def col(j):
    return slice(j * LANES, (j + 1) * LANES)


def tree(op, parts):
    while len(parts) > 1:
        parts = [op(parts[i], parts[i + 1]) for i in range(0, len(parts), 2)]
    return parts[0]


def store_col_scale(acc, v_ref, q_ref):
    for j in range(COLS):
        col_sum = jnp.sum(acc[j], axis=0, keepdims=True)
        v_ref[:, col(j)] = jnp.broadcast_to(q_ref[:, col(j)] / col_sum, (8, LANES))


def sweeps(count, kern, plan_b, u_b, v_ref, q_ref):
    lead = 128
    group = SWEEP_GROUP
    shape = (group // 8, 8, LANES)

    def sweep(_, carry):
        v = [v_ref[:, col(j)][None] for j in range(COLS)]

        def tile(row, j):
            return kern[row:row + group, col(j)].reshape(shape)

        acc = [jnp.zeros((8, LANES), F32) for _ in range(COLS)]
        for row in range(-lead, N, group):
            top = row + lead
            if top < N:
                total = tree(jnp.add, [tile(top, j) * v[j] for j in range(COLS)])
                u = plan_b[top:top + group, :].reshape(shape) / jnp.sum(total, axis=2, keepdims=True)
                u_b[top:top + group, :] = u.reshape(group, LANES)
            if row >= 0:
                u = u_b[row:row + group, :].reshape(shape)
                acc = [acc[j] + jnp.sum(tile(row, j) * u, axis=0) for j in range(COLS)]
        store_col_scale(acc, v_ref, q_ref)
        return carry

    lax.fori_loop(0, count, sweep, 0)


def scaled_rows(kern, u_b, v_ref, row, count):
    u = u_b[pl.ds(row, count), :].reshape(count // 8, 8, LANES)
    for j in range(COLS):
        k = kern[pl.ds(row, count), col(j)].reshape(count // 8, 8, LANES)
        yield j, (u * k * v_ref[:, col(j)][None]).reshape(count, LANES)


def kernel(c1_hbm, c2_hbm, t0_hbm, p_hbm, q_hbm, x_hbm, y_hbm, eps_ref, out_ref,
           q_ref, t_st, t_all, c1_rows, c1_side, quad_side, c2_all, y_all, x_all, g_all, a1_all, a2_all,
           kern, p_all, p_b, u_b, peak_b, first_b, acc_ref, v_ref,
           load_sem, link_send, link_recv, side_send, side_recv):
    raw0, raw1 = 0, CH
    current = [None]

    def mark(name):
        if current[0] is not None:
            current[0].__exit__(None, None, None)
            current[0] = None
        if name:
            current[0] = jax.named_scope(name)
            current[0].__enter__()

    me = lax.axis_index("rows")
    chip = me // 2
    core = me % 2
    partner = chip * 2 + (1 - core)
    far = (1 - chip) * 2 + core
    far_partner = (1 - chip) * 2 + (1 - core)

    y_st, x_st, c2_st = kern.at[:MB, :D], kern.at[MB:MB + NB, :D], kern.at[MB + NB:2 * MB + NB, :]
    loads = {}
    for i, (name, src, dst) in enumerate((
            ("y", y_hbm, y_st), ("p", p_hbm, p_all.at[me]), ("t", t0_hbm, t_st), ("c2", c2_hbm, c2_st), ("x", x_hbm, x_st),
            ("left", c1_hbm.at[:, :M], g_all.at[:NB]), ("right", c1_hbm.at[:, M:], g_all.at[NB:2 * NB]), ("q", q_hbm, q_ref))):
        loads[name] = pltpu.make_async_copy(src, dst, load_sem.at[i])
        loads[name].start()

    mark("barrier")
    barrier = pltpu.get_barrier_semaphore()
    for peer in (partner, far):
        pl.semaphore_signal(barrier, inc=1, device_id={"rows": peer}, device_id_type=pl.DeviceIdType.MESH)
    pl.semaphore_wait(barrier, 2)

    def to_far(src, dst, name):
        slot = LINK.names[name]
        return pltpu.make_async_remote_copy(
            src_ref=src, dst_ref=dst, send_sem=link_send.at[slot], recv_sem=link_recv.at[slot],
            device_id={"rows": far}, device_id_type=pl.DeviceIdType.MESH)

    def to_partner(src, dst, name):
        slot = SIDE.names[name]
        return pltpu.make_async_remote_copy(
            src_ref=src, dst_ref=dst, send_sem=side_send.at[slot], recv_sem=side_recv.at[slot],
            device_id={"rows": partner}, device_id_type=pl.DeviceIdType.MESH)

    sends = []

    def go(copy):
        copy.start()
        sends.append(copy)

    def far_arrived(ref, name):
        to_far(ref, ref, name).wait_recv()

    def partner_arrived(ref, name):
        to_partner(ref, ref, name).wait_recv()

    def t_rows(owner, k):
        return t_all.at[span(owner * NB + k * TR, TR), :]

    def c2_rows(owner):
        return c2_all.at[span(owner * MB, MB), :]

    def c2_pieces(owner, other, which):
        return (
            c2_all.at[span(owner * MB + 128, 128), span(other * MB, 128)],
            c2_all.at[span(owner * MB + which * 128, 128), span(other * MB + which * 128, 128)],
            c2_all.at[span(owner * MB, 128), span(owner * MB, MB)],
            c2_all.at[span(owner * MB + 128, 128), span(owner * MB + 128, 128)])

    def y_rows(owner):
        return y_all.at[span(owner * MB, MB), :]

    def x_rows(owner):
        return x_all.at[span(owner * NB, NB), :]

    def x_half(owner, k):
        return x_all.at[span(owner * NB + k * CH, CH), :]

    def c1_quads(base, other, which):
        return (c1_rows.at[base + HALF:base + NB, span(other * NB, HALF)],
                c1_rows.at[span(base + which * HALF, HALF), span(other * NB + which * HALF, HALF)])

    def c1_strip(base, owner, k):
        return c1_rows.at[base + k * 128:base + (k + 1) * 128, pl.ds(hint(owner * NB + k * 128, 128), NB - k * 128)]

    mark("cast_y")
    loads["y"].wait()
    y_all[span(me * MB, MB), :] = kern[:MB, :D].astype(BF16)
    loads["p"].wait()
    mark("cast_t")
    loads["t"].wait()
    for k in range(T_CHUNKS):
        t_all[span(me * NB + k * TR, TR), :] = t_st[k * TR:(k + 1) * TR, :].astype(BF16)
    go(to_far(y_rows(me), y_rows(me), "y"))
    go(to_far(p_all.at[me], p_all.at[me], "p"))
    for k in range(T_CHUNKS):
        go(to_far(t_rows(me, k), t_rows(me, k), ("t", k)))
    go(to_partner(y_rows(me), y_rows(me), "y"))
    go(to_partner(p_all.at[me], p_all.at[me], "p"))
    for k in range(T_CHUNKS):
        go(to_partner(t_rows(me, k), t_rows(me, k), ("t", k)))
    mark("cast_rest")
    for name in ("c2", "x", "left", "right", "q"):
        loads[name].wait()
    c2_all[span(me * MB, MB), :] = kern[MB + NB:2 * MB + NB, :].astype(BF16)
    x_all[span(me * NB, NB), :] = kern[MB:MB + NB, :D].astype(BF16)
    c1_rows[:NB, :M] = g_all[:NB, :].astype(BF16)
    c1_rows[:NB, M:] = g_all[NB:2 * NB, :].astype(BF16)
    for k, piece in enumerate(c2_pieces(me, partner, core)):
        go(to_far(piece, piece, ("c2", k)))
    for k, (src, dst) in enumerate(zip(c1_quads(0, partner, core), c1_quads(NB, partner, core))):
        go(to_far(src, dst, ("c1 quad", k)))
    for k in range(4):
        go(to_far(c1_strip(0, me, k), c1_strip(NB, me, k), ("c1 strip", k)))
    for k in range(2):
        go(to_far(x_half(me, k), x_half(me, k), ("x", k)))
    go(to_partner(c2_rows(me), c2_rows(me), "c2"))
    go(to_partner(x_rows(me), x_rows(me), "x"))
    go(to_partner(c1_rows.at[:NB, span(far_partner * NB, NB)], c1_side, "c1"))

    def mirror(src, src_row, src_col, dst, dst_row, dst_col, size):
        for i in range(size // LANES):
            for j in range(size // LANES):
                tile = src[span(src_row + i * LANES, LANES), span(src_col + j * LANES, LANES)]
                dst[span(dst_row + j * LANES, LANES), span(dst_col + i * LANES, LANES)] = (
                    tile.astype(F32).T.astype(BF16))

    mark("mirrors")
    mirror(c1_rows, 0, far * NB, c1_rows, NB, me * NB, NB)
    partner_arrived(c1_side, "c1")
    mirror(c1_side, 0, 0, c1_rows, NB, partner * NB, NB)
    partner_arrived(c2_rows(partner), "c2")
    mirror(c2_all, chip * 2 * MB, (1 - chip) * 2 * MB, c2_all, (1 - chip) * 2 * MB, chip * 2 * MB, 2 * MB)
    partner_arrived(y_rows(partner), "y")
    partner_arrived(p_all.at[partner], "p")
    partner_arrived(x_rows(partner), "x")

    def forward(ref, name):
        far_arrived(ref, name)
        go(to_partner(ref, ref, ("far " + name[0], name[1]) if isinstance(name, tuple) else "far " + name))

    def gram(owner):
        for n in range(4):
            g = lax.dot_general(x_all[span(owner * NB, NB), :], y_all[n * 256:(n + 1) * 256, :],
                                (((1,), (1,)), ((), ())), preferred_element_type=F32)
            g_all[span(owner * NB, NB), n * 256:(n + 1) * 256] = (2.0 * ALPHA) * g

    def grams(first, second):
        def one(i, carry):
            gram(first + i * (second - first))
            return carry
        lax.fori_loop(0, 2, one, 0)

    mark("wait_y")
    forward(y_rows(far), "y")
    forward(p_all.at[far], "p")
    partner_arrived(y_rows(far_partner), "far y")
    partner_arrived(p_all.at[far_partner], "far p")
    mark("p_b_gram")
    for owner in range(4):
        for i in range(NB // LANES):
            block = jnp.broadcast_to(p_all[owner, i:i + 1, :], (LANES, LANES))
            p_b[owner * NB + i * LANES:owner * NB + (i + 1) * LANES, :] = block.T
    grams(me, partner)
    mark("wait_t")
    for k in range(T_CHUNKS):
        partner_arrived(t_rows(partner, k), ("t", k))
    for k in range(T_CHUNKS):
        forward(t_rows(far, k), ("t", k))
    for k in range(T_CHUNKS):
        partner_arrived(t_rows(far_partner, k), ("far t", k))

    scale = LOG2E / eps_ref[0, 0]

    def a_rows(a_all, local, base, rows=CH):
        for n in range(4):
            a_all[span(base, rows), n * 256:(n + 1) * 256] = jnp.dot(
                c1_rows[span(local, rows), :], t_all[:, n * 256:(n + 1) * 256], preferred_element_type=F32).astype(BF16)

    def scores(a_all, base, raw):
        for n in range(4):
            b = jnp.dot(a_all[span(base, CH), :], c2_all[:, n * 256:(n + 1) * 256], preferred_element_type=F32)
            t_st[raw:raw + CH, n * 256:(n + 1) * 256] = g_all[span(base, CH), n * 256:(n + 1) * 256] + (2.0 * (1.0 - ALPHA)) * b

    def products(a_all, base):
        for n in range(4):
            b = jnp.dot(a_all[span(base, CH), :], c2_all[:, n * 256:(n + 1) * 256], preferred_element_type=F32)
            g_all[span(base, CH), n * 256:(n + 1) * 256] = (2.0 * (1.0 - ALPHA)) * b

    def late_scores(base, raw):
        for n in range(4):
            g = (2.0 * ALPHA) * lax.dot_general(x_all[span(base, CH), :], y_all[n * 256:(n + 1) * 256, :],
                                                (((1,), (1,)), ((), ())), preferred_element_type=F32)
            t_st[raw:raw + CH, n * 256:(n + 1) * 256] = g + g_all[span(base, CH), n * 256:(n + 1) * 256]
            g_all[span(base, CH), n * 256:(n + 1) * 256] = g

    def form(base, raw):
        acc = [acc_ref[:, col(j)] for j in range(COLS)]
        lead = 64
        group = FORM_GROUP
        shape = (group // 8, 8, LANES)
        for row in range(-2 * lead, CH, group):
            top = row + 2 * lead
            if top < CH:
                peak = tree(jnp.maximum, [t_st[raw + top:raw + top + group, col(j)] for j in range(COLS)])
                peak_b[top:top + group, :] = jnp.broadcast_to(jnp.max(peak, axis=1, keepdims=True), (group, LANES))
            mid = row + lead
            if 0 <= mid < CH:
                here = pl.ds(hint(base + mid, group), group)
                peak = peak_b[mid:mid + group, :]
                vals = [jnp.exp2((t_st[raw + mid:raw + mid + group, col(j)] - peak) * scale) for j in range(COLS)]
                for j in range(COLS):
                    kern[here, col(j)] = vals[j]
                total = jnp.sum(tree(jnp.add, vals), axis=1, keepdims=True)
                first_b[mid:mid + group, :] = p_b[here, :] / total
            if row >= 0:
                here = pl.ds(hint(base + row, group), group)
                u = first_b[row:row + group, :].reshape(shape)
                acc = [acc[j] + jnp.sum(kern[here, col(j)].reshape(shape) * u, axis=0) for j in range(COLS)]
        for j in range(COLS):
            acc_ref[:, col(j)] = acc[j]

    def b_rows(a_all, bases, ready=None):
        raws = (raw0, raw1)
        for i, base in enumerate(bases):
            if ready and ready[i]:
                ready[i]()
            scores(a_all, base, raws[i % 2])
            if i:
                form(bases[i - 1], raws[(i - 1) % 2])
        form(bases[-1], raws[(len(bases) - 1) % 2])

    def a_slice(a_all, base):
        return a_all.at[span(base, CH), :]

    def my_base(i):
        return jnp.where(i < 2, me * NB + i * CH, far * NB + (i - 2) * CH)

    def their_base(i):
        return jnp.where(i < 2, partner * NB + i * CH, far_partner * NB + (i - 2) * CH)

    mine = [my_base(i) for i in range(4)]
    theirs = [their_base(i) for i in range(4)]

    def share(a_all, name, start, stop):
        slot = SIDE.names[(name, 0)]

        def piece(i):
            ref = a_slice(a_all, my_base(i))
            return pltpu.make_async_remote_copy(
                src_ref=ref, dst_ref=ref, send_sem=side_send.at[slot + i], recv_sem=side_recv.at[slot + i],
                device_id={"rows": partner}, device_id_type=pl.DeviceIdType.MESH)

        def step(i, carry):
            a_rows(a_all, i * CH, my_base(i))
            piece(i).start()
            return carry
        if stop - start == 1:
            step(start, 0)
        else:
            lax.fori_loop(start, stop, step, 0)
        for i in range(start, stop):
            sends.append(piece(i))

    def b_groups(a_all, count, arrived):
        def group(g, carry):
            @pl.when(g == 1)
            def _():
                arrived()
            b_rows(a_all, [jnp.where(g == 0, mine[i], theirs[i]) for i in range(count)])
            return carry
        lax.fori_loop(0, 2, group, 0)

    acc_ref[...] = jnp.zeros_like(acc_ref)
    mark("a_own")
    share(a1_all, "a1", 0, 2)
    mark("wait_c2")
    for k, piece in enumerate(c2_pieces(far, far_partner, core)):
        forward(piece, ("c2", k))
    for k, piece in enumerate(c2_pieces(far_partner, far, 1 - core)):
        partner_arrived(piece, ("far c2", k))
    mark("c2_mirror")
    first = (1 - chip) * 2 * MB
    second = first + MB
    for base in (first, second):
        mirror(c2_all, base, base + 128, c2_all, base + 128, base, 128)
    mirror(c2_all, second + 128, first, c2_all, first, second + 128, 128)
    mirror(c2_all, second + 128, first + 128, c2_all, first + 128, second + 128, 128)
    mirror(c2_all, first, second, c2_all, second, first, 128)
    mirror(c2_all, first + 128, second, c2_all, second, first + 128, 128)
    mark("b_own")

    def a1_arrived():
        for i in range(2):
            partner_arrived(a_slice(a1_all, theirs[i]), ("a1", i))
    b_groups(a1_all, 2, a1_arrived)
    mark("wait_quads")
    for k, piece in enumerate(c1_quads(NB, far_partner, core)):
        far_arrived(piece, ("c1 quad", k))
        go(to_partner(piece, quad_side.at[k * HALF:(k + 1) * HALF, :], ("c1 quad", k)))
    for k in range(2):
        partner_arrived(quad_side.at[k * HALF:(k + 1) * HALF, :], ("c1 quad", k))
    mark("quad_mirror")
    mirror(quad_side, 0, 0, c1_rows, NB, far_partner * NB + HALF, HALF)
    mirror(quad_side, HALF, 0, c1_rows, NB + (1 - core) * HALF, far_partner * NB + (1 - core) * HALF, HALF)
    for i in range(2):
        mark("wait_strips%d" % i)
        for k in (2 * i, 2 * i + 1):
            far_arrived(c1_strip(NB, far, k), ("c1 strip", k))
            for below in range(k + 1, 4):
                mirror(c1_rows, NB + k * 128, far * NB + below * 128, c1_rows, NB + below * 128, far * NB + k * 128, 128)
        mark("a_far%d" % i)
        share(a1_all, "a1", 2 + i, 3 + i)
        mark("products%d" % i)
        products(a1_all, mine[2 + i])
    mark("products_theirs")
    for i in range(2):
        partner_arrived(a_slice(a1_all, theirs[2 + i]), ("a1", 2 + i))
        products(a1_all, theirs[2 + i])
    mark("late")
    bases = [mine[2], theirs[2], mine[3], theirs[3]]
    for i, base in enumerate(bases):
        half = i // 2
        if i % 2 == 0:
            forward(x_half(far, half), ("x", half))
        else:
            partner_arrived(x_half(far_partner, half), ("far x", half))
        late_scores(base, (raw0, raw1)[i % 2])
        form(base, (raw0, raw1)[i % 2])
    store_col_scale([acc_ref[:, col(j)] for j in range(COLS)], v_ref, q_ref)
    mark("sweeps")
    sweeps(SWEEPS - 1, kern, p_b, u_b, v_ref, q_ref)

    mark("next_plan")
    for copy in sends:
        copy.wait_send()
    sends.clear()

    def next_plan(i, carry):
        row = hint(i * 64, 64)
        for j, t in scaled_rows(kern, u_b, v_ref, row, 64):
            t_all[pl.ds(row, 64), col(j)] = t.astype(BF16)
        return carry
    lax.fori_loop(0, N // 64, next_plan, 0)

    acc_ref[...] = jnp.zeros_like(acc_ref)
    mark("a_2")
    first_slot = SIDE.names[("a2", 0)]

    def a2_piece(i):
        ref = a2_all.at[span(jnp.where(i == 0, me, far) * NB, NB), :]
        return pltpu.make_async_remote_copy(
            src_ref=ref, dst_ref=ref, send_sem=side_send.at[first_slot + i], recv_sem=side_recv.at[first_slot + i],
            device_id={"rows": partner}, device_id_type=pl.DeviceIdType.MESH)

    def a2_step(i, carry):
        a_rows(a2_all, i * NB, jnp.where(i == 0, me, far) * NB, NB)
        a2_piece(i).start()
        return carry
    lax.fori_loop(0, 2, a2_step, 0)
    sends.extend((a2_piece(0), a2_piece(1)))
    mark("b_2")

    def a2_arrived():
        for i in range(2):
            a2_piece(i).wait_recv()
    b_groups(a2_all, 4, a2_arrived)
    store_col_scale([acc_ref[:, col(j)] for j in range(COLS)], v_ref, q_ref)
    mark("sweeps")
    sweeps(SWEEPS - 1, kern, p_b, u_b, v_ref, q_ref)

    mark("result")

    def result(i, carry):
        row = hint(i * 64, 64)
        for j, t in scaled_rows(kern, u_b, v_ref, hint(me * NB + row, 64), 64):
            out_ref[pl.ds(row, 64), col(j)] = t
        return carry
    lax.fori_loop(0, NB // 64, result, 0)
    for copy in sends:
        copy.wait_send()
    mark(None)


def solution(mesh):
    vmem = pl.BlockSpec(memory_space=pltpu.VMEM)
    hbm = pl.BlockSpec(memory_space=pl.ANY)
    smem = pl.BlockSpec(memory_space=pltpu.SMEM)

    def local_fgw(cost_src, cost_tgt, plan_init, mass_src, mass_tgt, feat_src, feat_tgt, epsilon):
        return pl.pallas_call(
            kernel,
            out_shape=pltpu.VMEM((NB, M), F32),
            in_specs=[hbm] * 7 + [smem],
            out_specs=vmem,
            scratch_shapes=[
                pltpu.VMEM((1, M), F32),
                pltpu.VMEM((NB, M), F32),
                pltpu.VMEM((N, M), BF16),
                pltpu.VMEM((2 * NB, N), BF16),
                pltpu.VMEM((NB, NB), BF16),
                pltpu.VMEM((2 * HALF, HALF), BF16),
                pltpu.VMEM((M, M), BF16),
                pltpu.VMEM((M, D), BF16),
                pltpu.VMEM((N, D), BF16),
                pltpu.VMEM((N, M), F32),
                pltpu.VMEM((N, M), BF16),
                pltpu.VMEM((N, M), BF16),
                pltpu.VMEM((N, M), F32),
                pltpu.VMEM((4, NB // LANES, LANES), F32),
                pltpu.VMEM((N, LANES), F32),
                pltpu.VMEM((N, LANES), F32),
                pltpu.VMEM((CH, LANES), F32),
                pltpu.VMEM((CH, LANES), F32),
                pltpu.VMEM((8, M), F32),
                pltpu.VMEM((8, M), F32),
                pltpu.SemaphoreType.DMA((8,)),
                pltpu.SemaphoreType.DMA((len(LINK.names),)),
                pltpu.SemaphoreType.DMA((len(LINK.names),)),
                pltpu.SemaphoreType.DMA((len(SIDE.names),)),
                pltpu.SemaphoreType.DMA((len(SIDE.names),)),
            ],
            compiler_params=pltpu.CompilerParams(
                collective_id=0, has_side_effects=True, vmem_limit_bytes=54000 * 1024),
        )(*(pltpu.with_memory_space_constraint(x, pltpu.HBM) for x in (
            cost_src, cost_tgt, plan_init, mass_src.reshape(NB // LANES, LANES), mass_tgt.reshape(1, M),
            feat_src, feat_tgt)), epsilon.reshape(1, 1))

    row_spec = P(('pairs', 'rows'), None)
    vec_spec = P(('pairs', 'rows'))
    in_specs = (row_spec, row_spec, row_spec, vec_spec, P('pairs'), row_spec, row_spec, P())
    return jax.shard_map(local_fgw, mesh=mesh, in_specs=in_specs, out_specs=row_spec, check_vma=False)
```

```python
import jax
import jax.numpy as jnp
from jax import lax
from jax.experimental import pallas as pl
from jax.experimental.pallas import tpu as pltpu
from jax.sharding import PartitionSpec as P

ALPHA = 0.5
OUTER_STEPS = 2
SWEEPS = 10
LOG2E = 1.4426950408889634

N = 2048
M = 1024
D = 256
NB = 512
MB = 256
F32 = jnp.float32
BF16 = jnp.bfloat16
LANES = 128
COLS = M // LANES

T_CHUNKS = 4
TR = NB // T_CHUNKS
CH = 256
HALF = NB // 2
SWEEP_GROUP = 16
FORM_GROUP = 32


class Slots:
    def __init__(self):
        self.names = {}

    def __call__(self, name):
        return self.names.setdefault(name, len(self.names))


LINK = Slots()
SIDE = Slots()
for k in range(T_CHUNKS):
    LINK(("t", k)), SIDE(("t", k)), SIDE(("far t", k))
for k in range(4):
    LINK(("c2", k)), SIDE(("far c2", k)), LINK(("c1 strip", k))
for k in range(4):
    SIDE(("a1", k))
for k in range(2):
    SIDE(("a2", k))
for k in range(2):
    LINK(("c1 quad", k)), SIDE(("c1 quad", k))
for k in range(2):
    LINK(("x", k)), SIDE(("far x", k))
for name in ("y", "p"):
    LINK(name), SIDE(name), SIDE("far " + name)
SIDE("c2"), SIDE("c1"), SIDE("x")


def hint(value, multiple):
    return value if isinstance(value, int) else pl.multiple_of(value, multiple)


def span(start, size):
    return pl.ds(hint(start, size), size)


def col(j):
    return slice(j * LANES, (j + 1) * LANES)


def tree(op, parts):
    while len(parts) > 1:
        parts = [op(parts[i], parts[i + 1]) for i in range(0, len(parts), 2)]
    return parts[0]


def store_col_scale(acc, v_ref, q_ref):
    for j in range(COLS):
        col_sum = jnp.sum(acc[j], axis=0, keepdims=True)
        v_ref[:, col(j)] = jnp.broadcast_to(q_ref[:, col(j)] / col_sum, (8, LANES))


def sweeps(count, kern, plan_b, u_b, v_ref, q_ref):
    lead = 128
    group = SWEEP_GROUP
    shape = (group // 8, 8, LANES)

    def sweep(_, carry):
        v = [v_ref[:, col(j)][None] for j in range(COLS)]

        def tile(row, j):
            return kern[row:row + group, col(j)].reshape(shape)

        acc = [jnp.zeros((8, LANES), F32) for _ in range(COLS)]
        for row in range(-lead, N, group):
            top = row + lead
            if top < N:
                total = tree(jnp.add, [tile(top, j) * v[j] for j in range(COLS)])
                u = plan_b[top:top + group, :].reshape(shape) / jnp.sum(total, axis=2, keepdims=True)
                u_b[top:top + group, :] = u.reshape(group, LANES)
            if row >= 0:
                u = u_b[row:row + group, :].reshape(shape)
                acc = [acc[j] + jnp.sum(tile(row, j) * u, axis=0) for j in range(COLS)]
        store_col_scale(acc, v_ref, q_ref)
        return carry

    lax.fori_loop(0, count, sweep, 0)


def scaled_rows(kern, u_b, v_ref, row, count):
    u = u_b[pl.ds(row, count), :].reshape(count // 8, 8, LANES)
    for j in range(COLS):
        k = kern[pl.ds(row, count), col(j)].reshape(count // 8, 8, LANES)
        yield j, (u * k * v_ref[:, col(j)][None]).reshape(count, LANES)


def kernel(c1_hbm, c2_hbm, t0_hbm, p_hbm, q_hbm, x_hbm, y_hbm, eps_ref, out_ref,
           q_ref, t_st, t_all, c1_rows, c1_side, quad_side, c2_all, y_all, x_all, g_all, a1_all, a2_all,
           kern, p_all, p_b, u_b, peak_b, first_b, acc_ref, v_ref,
           load_sem, link_send, link_recv, side_send, side_recv):
    raw0, raw1 = 0, CH
    current = [None]

    def mark(name):
        if current[0] is not None:
            current[0].__exit__(None, None, None)
            current[0] = None
        if name:
            current[0] = jax.named_scope(name)
            current[0].__enter__()

    me = lax.axis_index("rows")
    chip = me // 2
    core = me % 2
    partner = chip * 2 + (1 - core)
    far = (1 - chip) * 2 + core
    far_partner = (1 - chip) * 2 + (1 - core)

    y_st, x_st, c2_st = kern.at[:MB, :D], kern.at[MB:MB + NB, :D], kern.at[MB + NB:2 * MB + NB, :]
    loads = {}
    for i, (name, src, dst) in enumerate((
            ("y", y_hbm, y_st), ("p", p_hbm, p_all.at[me]), ("t", t0_hbm, t_st), ("c2", c2_hbm, c2_st), ("x", x_hbm, x_st),
            ("left", c1_hbm.at[:, :M], g_all.at[:NB]), ("right", c1_hbm.at[:, M:], g_all.at[NB:2 * NB]), ("q", q_hbm, q_ref))):
        loads[name] = pltpu.make_async_copy(src, dst, load_sem.at[i])
        loads[name].start()

    mark("barrier")
    barrier = pltpu.get_barrier_semaphore()
    for peer in (partner, far):
        pl.semaphore_signal(barrier, inc=1, device_id={"rows": peer}, device_id_type=pl.DeviceIdType.MESH)
    pl.semaphore_wait(barrier, 2)

    def to_far(src, dst, name):
        slot = LINK.names[name]
        return pltpu.make_async_remote_copy(
            src_ref=src, dst_ref=dst, send_sem=link_send.at[slot], recv_sem=link_recv.at[slot],
            device_id={"rows": far}, device_id_type=pl.DeviceIdType.MESH)

    def to_partner(src, dst, name):
        slot = SIDE.names[name]
        return pltpu.make_async_remote_copy(
            src_ref=src, dst_ref=dst, send_sem=side_send.at[slot], recv_sem=side_recv.at[slot],
            device_id={"rows": partner}, device_id_type=pl.DeviceIdType.MESH)

    sends = []

    def go(copy):
        copy.start()
        sends.append(copy)

    def far_arrived(ref, name):
        to_far(ref, ref, name).wait_recv()

    def partner_arrived(ref, name):
        to_partner(ref, ref, name).wait_recv()

    def t_rows(owner, k):
        return t_all.at[span(owner * NB + k * TR, TR), :]

    def c2_rows(owner):
        return c2_all.at[span(owner * MB, MB), :]

    def c2_pieces(owner, other, which):
        return (
            c2_all.at[span(owner * MB + 128, 128), span(other * MB, 128)],
            c2_all.at[span(owner * MB + which * 128, 128), span(other * MB + which * 128, 128)],
            c2_all.at[span(owner * MB, 128), span(owner * MB, MB)],
            c2_all.at[span(owner * MB + 128, 128), span(owner * MB + 128, 128)])

    def y_rows(owner):
        return y_all.at[span(owner * MB, MB), :]

    def x_rows(owner):
        return x_all.at[span(owner * NB, NB), :]

    def x_half(owner, k):
        return x_all.at[span(owner * NB + k * CH, CH), :]

    def c1_quads(base, other, which):
        return (c1_rows.at[base + HALF:base + NB, span(other * NB, HALF)],
                c1_rows.at[span(base + which * HALF, HALF), span(other * NB + which * HALF, HALF)])

    def c1_strip(base, owner, k):
        return c1_rows.at[base + k * 128:base + (k + 1) * 128, pl.ds(hint(owner * NB + k * 128, 128), NB - k * 128)]

    mark("cast_y")
    loads["y"].wait()
    y_all[span(me * MB, MB), :] = kern[:MB, :D].astype(BF16)
    loads["p"].wait()
    mark("cast_t")
    loads["t"].wait()
    for k in range(T_CHUNKS):
        t_all[span(me * NB + k * TR, TR), :] = t_st[k * TR:(k + 1) * TR, :].astype(BF16)
    go(to_far(y_rows(me), y_rows(me), "y"))
    go(to_far(p_all.at[me], p_all.at[me], "p"))
    for k in range(T_CHUNKS):
        go(to_far(t_rows(me, k), t_rows(me, k), ("t", k)))
    go(to_partner(y_rows(me), y_rows(me), "y"))
    go(to_partner(p_all.at[me], p_all.at[me], "p"))
    for k in range(T_CHUNKS):
        go(to_partner(t_rows(me, k), t_rows(me, k), ("t", k)))
    mark("cast_rest")
    for name in ("c2", "x", "left", "right", "q"):
        loads[name].wait()
    c2_all[span(me * MB, MB), :] = kern[MB + NB:2 * MB + NB, :].astype(BF16)
    x_all[span(me * NB, NB), :] = kern[MB:MB + NB, :D].astype(BF16)
    c1_rows[:NB, :M] = g_all[:NB, :].astype(BF16)
    c1_rows[:NB, M:] = g_all[NB:2 * NB, :].astype(BF16)
    for k, piece in enumerate(c2_pieces(me, partner, core)):
        go(to_far(piece, piece, ("c2", k)))
    for k, (src, dst) in enumerate(zip(c1_quads(0, partner, core), c1_quads(NB, partner, core))):
        go(to_far(src, dst, ("c1 quad", k)))
    for k in range(4):
        go(to_far(c1_strip(0, me, k), c1_strip(NB, me, k), ("c1 strip", k)))
    for k in range(2):
        go(to_far(x_half(me, k), x_half(me, k), ("x", k)))
    go(to_partner(c2_rows(me), c2_rows(me), "c2"))
    go(to_partner(x_rows(me), x_rows(me), "x"))
    go(to_partner(c1_rows.at[:NB, span(far_partner * NB, NB)], c1_side, "c1"))

    def mirror(src, src_row, src_col, dst, dst_row, dst_col, size):
        for i in range(size // LANES):
            for j in range(size // LANES):
                tile = src[span(src_row + i * LANES, LANES), span(src_col + j * LANES, LANES)]
                dst[span(dst_row + j * LANES, LANES), span(dst_col + i * LANES, LANES)] = (
                    tile.astype(F32).T.astype(BF16))

    mark("mirrors")
    mirror(c1_rows, 0, far * NB, c1_rows, NB, me * NB, NB)
    partner_arrived(c1_side, "c1")
    mirror(c1_side, 0, 0, c1_rows, NB, partner * NB, NB)
    partner_arrived(c2_rows(partner), "c2")
    mirror(c2_all, chip * 2 * MB, (1 - chip) * 2 * MB, c2_all, (1 - chip) * 2 * MB, chip * 2 * MB, 2 * MB)
    partner_arrived(y_rows(partner), "y")
    partner_arrived(p_all.at[partner], "p")
    partner_arrived(x_rows(partner), "x")

    def forward(ref, name):
        far_arrived(ref, name)
        go(to_partner(ref, ref, ("far " + name[0], name[1]) if isinstance(name, tuple) else "far " + name))

    def gram(owner):
        for n in range(4):
            g = lax.dot_general(x_all[span(owner * NB, NB), :], y_all[n * 256:(n + 1) * 256, :],
                                (((1,), (1,)), ((), ())), preferred_element_type=F32)
            g_all[span(owner * NB, NB), n * 256:(n + 1) * 256] = (2.0 * ALPHA) * g

    def grams(first, second):
        def one(i, carry):
            gram(first + i * (second - first))
            return carry
        lax.fori_loop(0, 2, one, 0)

    mark("wait_y")
    forward(y_rows(far), "y")
    forward(p_all.at[far], "p")
    partner_arrived(y_rows(far_partner), "far y")
    partner_arrived(p_all.at[far_partner], "far p")
    mark("p_b_gram")
    for owner in range(4):
        for i in range(NB // LANES):
            block = jnp.broadcast_to(p_all[owner, i:i + 1, :], (LANES, LANES))
            p_b[owner * NB + i * LANES:owner * NB + (i + 1) * LANES, :] = block.T
    grams(me, partner)
    mark("wait_t")
    for k in range(T_CHUNKS):
        partner_arrived(t_rows(partner, k), ("t", k))
    for k in range(T_CHUNKS):
        forward(t_rows(far, k), ("t", k))
    for k in range(T_CHUNKS):
        partner_arrived(t_rows(far_partner, k), ("far t", k))

    scale = LOG2E / eps_ref[0, 0]

    def a_rows(a_all, local, base, rows=CH):
        for n in range(4):
            a_all[span(base, rows), n * 256:(n + 1) * 256] = jnp.dot(
                c1_rows[span(local, rows), :], t_all[:, n * 256:(n + 1) * 256], preferred_element_type=F32).astype(BF16)

    def scores(a_all, base, raw):
        for n in range(4):
            b = jnp.dot(a_all[span(base, CH), :], c2_all[:, n * 256:(n + 1) * 256], preferred_element_type=F32)
            t_st[raw:raw + CH, n * 256:(n + 1) * 256] = g_all[span(base, CH), n * 256:(n + 1) * 256] + (2.0 * (1.0 - ALPHA)) * b

    def products(a_all, base):
        for n in range(4):
            b = jnp.dot(a_all[span(base, CH), :], c2_all[:, n * 256:(n + 1) * 256], preferred_element_type=F32)
            g_all[span(base, CH), n * 256:(n + 1) * 256] = (2.0 * (1.0 - ALPHA)) * b

    def late_scores(base, raw):
        for n in range(4):
            g = (2.0 * ALPHA) * lax.dot_general(x_all[span(base, CH), :], y_all[n * 256:(n + 1) * 256, :],
                                                (((1,), (1,)), ((), ())), preferred_element_type=F32)
            t_st[raw:raw + CH, n * 256:(n + 1) * 256] = g + g_all[span(base, CH), n * 256:(n + 1) * 256]
            g_all[span(base, CH), n * 256:(n + 1) * 256] = g

    def form(base, raw):
        acc = [acc_ref[:, col(j)] for j in range(COLS)]
        lead = 64
        group = FORM_GROUP
        shape = (group // 8, 8, LANES)
        for row in range(-2 * lead, CH, group):
            top = row + 2 * lead
            if top < CH:
                peak = tree(jnp.maximum, [t_st[raw + top:raw + top + group, col(j)] for j in range(COLS)])
                peak_b[top:top + group, :] = jnp.broadcast_to(jnp.max(peak, axis=1, keepdims=True), (group, LANES))
            mid = row + lead
            if 0 <= mid < CH:
                here = pl.ds(hint(base + mid, group), group)
                peak = peak_b[mid:mid + group, :]
                vals = [jnp.exp2((t_st[raw + mid:raw + mid + group, col(j)] - peak) * scale) for j in range(COLS)]
                for j in range(COLS):
                    kern[here, col(j)] = vals[j]
                total = jnp.sum(tree(jnp.add, vals), axis=1, keepdims=True)
                first_b[mid:mid + group, :] = p_b[here, :] / total
            if row >= 0:
                here = pl.ds(hint(base + row, group), group)
                u = first_b[row:row + group, :].reshape(shape)
                acc = [acc[j] + jnp.sum(kern[here, col(j)].reshape(shape) * u, axis=0) for j in range(COLS)]
        for j in range(COLS):
            acc_ref[:, col(j)] = acc[j]

    def b_rows(a_all, bases, ready=None):
        raws = (raw0, raw1)
        for i, base in enumerate(bases):
            if ready and ready[i]:
                ready[i]()
            scores(a_all, base, raws[i % 2])
            if i:
                form(bases[i - 1], raws[(i - 1) % 2])
        form(bases[-1], raws[(len(bases) - 1) % 2])

    def a_slice(a_all, base):
        return a_all.at[span(base, CH), :]

    def my_base(i):
        return jnp.where(i < 2, me * NB + i * CH, far * NB + (i - 2) * CH)

    def their_base(i):
        return jnp.where(i < 2, partner * NB + i * CH, far_partner * NB + (i - 2) * CH)

    mine = [my_base(i) for i in range(4)]
    theirs = [their_base(i) for i in range(4)]

    def share(a_all, name, start, stop):
        slot = SIDE.names[(name, 0)]

        def piece(i):
            ref = a_slice(a_all, my_base(i))
            return pltpu.make_async_remote_copy(
                src_ref=ref, dst_ref=ref, send_sem=side_send.at[slot + i], recv_sem=side_recv.at[slot + i],
                device_id={"rows": partner}, device_id_type=pl.DeviceIdType.MESH)

        def step(i, carry):
            a_rows(a_all, i * CH, my_base(i))
            piece(i).start()
            return carry
        if stop - start == 1:
            step(start, 0)
        else:
            lax.fori_loop(start, stop, step, 0)
        for i in range(start, stop):
            sends.append(piece(i))

    def b_groups(a_all, count, arrived):
        def group(g, carry):
            @pl.when(g == 1)
            def _():
                arrived()
            b_rows(a_all, [jnp.where(g == 0, mine[i], theirs[i]) for i in range(count)])
            return carry
        lax.fori_loop(0, 2, group, 0)

    acc_ref[...] = jnp.zeros_like(acc_ref)
    mark("a_own")
    share(a1_all, "a1", 0, 2)
    mark("wait_c2")
    for k, piece in enumerate(c2_pieces(far, far_partner, core)):
        forward(piece, ("c2", k))
    for k, piece in enumerate(c2_pieces(far_partner, far, 1 - core)):
        partner_arrived(piece, ("far c2", k))
    mark("c2_mirror")
    first = (1 - chip) * 2 * MB
    second = first + MB
    for base in (first, second):
        mirror(c2_all, base, base + 128, c2_all, base + 128, base, 128)
    mirror(c2_all, second + 128, first, c2_all, first, second + 128, 128)
    mirror(c2_all, second + 128, first + 128, c2_all, first + 128, second + 128, 128)
    mirror(c2_all, first, second, c2_all, second, first, 128)
    mirror(c2_all, first + 128, second, c2_all, second, first + 128, 128)
    mark("b_own")

    def a1_arrived():
        for i in range(2):
            partner_arrived(a_slice(a1_all, theirs[i]), ("a1", i))
    b_groups(a1_all, 2, a1_arrived)
    mark("wait_quads")
    for k, piece in enumerate(c1_quads(NB, far_partner, core)):
        far_arrived(piece, ("c1 quad", k))
        go(to_partner(piece, quad_side.at[k * HALF:(k + 1) * HALF, :], ("c1 quad", k)))
    for k in range(2):
        partner_arrived(quad_side.at[k * HALF:(k + 1) * HALF, :], ("c1 quad", k))
    mark("quad_mirror")
    mirror(quad_side, 0, 0, c1_rows, NB, far_partner * NB + HALF, HALF)
    mirror(quad_side, HALF, 0, c1_rows, NB + (1 - core) * HALF, far_partner * NB + (1 - core) * HALF, HALF)
    mark("a_early")

    def a_early(i, carry):
        rows = span(NB + i * CH, CH)
        for n in range(4):
            cols = slice(n * 256, (n + 1) * 256)
            kern[span(far * NB + i * CH, CH), cols] = (
                jnp.dot(c1_rows[rows, span(chip * 2 * NB, 2 * NB)], t_all[span(chip * 2 * NB, 2 * NB), cols],
                        preferred_element_type=F32)
                + jnp.dot(c1_rows[rows, span(far_partner * NB, NB)], t_all[span(far_partner * NB, NB), cols],
                          preferred_element_type=F32))
        return carry
    lax.fori_loop(0, 2, a_early, 0)

    def a_late(i):
        base = mine[2 + i]
        for n in range(4):
            cols = slice(n * 256, (n + 1) * 256)
            a1_all[span(base, CH), cols] = (
                kern[span(base, CH), cols]
                + jnp.dot(c1_rows[NB + i * CH:NB + (i + 1) * CH, span(far * NB, NB)], t_all[span(far * NB, NB), cols],
                          preferred_element_type=F32)).astype(BF16)
        go(to_partner(a_slice(a1_all, base), a_slice(a1_all, base), ("a1", 2 + i)))

    for i in range(2):
        mark("wait_strips%d" % i)
        for k in (2 * i, 2 * i + 1):
            far_arrived(c1_strip(NB, far, k), ("c1 strip", k))
            for below in range(k + 1, 4):
                mirror(c1_rows, NB + k * 128, far * NB + below * 128, c1_rows, NB + below * 128, far * NB + k * 128, 128)
        mark("a_far%d" % i)
        a_late(i)
        mark("products%d" % i)
        products(a1_all, mine[2 + i])
    mark("products_theirs")
    for i in range(2):
        partner_arrived(a_slice(a1_all, theirs[2 + i]), ("a1", 2 + i))
        products(a1_all, theirs[2 + i])
    mark("late")
    for half in range(2):
        forward(x_half(far, half), ("x", half))
        partner_arrived(x_half(far_partner, half), ("far x", half))
        late_scores(mine[2 + half], raw0)
        late_scores(theirs[2 + half], raw1)
        form(mine[2 + half], raw0)
        form(theirs[2 + half], raw1)
    store_col_scale([acc_ref[:, col(j)] for j in range(COLS)], v_ref, q_ref)
    mark("sweeps")
    sweeps(SWEEPS - 1, kern, p_b, u_b, v_ref, q_ref)

    mark("next_plan")
    for copy in sends:
        copy.wait_send()
    sends.clear()

    def next_plan(i, carry):
        row = hint(i * 64, 64)
        for j, t in scaled_rows(kern, u_b, v_ref, row, 64):
            t_all[pl.ds(row, 64), col(j)] = t.astype(BF16)
        return carry
    lax.fori_loop(0, N // 64, next_plan, 0)

    acc_ref[...] = jnp.zeros_like(acc_ref)
    mark("a_2")
    first_slot = SIDE.names[("a2", 0)]

    def a2_piece(i):
        ref = a2_all.at[span(jnp.where(i == 0, me, far) * NB, NB), :]
        return pltpu.make_async_remote_copy(
            src_ref=ref, dst_ref=ref, send_sem=side_send.at[first_slot + i], recv_sem=side_recv.at[first_slot + i],
            device_id={"rows": partner}, device_id_type=pl.DeviceIdType.MESH)

    def a2_step(i, carry):
        a_rows(a2_all, i * NB, jnp.where(i == 0, me, far) * NB, NB)
        a2_piece(i).start()
        return carry
    lax.fori_loop(0, 2, a2_step, 0)
    sends.extend((a2_piece(0), a2_piece(1)))
    mark("b_2")

    def a2_arrived():
        for i in range(2):
            a2_piece(i).wait_recv()
    b_groups(a2_all, 4, a2_arrived)
    store_col_scale([acc_ref[:, col(j)] for j in range(COLS)], v_ref, q_ref)
    mark("sweeps")
    sweeps(SWEEPS - 1, kern, p_b, u_b, v_ref, q_ref)

    mark("result")

    def result(i, carry):
        row = hint(i * 64, 64)
        for j, t in scaled_rows(kern, u_b, v_ref, hint(me * NB + row, 64), 64):
            out_ref[pl.ds(row, 64), col(j)] = t
        return carry
    lax.fori_loop(0, NB // 64, result, 0)
    for copy in sends:
        copy.wait_send()
    mark(None)


def solution(mesh):
    vmem = pl.BlockSpec(memory_space=pltpu.VMEM)
    hbm = pl.BlockSpec(memory_space=pl.ANY)
    smem = pl.BlockSpec(memory_space=pltpu.SMEM)

    def local_fgw(cost_src, cost_tgt, plan_init, mass_src, mass_tgt, feat_src, feat_tgt, epsilon):
        return pl.pallas_call(
            kernel,
            out_shape=pltpu.VMEM((NB, M), F32),
            in_specs=[hbm] * 7 + [smem],
            out_specs=vmem,
            scratch_shapes=[
                pltpu.VMEM((1, M), F32),
                pltpu.VMEM((NB, M), F32),
                pltpu.VMEM((N, M), BF16),
                pltpu.VMEM((2 * NB, N), BF16),
                pltpu.VMEM((NB, NB), BF16),
                pltpu.VMEM((2 * HALF, HALF), BF16),
                pltpu.VMEM((M, M), BF16),
                pltpu.VMEM((M, D), BF16),
                pltpu.VMEM((N, D), BF16),
                pltpu.VMEM((N, M), F32),
                pltpu.VMEM((N, M), BF16),
                pltpu.VMEM((N, M), BF16),
                pltpu.VMEM((N, M), F32),
                pltpu.VMEM((4, NB // LANES, LANES), F32),
                pltpu.VMEM((N, LANES), F32),
                pltpu.VMEM((N, LANES), F32),
                pltpu.VMEM((CH, LANES), F32),
                pltpu.VMEM((CH, LANES), F32),
                pltpu.VMEM((8, M), F32),
                pltpu.VMEM((8, M), F32),
                pltpu.SemaphoreType.DMA((8,)),
                pltpu.SemaphoreType.DMA((len(LINK.names),)),
                pltpu.SemaphoreType.DMA((len(LINK.names),)),
                pltpu.SemaphoreType.DMA((len(SIDE.names),)),
                pltpu.SemaphoreType.DMA((len(SIDE.names),)),
            ],
            compiler_params=pltpu.CompilerParams(
                collective_id=0, has_side_effects=True, vmem_limit_bytes=54000 * 1024),
        )(*(pltpu.with_memory_space_constraint(x, pltpu.HBM) for x in (
            cost_src, cost_tgt, plan_init, mass_src.reshape(NB // LANES, LANES), mass_tgt.reshape(1, M),
            feat_src, feat_tgt)), epsilon.reshape(1, 1))

    row_spec = P(('pairs', 'rows'), None)
    vec_spec = P(('pairs', 'rows'))
    in_specs = (row_spec, row_spec, row_spec, vec_spec, P('pairs'), row_spec, row_spec, P())
    return jax.shard_map(local_fgw, mesh=mesh, in_specs=in_specs, out_specs=row_spec, check_vma=False)
```

```python
import jax
import jax.numpy as jnp
from jax import lax
from jax.experimental import pallas as pl
from jax.experimental.pallas import tpu as pltpu
from jax.sharding import PartitionSpec as P

ALPHA = 0.5
OUTER_STEPS = 2
SWEEPS = 10
LOG2E = 1.4426950408889634

N = 2048
M = 1024
D = 256
NB = 512
MB = 256
F32 = jnp.float32
BF16 = jnp.bfloat16
LANES = 128
COLS = M // LANES

T_CHUNKS = 4
TR = NB // T_CHUNKS
CH = 256
HALF = NB // 2
SWEEP_GROUP = 16
FORM_GROUP = 32


class Slots:
    def __init__(self):
        self.names = {}

    def __call__(self, name):
        return self.names.setdefault(name, len(self.names))


LINK = Slots()
SIDE = Slots()
for k in range(T_CHUNKS):
    LINK(("t", k)), SIDE(("t", k)), SIDE(("far t", k))
for k in range(4):
    LINK(("c2", k)), SIDE(("far c2", k)), LINK(("c1 strip", k))
for k in range(4):
    SIDE(("a1", k))
for k in range(2):
    SIDE(("a2", k))
for k in range(2):
    LINK(("c1 quad", k)), SIDE(("c1 quad", k))
X_PIECES = ((0, 256), (256, 128), (384, 128))
for k in range(len(X_PIECES)):
    LINK(("x", k)), SIDE(("far x", k))
for name in ("y", "p"):
    LINK(name), SIDE(name), SIDE("far " + name)
SIDE("c2"), SIDE("c1"), SIDE("x")


def hint(value, multiple):
    return value if isinstance(value, int) else pl.multiple_of(value, multiple)


def span(start, size):
    return pl.ds(hint(start, size), size)


def col(j):
    return slice(j * LANES, (j + 1) * LANES)


def tree(op, parts):
    while len(parts) > 1:
        parts = [op(parts[i], parts[i + 1]) for i in range(0, len(parts), 2)]
    return parts[0]


def store_col_scale(acc, v_ref, q_ref):
    for j in range(COLS):
        col_sum = jnp.sum(acc[j], axis=0, keepdims=True)
        v_ref[:, col(j)] = jnp.broadcast_to(q_ref[:, col(j)] / col_sum, (8, LANES))


def sweeps(count, kern, plan_b, u_b, v_ref, q_ref):
    lead = 128
    group = SWEEP_GROUP
    shape = (group // 8, 8, LANES)

    def sweep(_, carry):
        v = [v_ref[:, col(j)][None] for j in range(COLS)]

        def tile(row, j):
            return kern[row:row + group, col(j)].reshape(shape)

        acc = [jnp.zeros((8, LANES), F32) for _ in range(COLS)]
        for row in range(-lead, N, group):
            top = row + lead
            if top < N:
                total = tree(jnp.add, [tile(top, j) * v[j] for j in range(COLS)])
                u = plan_b[top:top + group, :].reshape(shape) / jnp.sum(total, axis=2, keepdims=True)
                u_b[top:top + group, :] = u.reshape(group, LANES)
            if row >= 0:
                u = u_b[row:row + group, :].reshape(shape)
                acc = [acc[j] + jnp.sum(tile(row, j) * u, axis=0) for j in range(COLS)]
        store_col_scale(acc, v_ref, q_ref)
        return carry

    lax.fori_loop(0, count, sweep, 0)


def scaled_rows(kern, u_b, v_ref, row, count):
    u = u_b[pl.ds(row, count), :].reshape(count // 8, 8, LANES)
    for j in range(COLS):
        k = kern[pl.ds(row, count), col(j)].reshape(count // 8, 8, LANES)
        yield j, (u * k * v_ref[:, col(j)][None]).reshape(count, LANES)


def kernel(c1_hbm, c2_hbm, t0_hbm, p_hbm, q_hbm, x_hbm, y_hbm, eps_ref, out_ref,
           q_ref, t_st, t_all, c1_rows, c1_side, quad_side, c2_all, y_all, x_all, g_all, a1_all, a2_all,
           kern, p_all, p_b, u_b, peak_b, first_b, acc_ref, v_ref,
           load_sem, link_send, link_recv, side_send, side_recv):
    raw0, raw1 = 0, CH
    current = [None]

    def mark(name):
        if current[0] is not None:
            current[0].__exit__(None, None, None)
            current[0] = None
        if name:
            current[0] = jax.named_scope(name)
            current[0].__enter__()

    me = lax.axis_index("rows")
    chip = me // 2
    core = me % 2
    partner = chip * 2 + (1 - core)
    far = (1 - chip) * 2 + core
    far_partner = (1 - chip) * 2 + (1 - core)

    y_st, x_st, c2_st = kern.at[:MB, :D], kern.at[MB:MB + NB, :D], kern.at[MB + NB:2 * MB + NB, :]
    loads = {}
    for i, (name, src, dst) in enumerate((
            ("y", y_hbm, y_st), ("p", p_hbm, p_all.at[me]), ("t", t0_hbm, t_st), ("c2", c2_hbm, c2_st), ("x", x_hbm, x_st),
            ("left", c1_hbm.at[:, :M], g_all.at[:NB]), ("right", c1_hbm.at[:, M:], g_all.at[NB:2 * NB]), ("q", q_hbm, q_ref))):
        loads[name] = pltpu.make_async_copy(src, dst, load_sem.at[i])
        loads[name].start()

    mark("barrier")
    barrier = pltpu.get_barrier_semaphore()
    for peer in (partner, far):
        pl.semaphore_signal(barrier, inc=1, device_id={"rows": peer}, device_id_type=pl.DeviceIdType.MESH)
    pl.semaphore_wait(barrier, 2)

    def to_far(src, dst, name):
        slot = LINK.names[name]
        return pltpu.make_async_remote_copy(
            src_ref=src, dst_ref=dst, send_sem=link_send.at[slot], recv_sem=link_recv.at[slot],
            device_id={"rows": far}, device_id_type=pl.DeviceIdType.MESH)

    def to_partner(src, dst, name):
        slot = SIDE.names[name]
        return pltpu.make_async_remote_copy(
            src_ref=src, dst_ref=dst, send_sem=side_send.at[slot], recv_sem=side_recv.at[slot],
            device_id={"rows": partner}, device_id_type=pl.DeviceIdType.MESH)

    sends = []

    def go(copy):
        copy.start()
        sends.append(copy)

    def far_arrived(ref, name):
        to_far(ref, ref, name).wait_recv()

    def partner_arrived(ref, name):
        to_partner(ref, ref, name).wait_recv()

    def t_rows(owner, k):
        return t_all.at[span(owner * NB + k * TR, TR), :]

    def c2_rows(owner):
        return c2_all.at[span(owner * MB, MB), :]

    def c2_pieces(owner, other, which):
        return (
            c2_all.at[span(owner * MB + 128, 128), span(other * MB, 128)],
            c2_all.at[span(owner * MB + which * 128, 128), span(other * MB + which * 128, 128)],
            c2_all.at[span(owner * MB, 128), span(owner * MB, MB)],
            c2_all.at[span(owner * MB + 128, 128), span(owner * MB + 128, 128)])

    def y_rows(owner):
        return y_all.at[span(owner * MB, MB), :]

    def x_rows(owner):
        return x_all.at[span(owner * NB, NB), :]

    def x_piece(owner, k):
        return x_all.at[span(owner * NB + X_PIECES[k][0], X_PIECES[k][1]), :]

    def c1_quads(base, other, which):
        return (c1_rows.at[base + HALF:base + NB, span(other * NB, HALF)],
                c1_rows.at[span(base + which * HALF, HALF), span(other * NB + which * HALF, HALF)])

    def c1_strip(base, owner, k):
        return c1_rows.at[base + k * 128:base + (k + 1) * 128, pl.ds(hint(owner * NB + k * 128, 128), NB - k * 128)]

    mark("cast_y")
    loads["y"].wait()
    y_all[span(me * MB, MB), :] = kern[:MB, :D].astype(BF16)
    loads["p"].wait()
    go(to_far(p_all.at[me], p_all.at[me], "p"))
    go(to_partner(p_all.at[me], p_all.at[me], "p"))
    go(to_far(y_rows(me), y_rows(me), "y"))
    go(to_partner(y_rows(me), y_rows(me), "y"))
    mark("cast_t")
    loads["t"].wait()
    for k in range(T_CHUNKS):
        t_all[span(me * NB + k * TR, TR), :] = t_st[k * TR:(k + 1) * TR, :].astype(BF16)
    for k in range(T_CHUNKS):
        go(to_far(t_rows(me, k), t_rows(me, k), ("t", k)))
    for k in range(T_CHUNKS):
        go(to_partner(t_rows(me, k), t_rows(me, k), ("t", k)))
    mark("cast_rest")
    for name in ("c2", "x", "left", "right", "q"):
        loads[name].wait()
    c2_all[span(me * MB, MB), :] = kern[MB + NB:2 * MB + NB, :].astype(BF16)
    x_all[span(me * NB, NB), :] = kern[MB:MB + NB, :D].astype(BF16)
    c1_rows[:NB, :M] = g_all[:NB, :].astype(BF16)
    c1_rows[:NB, M:] = g_all[NB:2 * NB, :].astype(BF16)
    for k, piece in enumerate(c2_pieces(me, partner, core)):
        go(to_far(piece, piece, ("c2", k)))
    for k, (src, dst) in enumerate(zip(c1_quads(0, partner, core), c1_quads(NB, partner, core))):
        go(to_far(src, dst, ("c1 quad", k)))
    for k in range(4):
        go(to_far(c1_strip(0, me, k), c1_strip(NB, me, k), ("c1 strip", k)))
    for k in range(len(X_PIECES)):
        go(to_far(x_piece(me, k), x_piece(me, k), ("x", k)))
    go(to_partner(c2_rows(me), c2_rows(me), "c2"))
    go(to_partner(x_rows(me), x_rows(me), "x"))
    go(to_partner(c1_rows.at[:NB, span(far_partner * NB, NB)], c1_side, "c1"))

    def mirror(src, src_row, src_col, dst, dst_row, dst_col, size):
        for i in range(size // LANES):
            for j in range(size // LANES):
                tile = src[span(src_row + i * LANES, LANES), span(src_col + j * LANES, LANES)]
                dst[span(dst_row + j * LANES, LANES), span(dst_col + i * LANES, LANES)] = (
                    tile.astype(F32).T.astype(BF16))

    mark("mirrors")
    mirror(c1_rows, 0, far * NB, c1_rows, NB, me * NB, NB)
    partner_arrived(c1_side, "c1")
    mirror(c1_side, 0, 0, c1_rows, NB, partner * NB, NB)
    partner_arrived(c2_rows(partner), "c2")
    mirror(c2_all, chip * 2 * MB, (1 - chip) * 2 * MB, c2_all, (1 - chip) * 2 * MB, chip * 2 * MB, 2 * MB)
    partner_arrived(y_rows(partner), "y")
    partner_arrived(p_all.at[partner], "p")
    partner_arrived(x_rows(partner), "x")

    def forward(ref, name):
        far_arrived(ref, name)
        go(to_partner(ref, ref, ("far " + name[0], name[1]) if isinstance(name, tuple) else "far " + name))

    def gram(owner):
        for n in range(4):
            g = lax.dot_general(x_all[span(owner * NB, NB), :], y_all[n * 256:(n + 1) * 256, :],
                                (((1,), (1,)), ((), ())), preferred_element_type=F32)
            g_all[span(owner * NB, NB), n * 256:(n + 1) * 256] = (2.0 * ALPHA) * g

    def grams(first, second):
        def one(i, carry):
            gram(first + i * (second - first))
            return carry
        lax.fori_loop(0, 2, one, 0)

    mark("wait_y")
    forward(y_rows(far), "y")
    forward(p_all.at[far], "p")
    partner_arrived(y_rows(far_partner), "far y")
    partner_arrived(p_all.at[far_partner], "far p")
    mark("p_b_gram")
    for owner in range(4):
        for i in range(NB // LANES):
            block = jnp.broadcast_to(p_all[owner, i:i + 1, :], (LANES, LANES))
            p_b[owner * NB + i * LANES:owner * NB + (i + 1) * LANES, :] = block.T
    grams(me, partner)
    mark("wait_t")
    for k in range(T_CHUNKS):
        partner_arrived(t_rows(partner, k), ("t", k))
    for k in range(T_CHUNKS):
        forward(t_rows(far, k), ("t", k))
    for k in range(T_CHUNKS):
        partner_arrived(t_rows(far_partner, k), ("far t", k))

    scale = LOG2E / eps_ref[0, 0]

    def a_rows(a_all, local, base, rows=CH):
        for n in range(4):
            a_all[span(base, rows), n * 256:(n + 1) * 256] = jnp.dot(
                c1_rows[span(local, rows), :], t_all[:, n * 256:(n + 1) * 256], preferred_element_type=F32).astype(BF16)

    def scores(a_all, base, raw):
        for n in range(4):
            b = jnp.dot(a_all[span(base, CH), :], c2_all[:, n * 256:(n + 1) * 256], preferred_element_type=F32)
            t_st[raw:raw + CH, n * 256:(n + 1) * 256] = g_all[span(base, CH), n * 256:(n + 1) * 256] + (2.0 * (1.0 - ALPHA)) * b

    def products(a_all, base):
        for n in range(4):
            b = jnp.dot(a_all[span(base, CH), :], c2_all[:, n * 256:(n + 1) * 256], preferred_element_type=F32)
            g_all[span(base, CH), n * 256:(n + 1) * 256] = (2.0 * (1.0 - ALPHA)) * b

    def late_scores(base, raw, rows):
        for n in range(4):
            g = (2.0 * ALPHA) * lax.dot_general(x_all[span(base, rows), :], y_all[n * 256:(n + 1) * 256, :],
                                                (((1,), (1,)), ((), ())), preferred_element_type=F32)
            t_st[raw:raw + rows, n * 256:(n + 1) * 256] = g + g_all[span(base, rows), n * 256:(n + 1) * 256]
            g_all[span(base, rows), n * 256:(n + 1) * 256] = g

    def form(base, raw, rows=CH):
        acc = [acc_ref[:, col(j)] for j in range(COLS)]
        lead = 64
        group = FORM_GROUP
        shape = (group // 8, 8, LANES)
        for row in range(-2 * lead, rows, group):
            top = row + 2 * lead
            if top < rows:
                peak = tree(jnp.maximum, [t_st[raw + top:raw + top + group, col(j)] for j in range(COLS)])
                peak_b[top:top + group, :] = jnp.broadcast_to(jnp.max(peak, axis=1, keepdims=True), (group, LANES))
            mid = row + lead
            if 0 <= mid < rows:
                here = pl.ds(hint(base + mid, group), group)
                peak = peak_b[mid:mid + group, :]
                vals = [jnp.exp2((t_st[raw + mid:raw + mid + group, col(j)] - peak) * scale) for j in range(COLS)]
                for j in range(COLS):
                    kern[here, col(j)] = vals[j]
                total = jnp.sum(tree(jnp.add, vals), axis=1, keepdims=True)
                first_b[mid:mid + group, :] = p_b[here, :] / total
            if row >= 0:
                here = pl.ds(hint(base + row, group), group)
                u = first_b[row:row + group, :].reshape(shape)
                acc = [acc[j] + jnp.sum(kern[here, col(j)].reshape(shape) * u, axis=0) for j in range(COLS)]
        for j in range(COLS):
            acc_ref[:, col(j)] = acc[j]

    def b_rows(a_all, bases, ready=None):
        raws = (raw0, raw1)
        for i, base in enumerate(bases):
            if ready and ready[i]:
                ready[i]()
            scores(a_all, base, raws[i % 2])
            if i:
                form(bases[i - 1], raws[(i - 1) % 2])
        form(bases[-1], raws[(len(bases) - 1) % 2])

    def b_loop(a_all, count, base_of, arrived):
        scores(a_all, base_of(0), raw0)

        def pair(i, carry):
            @pl.when(i == 1)
            def _():
                arrived()
            scores(a_all, base_of(2 * i + 1), raw1)
            form(base_of(2 * i), raw0)
            scores(a_all, base_of(2 * i + 2), raw0)
            form(base_of(2 * i + 1), raw1)
            return carry
        lax.fori_loop(0, count // 2 - 1, pair, 0)
        scores(a_all, base_of(count - 1), raw1)
        form(base_of(count - 2), raw0)
        form(base_of(count - 1), raw1)

    def a_slice(a_all, base):
        return a_all.at[span(base, CH), :]

    def my_base(i):
        return jnp.where(i < 2, me * NB + i * CH, far * NB + (i - 2) * CH)

    def their_base(i):
        return jnp.where(i < 2, partner * NB + i * CH, far_partner * NB + (i - 2) * CH)

    mine = [my_base(i) for i in range(4)]
    theirs = [their_base(i) for i in range(4)]

    def share(a_all, name, start, stop):
        slot = SIDE.names[(name, 0)]

        def piece(i):
            ref = a_slice(a_all, my_base(i))
            return pltpu.make_async_remote_copy(
                src_ref=ref, dst_ref=ref, send_sem=side_send.at[slot + i], recv_sem=side_recv.at[slot + i],
                device_id={"rows": partner}, device_id_type=pl.DeviceIdType.MESH)

        def step(i, carry):
            a_rows(a_all, i * CH, my_base(i))
            piece(i).start()
            return carry
        if stop - start == 1:
            step(start, 0)
        else:
            lax.fori_loop(start, stop, step, 0)
        for i in range(start, stop):
            sends.append(piece(i))

    def b_groups(a_all, count, arrived):
        def group(g, carry):
            @pl.when(g == 1)
            def _():
                arrived()
            b_rows(a_all, [jnp.where(g == 0, mine[i], theirs[i]) for i in range(count)])
            return carry
        lax.fori_loop(0, 2, group, 0)

    acc_ref[...] = jnp.zeros_like(acc_ref)
    mark("a_own")
    share(a1_all, "a1", 0, 2)
    mark("wait_c2")
    for k, piece in enumerate(c2_pieces(far, far_partner, core)):
        forward(piece, ("c2", k))
    for k, piece in enumerate(c2_pieces(far_partner, far, 1 - core)):
        partner_arrived(piece, ("far c2", k))
    mark("c2_mirror")
    first = (1 - chip) * 2 * MB
    second = first + MB
    for base in (first, second):
        mirror(c2_all, base, base + 128, c2_all, base + 128, base, 128)
    mirror(c2_all, second + 128, first, c2_all, first, second + 128, 128)
    mirror(c2_all, second + 128, first + 128, c2_all, first + 128, second + 128, 128)
    mirror(c2_all, first, second, c2_all, second, first, 128)
    mirror(c2_all, first + 128, second, c2_all, second, first + 128, 128)
    mark("b_own")

    def a1_arrived():
        for i in range(2):
            partner_arrived(a_slice(a1_all, theirs[i]), ("a1", i))
    b_groups(a1_all, 2, a1_arrived)
    mark("wait_quads")
    for k, piece in enumerate(c1_quads(NB, far_partner, core)):
        far_arrived(piece, ("c1 quad", k))
        go(to_partner(piece, quad_side.at[k * HALF:(k + 1) * HALF, :], ("c1 quad", k)))
    for k in range(2):
        partner_arrived(quad_side.at[k * HALF:(k + 1) * HALF, :], ("c1 quad", k))
    mark("quad_mirror")
    mirror(quad_side, 0, 0, c1_rows, NB, far_partner * NB + HALF, HALF)
    mirror(quad_side, HALF, 0, c1_rows, NB + (1 - core) * HALF, far_partner * NB + (1 - core) * HALF, HALF)
    mark("a_early")

    def a_early(i, carry):
        rows = span(NB + i * CH, CH)
        for n in range(4):
            cols = slice(n * 256, (n + 1) * 256)
            kern[span(far * NB + i * CH, CH), cols] = (
                jnp.dot(c1_rows[rows, span(chip * 2 * NB, 2 * NB)], t_all[span(chip * 2 * NB, 2 * NB), cols],
                        preferred_element_type=F32)
                + jnp.dot(c1_rows[rows, span(far_partner * NB, NB)], t_all[span(far_partner * NB, NB), cols],
                          preferred_element_type=F32))
        return carry
    lax.fori_loop(0, 2, a_early, 0)

    def a_late(i):
        base = mine[2 + i]
        for n in range(4):
            cols = slice(n * 256, (n + 1) * 256)
            a1_all[span(base, CH), cols] = (
                kern[span(base, CH), cols]
                + jnp.dot(c1_rows[NB + i * CH:NB + (i + 1) * CH, span(far * NB, NB)], t_all[span(far * NB, NB), cols],
                          preferred_element_type=F32)).astype(BF16)
        go(to_partner(a_slice(a1_all, base), a_slice(a1_all, base), ("a1", 2 + i)))

    for i in range(2):
        mark("wait_strips%d" % i)
        for k in (2 * i, 2 * i + 1):
            far_arrived(c1_strip(NB, far, k), ("c1 strip", k))
            for below in range(k + 1, 4):
                mirror(c1_rows, NB + k * 128, far * NB + below * 128, c1_rows, NB + below * 128, far * NB + k * 128, 128)
        mark("a_far%d" % i)
        a_late(i)
        mark("products%d" % i)
        products(a1_all, mine[2 + i])
    mark("products_theirs")
    for i in range(2):
        partner_arrived(a_slice(a1_all, theirs[2 + i]), ("a1", 2 + i))
        products(a1_all, theirs[2 + i])
    mark("late")
    for k, (start, rows) in enumerate(X_PIECES):
        forward(x_piece(far, k), ("x", k))
        partner_arrived(x_piece(far_partner, k), ("far x", k))
        late_scores(far * NB + start, raw0, rows)
        late_scores(far_partner * NB + start, raw1, rows)
        form(far * NB + start, raw0, rows)
        form(far_partner * NB + start, raw1, rows)
    store_col_scale([acc_ref[:, col(j)] for j in range(COLS)], v_ref, q_ref)
    mark("sweeps")
    sweeps(SWEEPS - 1, kern, p_b, u_b, v_ref, q_ref)

    mark("next_plan")
    for copy in sends:
        copy.wait_send()
    sends.clear()

    def next_plan(i, carry):
        row = hint(i * 64, 64)
        for j, t in scaled_rows(kern, u_b, v_ref, row, 64):
            t_all[pl.ds(row, 64), col(j)] = t.astype(BF16)
        return carry
    lax.fori_loop(0, N // 64, next_plan, 0)

    acc_ref[...] = jnp.zeros_like(acc_ref)
    mark("a_2")
    first_slot = SIDE.names[("a2", 0)]

    def a2_piece(i):
        ref = a2_all.at[span(jnp.where(i == 0, me, far) * NB, NB), :]
        return pltpu.make_async_remote_copy(
            src_ref=ref, dst_ref=ref, send_sem=side_send.at[first_slot + i], recv_sem=side_recv.at[first_slot + i],
            device_id={"rows": partner}, device_id_type=pl.DeviceIdType.MESH)

    def a2_step(i, carry):
        a_rows(a2_all, i * NB, jnp.where(i == 0, me, far) * NB, NB)
        a2_piece(i).start()
        return carry
    lax.fori_loop(0, 2, a2_step, 0)
    sends.extend((a2_piece(0), a2_piece(1)))
    mark("b_2")

    def a2_arrived():
        for i in range(2):
            a2_piece(i).wait_recv()
    b_loop(a2_all, 8, lambda i: jnp.where(i < 4, my_base(i), their_base(i - 4)), a2_arrived)
    store_col_scale([acc_ref[:, col(j)] for j in range(COLS)], v_ref, q_ref)
    mark("sweeps")
    sweeps(SWEEPS - 1, kern, p_b, u_b, v_ref, q_ref)

    mark("result")

    def result(i, carry):
        row = hint(i * 64, 64)
        for j, t in scaled_rows(kern, u_b, v_ref, hint(me * NB + row, 64), 64):
            out_ref[pl.ds(row, 64), col(j)] = t
        return carry
    lax.fori_loop(0, NB // 64, result, 0)
    for copy in sends:
        copy.wait_send()
    mark(None)


def solution(mesh):
    vmem = pl.BlockSpec(memory_space=pltpu.VMEM)
    hbm = pl.BlockSpec(memory_space=pl.ANY)
    smem = pl.BlockSpec(memory_space=pltpu.SMEM)

    def local_fgw(cost_src, cost_tgt, plan_init, mass_src, mass_tgt, feat_src, feat_tgt, epsilon):
        return pl.pallas_call(
            kernel,
            out_shape=pltpu.VMEM((NB, M), F32),
            in_specs=[hbm] * 7 + [smem],
            out_specs=vmem,
            scratch_shapes=[
                pltpu.VMEM((1, M), F32),
                pltpu.VMEM((NB, M), F32),
                pltpu.VMEM((N, M), BF16),
                pltpu.VMEM((2 * NB, N), BF16),
                pltpu.VMEM((NB, NB), BF16),
                pltpu.VMEM((2 * HALF, HALF), BF16),
                pltpu.VMEM((M, M), BF16),
                pltpu.VMEM((M, D), BF16),
                pltpu.VMEM((N, D), BF16),
                pltpu.VMEM((N, M), F32),
                pltpu.VMEM((N, M), BF16),
                pltpu.VMEM((N, M), BF16),
                pltpu.VMEM((N, M), F32),
                pltpu.VMEM((4, NB // LANES, LANES), F32),
                pltpu.VMEM((N, LANES), F32),
                pltpu.VMEM((N, LANES), F32),
                pltpu.VMEM((CH, LANES), F32),
                pltpu.VMEM((CH, LANES), F32),
                pltpu.VMEM((8, M), F32),
                pltpu.VMEM((8, M), F32),
                pltpu.SemaphoreType.DMA((8,)),
                pltpu.SemaphoreType.DMA((len(LINK.names),)),
                pltpu.SemaphoreType.DMA((len(LINK.names),)),
                pltpu.SemaphoreType.DMA((len(SIDE.names),)),
                pltpu.SemaphoreType.DMA((len(SIDE.names),)),
            ],
            compiler_params=pltpu.CompilerParams(
                collective_id=0, has_side_effects=True, vmem_limit_bytes=54000 * 1024),
        )(*(pltpu.with_memory_space_constraint(x, pltpu.HBM) for x in (
            cost_src, cost_tgt, plan_init, mass_src.reshape(NB // LANES, LANES), mass_tgt.reshape(1, M),
            feat_src, feat_tgt)), epsilon.reshape(1, 1))

    row_spec = P(('pairs', 'rows'), None)
    vec_spec = P(('pairs', 'rows'))
    in_specs = (row_spec, row_spec, row_spec, vec_spec, P('pairs'), row_spec, row_spec, P())
    return jax.shard_map(local_fgw, mesh=mesh, in_specs=in_specs, out_specs=row_spec, check_vma=False)
```

```python
import jax
import jax.numpy as jnp
from jax import lax
from jax.experimental import pallas as pl
from jax.experimental.pallas import tpu as pltpu
from jax.sharding import PartitionSpec as P

ALPHA = 0.5
OUTER_STEPS = 2
SWEEPS = 10
LOG2E = 1.4426950408889634

N = 2048
M = 1024
D = 256
NB = 512
MB = 256
F32 = jnp.float32
BF16 = jnp.bfloat16
LANES = 128
COLS = M // LANES

T_CHUNKS = 4
TR = NB // T_CHUNKS
CH = 256
HALF = NB // 2
FORM_GROUP = 32


class Slots:
    def __init__(self):
        self.names = {}

    def __call__(self, name):
        return self.names.setdefault(name, len(self.names))


LINK = Slots()
SIDE = Slots()
for k in range(T_CHUNKS):
    LINK(("t", k)), SIDE(("t", k)), SIDE(("far t", k))
for k in range(4):
    LINK(("c2", k)), SIDE(("far c2", k)), LINK(("c1 strip", k))
for k in range(4):
    SIDE(("a1", k))
for k in range(2):
    SIDE(("a2", k))
for k in range(2):
    LINK(("c1 quad", k)), SIDE(("c1 quad", k))
for k in range(2):
    LINK(("x", k)), SIDE(("far x", k))
for name in ("y", "p"):
    LINK(name), SIDE(name), SIDE("far " + name)
SIDE("c2"), SIDE("c1"), SIDE("x")


def hint(value, multiple):
    return value if isinstance(value, int) else pl.multiple_of(value, multiple)


def span(start, size):
    return pl.ds(hint(start, size), size)


def col(j):
    return slice(j * LANES, (j + 1) * LANES)


def tree(op, parts):
    while len(parts) > 1:
        parts = [op(parts[i], parts[i + 1]) for i in range(0, len(parts), 2)]
    return parts[0]


def store_col_scale(acc, v_ref, q_ref):
    for j in range(COLS):
        col_sum = jnp.sum(acc[j], axis=0, keepdims=True)
        v_ref[:, col(j)] = jnp.broadcast_to(q_ref[:, col(j)] / col_sum, (8, LANES))


def sweeps(count, kern, plan_b, u_b, v_ref, q_ref, group):
    lead = 128
    shape = (group // 8, 8, LANES)

    def sweep(_, carry):
        v = [v_ref[:, col(j)][None] for j in range(COLS)]

        def tile(row, j):
            return kern[row:row + group, col(j)].reshape(shape)

        acc = [jnp.zeros((8, LANES), F32) for _ in range(COLS)]
        for row in range(-lead, N, group):
            top = row + lead
            if top < N:
                total = tree(jnp.add, [tile(top, j) * v[j] for j in range(COLS)])
                u = plan_b[top:top + group, :].reshape(shape) / jnp.sum(total, axis=2, keepdims=True)
                u_b[top:top + group, :] = u.reshape(group, LANES)
            if row >= 0:
                u = u_b[row:row + group, :].reshape(shape)
                acc = [acc[j] + jnp.sum(tile(row, j) * u, axis=0) for j in range(COLS)]
        store_col_scale(acc, v_ref, q_ref)
        return carry

    lax.fori_loop(0, count, sweep, 0)


def scaled_rows(kern, u_b, v_ref, row, count):
    u = u_b[pl.ds(row, count), :].reshape(count // 8, 8, LANES)
    for j in range(COLS):
        k = kern[pl.ds(row, count), col(j)].reshape(count // 8, 8, LANES)
        yield j, (u * k * v_ref[:, col(j)][None]).reshape(count, LANES)


def kernel(c1_hbm, c2_hbm, t0_hbm, p_hbm, q_hbm, x_hbm, y_hbm, eps_ref, out_ref,
           q_ref, t_st, t_all, c1_rows, c1_side, quad_side, c2_all, y_all, x_all, g_all, a1_all, a2_all,
           kern, p_all, p_b, u_b, peak_b, first_b, acc_ref, v_ref,
           load_sem, link_send, link_recv, side_send, side_recv):
    raw0, raw1 = 0, CH
    current = [None]

    def mark(name):
        if current[0] is not None:
            current[0].__exit__(None, None, None)
            current[0] = None
        if name:
            current[0] = jax.named_scope(name)
            current[0].__enter__()

    me = lax.axis_index("rows")
    chip = me // 2
    core = me % 2
    partner = chip * 2 + (1 - core)
    far = (1 - chip) * 2 + core
    far_partner = (1 - chip) * 2 + (1 - core)

    y_st, x_st, c2_st = kern.at[:MB, :D], kern.at[MB:MB + NB, :D], kern.at[MB + NB:2 * MB + NB, :]
    loads = {}
    for i, (name, src, dst) in enumerate((
            ("y", y_hbm, y_st), ("p", p_hbm, p_all.at[me]), ("t", t0_hbm, t_st), ("c2", c2_hbm, c2_st), ("x", x_hbm, x_st),
            ("left", c1_hbm.at[:, :M], g_all.at[:NB]), ("right", c1_hbm.at[:, M:], g_all.at[NB:2 * NB]), ("q", q_hbm, q_ref))):
        loads[name] = pltpu.make_async_copy(src, dst, load_sem.at[i])
        loads[name].start()

    mark("barrier")
    barrier = pltpu.get_barrier_semaphore()
    for peer in (partner, far):
        pl.semaphore_signal(barrier, inc=1, device_id={"rows": peer}, device_id_type=pl.DeviceIdType.MESH)
    pl.semaphore_wait(barrier, 2)

    def to_far(src, dst, name):
        slot = LINK.names[name]
        return pltpu.make_async_remote_copy(
            src_ref=src, dst_ref=dst, send_sem=link_send.at[slot], recv_sem=link_recv.at[slot],
            device_id={"rows": far}, device_id_type=pl.DeviceIdType.MESH)

    def to_partner(src, dst, name):
        slot = SIDE.names[name]
        return pltpu.make_async_remote_copy(
            src_ref=src, dst_ref=dst, send_sem=side_send.at[slot], recv_sem=side_recv.at[slot],
            device_id={"rows": partner}, device_id_type=pl.DeviceIdType.MESH)

    sends = []

    def go(copy):
        copy.start()
        sends.append(copy)

    def far_arrived(ref, name):
        to_far(ref, ref, name).wait_recv()

    def partner_arrived(ref, name):
        to_partner(ref, ref, name).wait_recv()

    def t_rows(owner, k):
        return t_all.at[span(owner * NB + k * TR, TR), :]

    def c2_rows(owner):
        return c2_all.at[span(owner * MB, MB), :]

    def c2_pieces(owner, other, which):
        return (
            c2_all.at[span(owner * MB + 128, 128), span(other * MB, 128)],
            c2_all.at[span(owner * MB + which * 128, 128), span(other * MB + which * 128, 128)],
            c2_all.at[span(owner * MB, 128), span(owner * MB, MB)],
            c2_all.at[span(owner * MB + 128, 128), span(owner * MB + 128, 128)])

    def y_rows(owner):
        return y_all.at[span(owner * MB, MB), :]

    def x_rows(owner):
        return x_all.at[span(owner * NB, NB), :]

    def x_half(owner, k):
        return x_all.at[span(owner * NB + k * CH, CH), :]

    def c1_quads(base, other, which):
        return (c1_rows.at[base + HALF:base + NB, span(other * NB, HALF)],
                c1_rows.at[span(base + which * HALF, HALF), span(other * NB + which * HALF, HALF)])

    def c1_strip(base, owner, k):
        return c1_rows.at[base + k * 128:base + (k + 1) * 128, pl.ds(hint(owner * NB + k * 128, 128), NB - k * 128)]

    mark("cast_y")
    loads["y"].wait()
    y_all[span(me * MB, MB), :] = kern[:MB, :D].astype(BF16)
    loads["p"].wait()
    go(to_far(p_all.at[me], p_all.at[me], "p"))
    go(to_partner(p_all.at[me], p_all.at[me], "p"))
    go(to_far(y_rows(me), y_rows(me), "y"))
    go(to_partner(y_rows(me), y_rows(me), "y"))
    mark("cast_t")
    loads["t"].wait()
    for k in range(T_CHUNKS):
        t_all[span(me * NB + k * TR, TR), :] = t_st[k * TR:(k + 1) * TR, :].astype(BF16)
    for k in range(T_CHUNKS):
        go(to_far(t_rows(me, k), t_rows(me, k), ("t", k)))
    for k in range(T_CHUNKS):
        go(to_partner(t_rows(me, k), t_rows(me, k), ("t", k)))
    mark("cast_rest")
    for name in ("c2", "x", "left", "right", "q"):
        loads[name].wait()
    c2_all[span(me * MB, MB), :] = kern[MB + NB:2 * MB + NB, :].astype(BF16)
    x_all[span(me * NB, NB), :] = kern[MB:MB + NB, :D].astype(BF16)
    c1_rows[:NB, :M] = g_all[:NB, :].astype(BF16)
    c1_rows[:NB, M:] = g_all[NB:2 * NB, :].astype(BF16)
    for k, piece in enumerate(c2_pieces(me, partner, core)):
        go(to_far(piece, piece, ("c2", k)))
    for k, (src, dst) in enumerate(zip(c1_quads(0, partner, core), c1_quads(NB, partner, core))):
        go(to_far(src, dst, ("c1 quad", k)))
    for k in range(4):
        go(to_far(c1_strip(0, me, k), c1_strip(NB, me, k), ("c1 strip", k)))
    for k in range(2):
        go(to_far(x_half(me, k), x_half(me, k), ("x", k)))
    go(to_partner(c2_rows(me), c2_rows(me), "c2"))
    go(to_partner(x_rows(me), x_rows(me), "x"))
    go(to_partner(c1_rows.at[:NB, span(far_partner * NB, NB)], c1_side, "c1"))

    def mirror(src, src_row, src_col, dst, dst_row, dst_col, size):
        for i in range(size // LANES):
            for j in range(size // LANES):
                tile = src[span(src_row + i * LANES, LANES), span(src_col + j * LANES, LANES)]
                dst[span(dst_row + j * LANES, LANES), span(dst_col + i * LANES, LANES)] = (
                    tile.astype(F32).T.astype(BF16))

    mark("mirrors")
    mirror(c1_rows, 0, far * NB, c1_rows, NB, me * NB, NB)
    partner_arrived(c1_side, "c1")
    mirror(c1_side, 0, 0, c1_rows, NB, partner * NB, NB)
    partner_arrived(c2_rows(partner), "c2")
    mirror(c2_all, chip * 2 * MB, (1 - chip) * 2 * MB, c2_all, (1 - chip) * 2 * MB, chip * 2 * MB, 2 * MB)
    partner_arrived(y_rows(partner), "y")
    partner_arrived(p_all.at[partner], "p")
    partner_arrived(x_rows(partner), "x")

    def forward(ref, name):
        far_arrived(ref, name)
        go(to_partner(ref, ref, ("far " + name[0], name[1]) if isinstance(name, tuple) else "far " + name))

    def gram(owner):
        for n in range(4):
            g = lax.dot_general(x_all[span(owner * NB, NB), :], y_all[n * 256:(n + 1) * 256, :],
                                (((1,), (1,)), ((), ())), preferred_element_type=F32)
            g_all[span(owner * NB, NB), n * 256:(n + 1) * 256] = (2.0 * ALPHA) * g

    def grams(first, second):
        def one(i, carry):
            gram(first + i * (second - first))
            return carry
        lax.fori_loop(0, 2, one, 0)

    mark("wait_y")
    forward(y_rows(far), "y")
    forward(p_all.at[far], "p")
    partner_arrived(y_rows(far_partner), "far y")
    partner_arrived(p_all.at[far_partner], "far p")
    mark("p_b_gram")
    for owner in range(4):
        for i in range(NB // LANES):
            block = jnp.broadcast_to(p_all[owner, i:i + 1, :], (LANES, LANES))
            p_b[owner * NB + i * LANES:owner * NB + (i + 1) * LANES, :] = block.T
    grams(me, partner)
    mark("wait_t")
    for k in range(T_CHUNKS):
        partner_arrived(t_rows(partner, k), ("t", k))
    for k in range(T_CHUNKS):
        forward(t_rows(far, k), ("t", k))
    for k in range(T_CHUNKS):
        partner_arrived(t_rows(far_partner, k), ("far t", k))

    scale = LOG2E / eps_ref[0, 0]

    def a_rows(a_all, local, base, rows=CH):
        for n in range(4):
            a_all[span(base, rows), n * 256:(n + 1) * 256] = jnp.dot(
                c1_rows[span(local, rows), :], t_all[:, n * 256:(n + 1) * 256], preferred_element_type=F32).astype(BF16)

    def scores(a_all, base, raw):
        for n in range(4):
            b = jnp.dot(a_all[span(base, CH), :], c2_all[:, n * 256:(n + 1) * 256], preferred_element_type=F32)
            t_st[raw:raw + CH, n * 256:(n + 1) * 256] = g_all[span(base, CH), n * 256:(n + 1) * 256] + (2.0 * (1.0 - ALPHA)) * b

    def products(a_all, base):
        for n in range(4):
            b = jnp.dot(a_all[span(base, CH), :], c2_all[:, n * 256:(n + 1) * 256], preferred_element_type=F32)
            g_all[span(base, CH), n * 256:(n + 1) * 256] = (2.0 * (1.0 - ALPHA)) * b

    def late_scores(base, raw):
        for n in range(4):
            g = (2.0 * ALPHA) * lax.dot_general(x_all[span(base, CH), :], y_all[n * 256:(n + 1) * 256, :],
                                                (((1,), (1,)), ((), ())), preferred_element_type=F32)
            t_st[raw:raw + CH, n * 256:(n + 1) * 256] = g + g_all[span(base, CH), n * 256:(n + 1) * 256]
            g_all[span(base, CH), n * 256:(n + 1) * 256] = g

    def form(base, raw):
        acc = [acc_ref[:, col(j)] for j in range(COLS)]
        lead = 64
        group = FORM_GROUP
        shape = (group // 8, 8, LANES)
        for row in range(-2 * lead, CH, group):
            top = row + 2 * lead
            if top < CH:
                peak = tree(jnp.maximum, [t_st[raw + top:raw + top + group, col(j)] for j in range(COLS)])
                peak_b[raw + top:raw + top + group, :] = jnp.broadcast_to(jnp.max(peak, axis=1, keepdims=True), (group, LANES))
            mid = row + lead
            if 0 <= mid < CH:
                here = pl.ds(hint(base + mid, group), group)
                peak = peak_b[raw + mid:raw + mid + group, :]
                vals = [jnp.exp2((t_st[raw + mid:raw + mid + group, col(j)] - peak) * scale) for j in range(COLS)]
                for j in range(COLS):
                    kern[here, col(j)] = vals[j]
                    t_st[raw + mid:raw + mid + group, col(j)] = vals[j]
                total = jnp.sum(tree(jnp.add, vals), axis=1, keepdims=True)
                first_b[raw + mid:raw + mid + group, :] = p_b[here, :] / total
            if row >= 0:
                u = first_b[raw + row:raw + row + group, :].reshape(shape)
                acc = [acc[j] + jnp.sum(t_st[raw + row:raw + row + group, col(j)].reshape(shape) * u, axis=0)
                       for j in range(COLS)]
        for j in range(COLS):
            acc_ref[:, col(j)] = acc[j]

    def b_rows(a_all, bases, ready=None):
        raws = (raw0, raw1)
        for i, base in enumerate(bases):
            if ready and ready[i]:
                ready[i]()
            scores(a_all, base, raws[i % 2])
            if i:
                form(bases[i - 1], raws[(i - 1) % 2])
        form(bases[-1], raws[(len(bases) - 1) % 2])

    def a_slice(a_all, base):
        return a_all.at[span(base, CH), :]

    def my_base(i):
        return jnp.where(i < 2, me * NB + i * CH, far * NB + (i - 2) * CH)

    def their_base(i):
        return jnp.where(i < 2, partner * NB + i * CH, far_partner * NB + (i - 2) * CH)

    mine = [my_base(i) for i in range(4)]
    theirs = [their_base(i) for i in range(4)]

    def share(a_all, name, start, stop):
        slot = SIDE.names[(name, 0)]

        def piece(i):
            ref = a_slice(a_all, my_base(i))
            return pltpu.make_async_remote_copy(
                src_ref=ref, dst_ref=ref, send_sem=side_send.at[slot + i], recv_sem=side_recv.at[slot + i],
                device_id={"rows": partner}, device_id_type=pl.DeviceIdType.MESH)

        def step(i, carry):
            a_rows(a_all, i * CH, my_base(i))
            piece(i).start()
            return carry
        if stop - start == 1:
            step(start, 0)
        else:
            lax.fori_loop(start, stop, step, 0)
        for i in range(start, stop):
            sends.append(piece(i))

    def b_groups(a_all, count, arrived):
        def group(g, carry):
            @pl.when(g == 1)
            def _():
                arrived()
            b_rows(a_all, [jnp.where(g == 0, mine[i], theirs[i]) for i in range(count)])
            return carry
        lax.fori_loop(0, 2, group, 0)

    acc_ref[...] = jnp.zeros_like(acc_ref)
    mark("a_own")
    share(a1_all, "a1", 0, 2)
    mark("wait_c2")
    for k, piece in enumerate(c2_pieces(far, far_partner, core)):
        forward(piece, ("c2", k))
    for k, piece in enumerate(c2_pieces(far_partner, far, 1 - core)):
        partner_arrived(piece, ("far c2", k))
    mark("c2_mirror")
    first = (1 - chip) * 2 * MB
    second = first + MB
    for base in (first, second):
        mirror(c2_all, base, base + 128, c2_all, base + 128, base, 128)
    mirror(c2_all, second + 128, first, c2_all, first, second + 128, 128)
    mirror(c2_all, second + 128, first + 128, c2_all, first + 128, second + 128, 128)
    mirror(c2_all, first, second, c2_all, second, first, 128)
    mirror(c2_all, first + 128, second, c2_all, second, first + 128, 128)
    mark("b_own")

    def a1_arrived():
        for i in range(2):
            partner_arrived(a_slice(a1_all, theirs[i]), ("a1", i))
    b_groups(a1_all, 2, a1_arrived)
    mark("wait_quads")
    for k, piece in enumerate(c1_quads(NB, far_partner, core)):
        far_arrived(piece, ("c1 quad", k))
        go(to_partner(piece, quad_side.at[k * HALF:(k + 1) * HALF, :], ("c1 quad", k)))
    for k in range(2):
        partner_arrived(quad_side.at[k * HALF:(k + 1) * HALF, :], ("c1 quad", k))
    mark("quad_mirror")
    mirror(quad_side, 0, 0, c1_rows, NB, far_partner * NB + HALF, HALF)
    mirror(quad_side, HALF, 0, c1_rows, NB + (1 - core) * HALF, far_partner * NB + (1 - core) * HALF, HALF)
    mark("a_early")

    def a_early(i, carry):
        rows = span(NB + i * CH, CH)
        for n in range(4):
            cols = slice(n * 256, (n + 1) * 256)
            kern[span(far * NB + i * CH, CH), cols] = (
                jnp.dot(c1_rows[rows, span(chip * 2 * NB, 2 * NB)], t_all[span(chip * 2 * NB, 2 * NB), cols],
                        preferred_element_type=F32)
                + jnp.dot(c1_rows[rows, span(far_partner * NB, NB)], t_all[span(far_partner * NB, NB), cols],
                          preferred_element_type=F32))
        return carry
    lax.fori_loop(0, 2, a_early, 0)

    def a_late(i):
        base = mine[2 + i]
        for n in range(4):
            cols = slice(n * 256, (n + 1) * 256)
            a1_all[span(base, CH), cols] = (
                kern[span(base, CH), cols]
                + jnp.dot(c1_rows[NB + i * CH:NB + (i + 1) * CH, span(far * NB, NB)], t_all[span(far * NB, NB), cols],
                          preferred_element_type=F32)).astype(BF16)
        go(to_partner(a_slice(a1_all, base), a_slice(a1_all, base), ("a1", 2 + i)))

    for i in range(2):
        mark("wait_strips%d" % i)
        for k in (2 * i, 2 * i + 1):
            far_arrived(c1_strip(NB, far, k), ("c1 strip", k))
            for below in range(k + 1, 4):
                mirror(c1_rows, NB + k * 128, far * NB + below * 128, c1_rows, NB + below * 128, far * NB + k * 128, 128)
        mark("a_far%d" % i)
        a_late(i)
        mark("products%d" % i)
        products(a1_all, mine[2 + i])
    mark("products_theirs")
    for i in range(2):
        partner_arrived(a_slice(a1_all, theirs[2 + i]), ("a1", 2 + i))
        products(a1_all, theirs[2 + i])
    mark("late")
    for half in range(2):
        forward(x_half(far, half), ("x", half))
        late_scores(mine[2 + half], raw0)
        form(mine[2 + half], raw0)
        partner_arrived(x_half(far_partner, half), ("far x", half))
        late_scores(theirs[2 + half], raw1)
        form(theirs[2 + half], raw1)
    store_col_scale([acc_ref[:, col(j)] for j in range(COLS)], v_ref, q_ref)
    mark("sweeps")
    sweeps(SWEEPS - 1, kern, p_b, u_b, v_ref, q_ref, 32)

    mark("next_plan")
    for copy in sends:
        copy.wait_send()
    sends.clear()

    def next_plan(i, carry):
        row = hint(i * 64, 64)
        for j, t in scaled_rows(kern, u_b, v_ref, row, 64):
            t_all[pl.ds(row, 64), col(j)] = t.astype(BF16)
        return carry
    lax.fori_loop(0, N // 64, next_plan, 0)

    acc_ref[...] = jnp.zeros_like(acc_ref)
    mark("a_2")
    first_slot = SIDE.names[("a2", 0)]

    def a2_piece(i):
        ref = a2_all.at[span(jnp.where(i == 0, me, far) * NB, NB), :]
        return pltpu.make_async_remote_copy(
            src_ref=ref, dst_ref=ref, send_sem=side_send.at[first_slot + i], recv_sem=side_recv.at[first_slot + i],
            device_id={"rows": partner}, device_id_type=pl.DeviceIdType.MESH)

    def a2_step(i, carry):
        a_rows(a2_all, i * NB, jnp.where(i == 0, me, far) * NB, NB)
        a2_piece(i).start()
        return carry
    lax.fori_loop(0, 2, a2_step, 0)
    sends.extend((a2_piece(0), a2_piece(1)))
    mark("b_2")

    def a2_arrived():
        for i in range(2):
            a2_piece(i).wait_recv()
    b_groups(a2_all, 4, a2_arrived)
    store_col_scale([acc_ref[:, col(j)] for j in range(COLS)], v_ref, q_ref)
    mark("sweeps")
    sweeps(SWEEPS - 1, kern, p_b, u_b, v_ref, q_ref, 16)

    mark("result")

    def result(i, carry):
        row = hint(i * 64, 64)
        for j, t in scaled_rows(kern, u_b, v_ref, hint(me * NB + row, 64), 64):
            out_ref[pl.ds(row, 64), col(j)] = t
        return carry
    lax.fori_loop(0, NB // 64, result, 0)
    for copy in sends:
        copy.wait_send()
    mark(None)


def solution(mesh):
    vmem = pl.BlockSpec(memory_space=pltpu.VMEM)
    hbm = pl.BlockSpec(memory_space=pl.ANY)
    smem = pl.BlockSpec(memory_space=pltpu.SMEM)

    def local_fgw(cost_src, cost_tgt, plan_init, mass_src, mass_tgt, feat_src, feat_tgt, epsilon):
        return pl.pallas_call(
            kernel,
            out_shape=pltpu.VMEM((NB, M), F32),
            in_specs=[hbm] * 7 + [smem],
            out_specs=vmem,
            scratch_shapes=[
                pltpu.VMEM((1, M), F32),
                pltpu.VMEM((NB, M), F32),
                pltpu.VMEM((N, M), BF16),
                pltpu.VMEM((2 * NB, N), BF16),
                pltpu.VMEM((NB, NB), BF16),
                pltpu.VMEM((2 * HALF, HALF), BF16),
                pltpu.VMEM((M, M), BF16),
                pltpu.VMEM((M, D), BF16),
                pltpu.VMEM((N, D), BF16),
                pltpu.VMEM((N, M), F32),
                pltpu.VMEM((N, M), BF16),
                pltpu.VMEM((N, M), BF16),
                pltpu.VMEM((N, M), F32),
                pltpu.VMEM((4, NB // LANES, LANES), F32),
                pltpu.VMEM((N, LANES), F32),
                pltpu.VMEM((N, LANES), F32),
                pltpu.VMEM((2 * CH, LANES), F32),
                pltpu.VMEM((2 * CH, LANES), F32),
                pltpu.VMEM((8, M), F32),
                pltpu.VMEM((8, M), F32),
                pltpu.SemaphoreType.DMA((8,)),
                pltpu.SemaphoreType.DMA((len(LINK.names),)),
                pltpu.SemaphoreType.DMA((len(LINK.names),)),
                pltpu.SemaphoreType.DMA((len(SIDE.names),)),
                pltpu.SemaphoreType.DMA((len(SIDE.names),)),
            ],
            compiler_params=pltpu.CompilerParams(
                collective_id=0, has_side_effects=True, vmem_limit_bytes=54000 * 1024),
        )(*(pltpu.with_memory_space_constraint(x, pltpu.HBM) for x in (
            cost_src, cost_tgt, plan_init, mass_src.reshape(NB // LANES, LANES), mass_tgt.reshape(1, M),
            feat_src, feat_tgt)), epsilon.reshape(1, 1))

    row_spec = P(('pairs', 'rows'), None)
    vec_spec = P(('pairs', 'rows'))
    in_specs = (row_spec, row_spec, row_spec, vec_spec, P('pairs'), row_spec, row_spec, P())
    return jax.shard_map(local_fgw, mesh=mesh, in_specs=in_specs, out_specs=row_spec, check_vma=False)
```

```python
import jax
import jax.numpy as jnp
from jax import lax
from jax.experimental import pallas as pl
from jax.experimental.pallas import tpu as pltpu
from jax.sharding import PartitionSpec as P

ALPHA = 0.5
OUTER_STEPS = 2
SWEEPS = 10
LOG2E = 1.4426950408889634

N = 2048
M = 1024
D = 256
NB = 512
MB = 256
F32 = jnp.float32
BF16 = jnp.bfloat16
LANES = 128
COLS = M // LANES

T_CHUNKS = 4
TR = NB // T_CHUNKS
CH = 256
HALF = NB // 2
FORM_GROUP = 32


class Slots:
    def __init__(self):
        self.names = {}

    def __call__(self, name):
        return self.names.setdefault(name, len(self.names))


LINK = Slots()
SIDE = Slots()
for k in range(T_CHUNKS):
    LINK(("t", k)), SIDE(("t", k)), SIDE(("far t", k))
for k in range(4):
    LINK(("c2", k)), SIDE(("far c2", k)), LINK(("c1 strip", k))
for k in range(4):
    SIDE(("a1", k))
for k in range(2):
    SIDE(("a2", k))
for k in range(2):
    LINK(("c1 quad", k)), SIDE(("c1 quad", k))
for k in range(2):
    LINK(("x", k)), SIDE(("far x", k))
for name in ("y", "p"):
    LINK(name), SIDE(name), SIDE("far " + name)
SIDE("c2"), SIDE("c1"), SIDE("x")


def hint(value, multiple):
    return value if isinstance(value, int) else pl.multiple_of(value, multiple)


def span(start, size):
    return pl.ds(hint(start, size), size)


def col(j):
    return slice(j * LANES, (j + 1) * LANES)


def tree(op, parts):
    while len(parts) > 1:
        parts = [op(parts[i], parts[i + 1]) for i in range(0, len(parts), 2)]
    return parts[0]


def store_col_scale(acc, v_ref, q_ref):
    for j in range(COLS):
        col_sum = jnp.sum(acc[j], axis=0, keepdims=True)
        v_ref[:, col(j)] = jnp.broadcast_to(q_ref[:, col(j)] / col_sum, (8, LANES))


def sweeps(count, kern, plan_b, u_b, v_ref, q_ref, group):
    lead = 128
    shape = (group // 8, 8, LANES)

    def sweep(_, carry):
        v = [v_ref[:, col(j)][None] for j in range(COLS)]

        def tile(row, j):
            return kern[row:row + group, col(j)].reshape(shape)

        acc = [jnp.zeros((8, LANES), F32) for _ in range(COLS)]
        for row in range(-lead, N, group):
            top = row + lead
            if top < N:
                total = tree(jnp.add, [tile(top, j) * v[j] for j in range(COLS)])
                u = plan_b[top:top + group, :].reshape(shape) / jnp.sum(total, axis=2, keepdims=True)
                u_b[top:top + group, :] = u.reshape(group, LANES)
            if row >= 0:
                u = u_b[row:row + group, :].reshape(shape)
                acc = [acc[j] + jnp.sum(tile(row, j) * u, axis=0) for j in range(COLS)]
        store_col_scale(acc, v_ref, q_ref)
        return carry

    lax.fori_loop(0, count, sweep, 0)


def scaled_rows(kern, u_b, v_ref, row, count):
    u = u_b[pl.ds(row, count), :].reshape(count // 8, 8, LANES)
    for j in range(COLS):
        k = kern[pl.ds(row, count), col(j)].reshape(count // 8, 8, LANES)
        yield j, (u * k * v_ref[:, col(j)][None]).reshape(count, LANES)


def kernel(c1_hbm, c2_hbm, t0_hbm, p_hbm, q_hbm, x_hbm, y_hbm, eps_ref, out_ref,
           q_ref, t_st, t_all, c1_rows, c1_side, quad_side, c2_all, y_all, x_all, g_all, a1_all, a2_all,
           kern, p_all, p_b, u_b, peak_b, first_b, acc_ref, v_ref,
           load_sem, link_send, link_recv, side_send, side_recv):
    raw0, raw1 = 0, CH
    me = lax.axis_index("rows")
    chip = me // 2
    core = me % 2
    partner = chip * 2 + (1 - core)
    far = (1 - chip) * 2 + core
    far_partner = (1 - chip) * 2 + (1 - core)

    y_st, x_st, c2_st = kern.at[:MB, :D], kern.at[MB:MB + NB, :D], kern.at[MB + NB:2 * MB + NB, :]
    loads = {}
    for i, (name, src, dst) in enumerate((
            ("y", y_hbm, y_st), ("p", p_hbm, p_all.at[me]), ("t", t0_hbm, t_st), ("c2", c2_hbm, c2_st), ("x", x_hbm, x_st),
            ("left", c1_hbm.at[:, :M], g_all.at[:NB]), ("right", c1_hbm.at[:, M:], g_all.at[NB:2 * NB]), ("q", q_hbm, q_ref))):
        loads[name] = pltpu.make_async_copy(src, dst, load_sem.at[i])
        loads[name].start()

    barrier = pltpu.get_barrier_semaphore()
    for peer in (partner, far):
        pl.semaphore_signal(barrier, inc=1, device_id={"rows": peer}, device_id_type=pl.DeviceIdType.MESH)
    pl.semaphore_wait(barrier, 2)

    def to_far(src, dst, name):
        slot = LINK.names[name]
        return pltpu.make_async_remote_copy(
            src_ref=src, dst_ref=dst, send_sem=link_send.at[slot], recv_sem=link_recv.at[slot],
            device_id={"rows": far}, device_id_type=pl.DeviceIdType.MESH)

    def to_partner(src, dst, name):
        slot = SIDE.names[name]
        return pltpu.make_async_remote_copy(
            src_ref=src, dst_ref=dst, send_sem=side_send.at[slot], recv_sem=side_recv.at[slot],
            device_id={"rows": partner}, device_id_type=pl.DeviceIdType.MESH)

    sends = []

    def go(copy):
        copy.start()
        sends.append(copy)

    def far_arrived(ref, name):
        to_far(ref, ref, name).wait_recv()

    def partner_arrived(ref, name):
        to_partner(ref, ref, name).wait_recv()

    def t_rows(owner, k):
        return t_all.at[span(owner * NB + k * TR, TR), :]

    def c2_rows(owner):
        return c2_all.at[span(owner * MB, MB), :]

    def c2_pieces(owner, other, which):
        return (
            c2_all.at[span(owner * MB + 128, 128), span(other * MB, 128)],
            c2_all.at[span(owner * MB + which * 128, 128), span(other * MB + which * 128, 128)],
            c2_all.at[span(owner * MB, 128), span(owner * MB, MB)],
            c2_all.at[span(owner * MB + 128, 128), span(owner * MB + 128, 128)])

    def y_rows(owner):
        return y_all.at[span(owner * MB, MB), :]

    def x_rows(owner):
        return x_all.at[span(owner * NB, NB), :]

    def x_half(owner, k):
        return x_all.at[span(owner * NB + k * CH, CH), :]

    def c1_quads(base, other, which):
        return (c1_rows.at[base + HALF:base + NB, span(other * NB, HALF)],
                c1_rows.at[span(base + which * HALF, HALF), span(other * NB + which * HALF, HALF)])

    def c1_strip(base, owner, k):
        return c1_rows.at[base + k * 128:base + (k + 1) * 128, pl.ds(hint(owner * NB + k * 128, 128), NB - k * 128)]

    loads["y"].wait()
    y_all[span(me * MB, MB), :] = kern[:MB, :D].astype(BF16)
    loads["p"].wait()
    go(to_far(p_all.at[me], p_all.at[me], "p"))
    go(to_partner(p_all.at[me], p_all.at[me], "p"))
    go(to_far(y_rows(me), y_rows(me), "y"))
    go(to_partner(y_rows(me), y_rows(me), "y"))
    loads["t"].wait()
    for k in range(T_CHUNKS):
        t_all[span(me * NB + k * TR, TR), :] = t_st[k * TR:(k + 1) * TR, :].astype(BF16)
    for k in range(T_CHUNKS):
        go(to_far(t_rows(me, k), t_rows(me, k), ("t", k)))
    for k in range(T_CHUNKS):
        go(to_partner(t_rows(me, k), t_rows(me, k), ("t", k)))
    for name in ("c2", "x", "left", "right", "q"):
        loads[name].wait()
    c2_all[span(me * MB, MB), :] = kern[MB + NB:2 * MB + NB, :].astype(BF16)
    x_all[span(me * NB, NB), :] = kern[MB:MB + NB, :D].astype(BF16)
    c1_rows[:NB, :M] = g_all[:NB, :].astype(BF16)
    c1_rows[:NB, M:] = g_all[NB:2 * NB, :].astype(BF16)
    for k, piece in enumerate(c2_pieces(me, partner, core)):
        go(to_far(piece, piece, ("c2", k)))
    for k, (src, dst) in enumerate(zip(c1_quads(0, partner, core), c1_quads(NB, partner, core))):
        go(to_far(src, dst, ("c1 quad", k)))
    for k in range(4):
        go(to_far(c1_strip(0, me, k), c1_strip(NB, me, k), ("c1 strip", k)))
    for k in range(2):
        go(to_far(x_half(me, k), x_half(me, k), ("x", k)))
    go(to_partner(c2_rows(me), c2_rows(me), "c2"))
    go(to_partner(x_rows(me), x_rows(me), "x"))
    go(to_partner(c1_rows.at[:NB, span(far_partner * NB, NB)], c1_side, "c1"))

    def mirror(src, src_row, src_col, dst, dst_row, dst_col, size):
        for i in range(size // LANES):
            for j in range(size // LANES):
                tile = src[span(src_row + i * LANES, LANES), span(src_col + j * LANES, LANES)]
                dst[span(dst_row + j * LANES, LANES), span(dst_col + i * LANES, LANES)] = (
                    tile.astype(F32).T.astype(BF16))

    mirror(c1_rows, 0, far * NB, c1_rows, NB, me * NB, NB)
    partner_arrived(c1_side, "c1")
    mirror(c1_side, 0, 0, c1_rows, NB, partner * NB, NB)
    partner_arrived(c2_rows(partner), "c2")
    mirror(c2_all, chip * 2 * MB, (1 - chip) * 2 * MB, c2_all, (1 - chip) * 2 * MB, chip * 2 * MB, 2 * MB)
    partner_arrived(y_rows(partner), "y")
    partner_arrived(p_all.at[partner], "p")
    partner_arrived(x_rows(partner), "x")

    def forward(ref, name):
        far_arrived(ref, name)
        go(to_partner(ref, ref, ("far " + name[0], name[1]) if isinstance(name, tuple) else "far " + name))

    def gram(owner):
        for n in range(4):
            g = lax.dot_general(x_all[span(owner * NB, NB), :], y_all[n * 256:(n + 1) * 256, :],
                                (((1,), (1,)), ((), ())), preferred_element_type=F32)
            g_all[span(owner * NB, NB), n * 256:(n + 1) * 256] = (2.0 * ALPHA) * g

    def grams(first, second):
        def one(i, carry):
            gram(first + i * (second - first))
            return carry
        lax.fori_loop(0, 2, one, 0)

    forward(y_rows(far), "y")
    forward(p_all.at[far], "p")
    partner_arrived(y_rows(far_partner), "far y")
    partner_arrived(p_all.at[far_partner], "far p")
    for owner in range(4):
        for i in range(NB // LANES):
            block = jnp.broadcast_to(p_all[owner, i:i + 1, :], (LANES, LANES))
            p_b[owner * NB + i * LANES:owner * NB + (i + 1) * LANES, :] = block.T
    grams(me, partner)
    for k in range(T_CHUNKS):
        partner_arrived(t_rows(partner, k), ("t", k))
    for k in range(T_CHUNKS):
        forward(t_rows(far, k), ("t", k))
    for k in range(T_CHUNKS):
        partner_arrived(t_rows(far_partner, k), ("far t", k))

    scale = LOG2E / eps_ref[0, 0]

    def a_rows(a_all, local, base, rows=CH):
        for n in range(4):
            a_all[span(base, rows), n * 256:(n + 1) * 256] = jnp.dot(
                c1_rows[span(local, rows), :], t_all[:, n * 256:(n + 1) * 256], preferred_element_type=F32).astype(BF16)

    def scores(a_all, base, raw):
        for n in range(4):
            b = jnp.dot(a_all[span(base, CH), :], c2_all[:, n * 256:(n + 1) * 256], preferred_element_type=F32)
            t_st[raw:raw + CH, n * 256:(n + 1) * 256] = g_all[span(base, CH), n * 256:(n + 1) * 256] + (2.0 * (1.0 - ALPHA)) * b

    def products(a_all, base):
        for n in range(4):
            b = jnp.dot(a_all[span(base, CH), :], c2_all[:, n * 256:(n + 1) * 256], preferred_element_type=F32)
            g_all[span(base, CH), n * 256:(n + 1) * 256] = (2.0 * (1.0 - ALPHA)) * b

    def late_scores(base, raw):
        for n in range(4):
            g = (2.0 * ALPHA) * lax.dot_general(x_all[span(base, CH), :], y_all[n * 256:(n + 1) * 256, :],
                                                (((1,), (1,)), ((), ())), preferred_element_type=F32)
            t_st[raw:raw + CH, n * 256:(n + 1) * 256] = g + g_all[span(base, CH), n * 256:(n + 1) * 256]
            g_all[span(base, CH), n * 256:(n + 1) * 256] = g

    def form(base, raw):
        acc = [acc_ref[:, col(j)] for j in range(COLS)]
        lead = 64
        group = FORM_GROUP
        shape = (group // 8, 8, LANES)
        for row in range(-2 * lead, CH, group):
            top = row + 2 * lead
            if top < CH:
                peak = tree(jnp.maximum, [t_st[raw + top:raw + top + group, col(j)] for j in range(COLS)])
                peak_b[raw + top:raw + top + group, :] = jnp.broadcast_to(jnp.max(peak, axis=1, keepdims=True), (group, LANES))
            mid = row + lead
            if 0 <= mid < CH:
                here = pl.ds(hint(base + mid, group), group)
                peak = peak_b[raw + mid:raw + mid + group, :]
                vals = [jnp.exp2((t_st[raw + mid:raw + mid + group, col(j)] - peak) * scale) for j in range(COLS)]
                for j in range(COLS):
                    kern[here, col(j)] = vals[j]
                    t_st[raw + mid:raw + mid + group, col(j)] = vals[j]
                total = jnp.sum(tree(jnp.add, vals), axis=1, keepdims=True)
                first_b[raw + mid:raw + mid + group, :] = p_b[here, :] / total
            if row >= 0:
                u = first_b[raw + row:raw + row + group, :].reshape(shape)
                acc = [acc[j] + jnp.sum(t_st[raw + row:raw + row + group, col(j)].reshape(shape) * u, axis=0)
                       for j in range(COLS)]
        for j in range(COLS):
            acc_ref[:, col(j)] = acc[j]

    def b_rows(a_all, bases, ready=None):
        raws = (raw0, raw1)
        for i, base in enumerate(bases):
            if ready and ready[i]:
                ready[i]()
            scores(a_all, base, raws[i % 2])
            if i:
                form(bases[i - 1], raws[(i - 1) % 2])
        form(bases[-1], raws[(len(bases) - 1) % 2])

    def a_slice(a_all, base):
        return a_all.at[span(base, CH), :]

    def my_base(i):
        return jnp.where(i < 2, me * NB + i * CH, far * NB + (i - 2) * CH)

    def their_base(i):
        return jnp.where(i < 2, partner * NB + i * CH, far_partner * NB + (i - 2) * CH)

    mine = [my_base(i) for i in range(4)]
    theirs = [their_base(i) for i in range(4)]

    def share(a_all, name, start, stop):
        slot = SIDE.names[(name, 0)]

        def piece(i):
            ref = a_slice(a_all, my_base(i))
            return pltpu.make_async_remote_copy(
                src_ref=ref, dst_ref=ref, send_sem=side_send.at[slot + i], recv_sem=side_recv.at[slot + i],
                device_id={"rows": partner}, device_id_type=pl.DeviceIdType.MESH)

        def step(i, carry):
            a_rows(a_all, i * CH, my_base(i))
            piece(i).start()
            return carry
        if stop - start == 1:
            step(start, 0)
        else:
            lax.fori_loop(start, stop, step, 0)
        for i in range(start, stop):
            sends.append(piece(i))

    def b_groups(a_all, count, arrived):
        def group(g, carry):
            @pl.when(g == 1)
            def _():
                arrived()
            b_rows(a_all, [jnp.where(g == 0, mine[i], theirs[i]) for i in range(count)])
            return carry
        lax.fori_loop(0, 2, group, 0)

    acc_ref[...] = jnp.zeros_like(acc_ref)
    share(a1_all, "a1", 0, 2)
    for k, piece in enumerate(c2_pieces(far, far_partner, core)):
        forward(piece, ("c2", k))
    for k, piece in enumerate(c2_pieces(far_partner, far, 1 - core)):
        partner_arrived(piece, ("far c2", k))
    first = (1 - chip) * 2 * MB
    second = first + MB
    for base in (first, second):
        mirror(c2_all, base, base + 128, c2_all, base + 128, base, 128)
    mirror(c2_all, second + 128, first, c2_all, first, second + 128, 128)
    mirror(c2_all, second + 128, first + 128, c2_all, first + 128, second + 128, 128)
    mirror(c2_all, first, second, c2_all, second, first, 128)
    mirror(c2_all, first + 128, second, c2_all, second, first + 128, 128)

    def a1_arrived():
        for i in range(2):
            partner_arrived(a_slice(a1_all, theirs[i]), ("a1", i))
    b_groups(a1_all, 2, a1_arrived)
    for k, piece in enumerate(c1_quads(NB, far_partner, core)):
        far_arrived(piece, ("c1 quad", k))
        go(to_partner(piece, quad_side.at[k * HALF:(k + 1) * HALF, :], ("c1 quad", k)))
    for k in range(2):
        partner_arrived(quad_side.at[k * HALF:(k + 1) * HALF, :], ("c1 quad", k))
    mirror(quad_side, 0, 0, c1_rows, NB, far_partner * NB + HALF, HALF)
    mirror(quad_side, HALF, 0, c1_rows, NB + (1 - core) * HALF, far_partner * NB + (1 - core) * HALF, HALF)

    def a_early(i, carry):
        rows = span(NB + i * CH, CH)
        for n in range(4):
            cols = slice(n * 256, (n + 1) * 256)
            kern[span(far * NB + i * CH, CH), cols] = (
                jnp.dot(c1_rows[rows, span(chip * 2 * NB, 2 * NB)], t_all[span(chip * 2 * NB, 2 * NB), cols],
                        preferred_element_type=F32)
                + jnp.dot(c1_rows[rows, span(far_partner * NB, NB)], t_all[span(far_partner * NB, NB), cols],
                          preferred_element_type=F32))
        return carry
    lax.fori_loop(0, 2, a_early, 0)

    def a_late(i):
        base = mine[2 + i]
        for n in range(4):
            cols = slice(n * 256, (n + 1) * 256)
            a1_all[span(base, CH), cols] = (
                kern[span(base, CH), cols]
                + jnp.dot(c1_rows[NB + i * CH:NB + (i + 1) * CH, span(far * NB, NB)], t_all[span(far * NB, NB), cols],
                          preferred_element_type=F32)).astype(BF16)
        go(to_partner(a_slice(a1_all, base), a_slice(a1_all, base), ("a1", 2 + i)))

    for i in range(2):
        for k in (2 * i, 2 * i + 1):
            far_arrived(c1_strip(NB, far, k), ("c1 strip", k))
            for below in range(k + 1, 4):
                mirror(c1_rows, NB + k * 128, far * NB + below * 128, c1_rows, NB + below * 128, far * NB + k * 128, 128)
        a_late(i)
        products(a1_all, mine[2 + i])
    for i in range(2):
        partner_arrived(a_slice(a1_all, theirs[2 + i]), ("a1", 2 + i))
        products(a1_all, theirs[2 + i])
    for half in range(2):
        forward(x_half(far, half), ("x", half))
        late_scores(mine[2 + half], raw0)
        form(mine[2 + half], raw0)
        partner_arrived(x_half(far_partner, half), ("far x", half))
        late_scores(theirs[2 + half], raw1)
        form(theirs[2 + half], raw1)
    store_col_scale([acc_ref[:, col(j)] for j in range(COLS)], v_ref, q_ref)
    sweeps(SWEEPS - 1, kern, p_b, u_b, v_ref, q_ref, 32)

    for copy in sends:
        copy.wait_send()
    sends.clear()

    def next_plan(i, carry):
        row = hint(i * 64, 64)
        for j, t in scaled_rows(kern, u_b, v_ref, row, 64):
            t_all[pl.ds(row, 64), col(j)] = t.astype(BF16)
        return carry
    lax.fori_loop(0, N // 64, next_plan, 0)

    acc_ref[...] = jnp.zeros_like(acc_ref)
    first_slot = SIDE.names[("a2", 0)]

    def a2_piece(i):
        ref = a2_all.at[span(jnp.where(i == 0, me, far) * NB, NB), :]
        return pltpu.make_async_remote_copy(
            src_ref=ref, dst_ref=ref, send_sem=side_send.at[first_slot + i], recv_sem=side_recv.at[first_slot + i],
            device_id={"rows": partner}, device_id_type=pl.DeviceIdType.MESH)

    def a2_step(i, carry):
        a_rows(a2_all, i * NB, jnp.where(i == 0, me, far) * NB, NB)
        a2_piece(i).start()
        return carry
    lax.fori_loop(0, 2, a2_step, 0)
    sends.extend((a2_piece(0), a2_piece(1)))

    def a2_arrived():
        for i in range(2):
            a2_piece(i).wait_recv()
    b_groups(a2_all, 4, a2_arrived)
    store_col_scale([acc_ref[:, col(j)] for j in range(COLS)], v_ref, q_ref)
    sweeps(SWEEPS - 1, kern, p_b, u_b, v_ref, q_ref, 16)


    def result(i, carry):
        row = hint(i * 64, 64)
        for j, t in scaled_rows(kern, u_b, v_ref, hint(me * NB + row, 64), 64):
            out_ref[pl.ds(row, 64), col(j)] = t
        return carry
    lax.fori_loop(0, NB // 64, result, 0)
    for copy in sends:
        copy.wait_send()


def solution(mesh):
    vmem = pl.BlockSpec(memory_space=pltpu.VMEM)
    hbm = pl.BlockSpec(memory_space=pl.ANY)
    smem = pl.BlockSpec(memory_space=pltpu.SMEM)

    def local_fgw(cost_src, cost_tgt, plan_init, mass_src, mass_tgt, feat_src, feat_tgt, epsilon):
        return pl.pallas_call(
            kernel,
            out_shape=pltpu.VMEM((NB, M), F32),
            in_specs=[hbm] * 7 + [smem],
            out_specs=vmem,
            scratch_shapes=[
                pltpu.VMEM((1, M), F32),
                pltpu.VMEM((NB, M), F32),
                pltpu.VMEM((N, M), BF16),
                pltpu.VMEM((2 * NB, N), BF16),
                pltpu.VMEM((NB, NB), BF16),
                pltpu.VMEM((2 * HALF, HALF), BF16),
                pltpu.VMEM((M, M), BF16),
                pltpu.VMEM((M, D), BF16),
                pltpu.VMEM((N, D), BF16),
                pltpu.VMEM((N, M), F32),
                pltpu.VMEM((N, M), BF16),
                pltpu.VMEM((N, M), BF16),
                pltpu.VMEM((N, M), F32),
                pltpu.VMEM((4, NB // LANES, LANES), F32),
                pltpu.VMEM((N, LANES), F32),
                pltpu.VMEM((N, LANES), F32),
                pltpu.VMEM((2 * CH, LANES), F32),
                pltpu.VMEM((2 * CH, LANES), F32),
                pltpu.VMEM((8, M), F32),
                pltpu.VMEM((8, M), F32),
                pltpu.SemaphoreType.DMA((8,)),
                pltpu.SemaphoreType.DMA((len(LINK.names),)),
                pltpu.SemaphoreType.DMA((len(LINK.names),)),
                pltpu.SemaphoreType.DMA((len(SIDE.names),)),
                pltpu.SemaphoreType.DMA((len(SIDE.names),)),
            ],
            compiler_params=pltpu.CompilerParams(
                collective_id=0, has_side_effects=True, vmem_limit_bytes=54000 * 1024),
        )(*(pltpu.with_memory_space_constraint(x, pltpu.HBM) for x in (
            cost_src, cost_tgt, plan_init, mass_src.reshape(NB // LANES, LANES), mass_tgt.reshape(1, M),
            feat_src, feat_tgt)), epsilon.reshape(1, 1))

    row_spec = P(('pairs', 'rows'), None)
    vec_spec = P(('pairs', 'rows'))
    in_specs = (row_spec, row_spec, row_spec, vec_spec, P('pairs'), row_spec, row_spec, P())
    return jax.shard_map(local_fgw, mesh=mesh, in_specs=in_specs, out_specs=row_spec, check_vma=False)
```

```python
import jax
import jax.numpy as jnp
from jax import lax
from jax.experimental import pallas as pl
from jax.experimental.pallas import tpu as pltpu
from jax.sharding import PartitionSpec as P

ALPHA = 0.5
OUTER_STEPS = 2
SWEEPS = 10
LOG2E = 1.4426950408889634

N = 2048
M = 1024
D = 256
NB = 512
MB = 256
F32 = jnp.float32
BF16 = jnp.bfloat16
LANES = 128
COLS = M // LANES

T_CHUNKS = 2
TR = NB // T_CHUNKS
CH = 256
HALF = NB // 2
FORM_GROUP = 32


class Slots:
    def __init__(self):
        self.names = {}

    def __call__(self, name):
        return self.names.setdefault(name, len(self.names))


LINK = Slots()
SIDE = Slots()
for k in range(T_CHUNKS):
    LINK(("t", k)), SIDE(("t", k)), SIDE(("far t", k))
for k in range(4):
    LINK(("c2", k)), SIDE(("far c2", k)), LINK(("c1 strip", k))
for k in range(4):
    SIDE(("a1", k))
for k in range(2):
    SIDE(("a2", k))
for k in range(2):
    LINK(("c1 quad", k)), SIDE(("c1 quad", k))
for k in range(2):
    LINK(("x", k)), SIDE(("far x", k))
for name in ("y", "p"):
    LINK(name), SIDE(name), SIDE("far " + name)
SIDE("c2"), SIDE("c1"), SIDE("x")


def hint(value, multiple):
    return value if isinstance(value, int) else pl.multiple_of(value, multiple)


def span(start, size):
    return pl.ds(hint(start, size), size)


def col(j):
    return slice(j * LANES, (j + 1) * LANES)


def tree(op, parts):
    while len(parts) > 1:
        parts = [op(parts[i], parts[i + 1]) for i in range(0, len(parts), 2)]
    return parts[0]


def store_col_scale(acc, v_ref, q_ref):
    for j in range(COLS):
        col_sum = jnp.sum(acc[j], axis=0, keepdims=True)
        v_ref[:, col(j)] = jnp.broadcast_to(q_ref[:, col(j)] / col_sum, (8, LANES))


def sweeps(count, kern, plan_b, u_b, v_ref, q_ref, group):
    lead = 128
    shape = (group // 8, 8, LANES)

    def sweep(_, carry):
        v = [v_ref[:, col(j)][None] for j in range(COLS)]

        def tile(row, j):
            return kern[row:row + group, col(j)].reshape(shape)

        acc = [jnp.zeros((8, LANES), F32) for _ in range(COLS)]
        for row in range(-lead, N, group):
            top = row + lead
            if top < N:
                total = tree(jnp.add, [tile(top, j) * v[j] for j in range(COLS)])
                u = plan_b[top:top + group, :].reshape(shape) / jnp.sum(total, axis=2, keepdims=True)
                u_b[top:top + group, :] = u.reshape(group, LANES)
            if row >= 0:
                u = u_b[row:row + group, :].reshape(shape)
                acc = [acc[j] + jnp.sum(tile(row, j) * u, axis=0) for j in range(COLS)]
        store_col_scale(acc, v_ref, q_ref)
        return carry

    lax.fori_loop(0, count, sweep, 0)


def scaled_rows(kern, u_b, v_ref, row, count):
    u = u_b[pl.ds(row, count), :].reshape(count // 8, 8, LANES)
    for j in range(COLS):
        k = kern[pl.ds(row, count), col(j)].reshape(count // 8, 8, LANES)
        yield j, (u * k * v_ref[:, col(j)][None]).reshape(count, LANES)


def kernel(c1_hbm, c2_hbm, t0_hbm, p_hbm, q_hbm, x_hbm, y_hbm, eps_ref, out_ref,
           q_ref, t_st, t_all, c1_rows, c1_side, quad_side, c2_all, y_all, x_all, g_all, a1_all, a2_all,
           kern, p_all, p_b, u_b, peak_b, first_b, acc_ref, v_ref,
           load_sem, link_send, link_recv, side_send, side_recv):
    raw0, raw1 = 0, CH
    current = [None]

    def mark(name):
        if current[0] is not None:
            current[0].__exit__(None, None, None)
            current[0] = None
        if name:
            current[0] = jax.named_scope(name)
            current[0].__enter__()

    me = lax.axis_index("rows")
    chip = me // 2
    core = me % 2
    partner = chip * 2 + (1 - core)
    far = (1 - chip) * 2 + core
    far_partner = (1 - chip) * 2 + (1 - core)

    y_st, x_st, c2_st = kern.at[:MB, :D], kern.at[MB:MB + NB, :D], kern.at[MB + NB:2 * MB + NB, :]
    loads = {}
    for i, (name, src, dst) in enumerate((
            ("y", y_hbm, y_st), ("p", p_hbm, p_all.at[me]), ("t", t0_hbm, t_st), ("c2", c2_hbm, c2_st), ("x", x_hbm, x_st),
            ("left", c1_hbm.at[:, :M], g_all.at[:NB]), ("right", c1_hbm.at[:, M:], g_all.at[NB:2 * NB]), ("q", q_hbm, q_ref))):
        loads[name] = pltpu.make_async_copy(src, dst, load_sem.at[i])
        loads[name].start()

    mark("barrier")
    barrier = pltpu.get_barrier_semaphore()
    for peer in (partner, far):
        pl.semaphore_signal(barrier, inc=1, device_id={"rows": peer}, device_id_type=pl.DeviceIdType.MESH)
    pl.semaphore_wait(barrier, 2)

    def to_far(src, dst, name):
        slot = LINK.names[name]
        return pltpu.make_async_remote_copy(
            src_ref=src, dst_ref=dst, send_sem=link_send.at[slot], recv_sem=link_recv.at[slot],
            device_id={"rows": far}, device_id_type=pl.DeviceIdType.MESH)

    def to_partner(src, dst, name):
        slot = SIDE.names[name]
        return pltpu.make_async_remote_copy(
            src_ref=src, dst_ref=dst, send_sem=side_send.at[slot], recv_sem=side_recv.at[slot],
            device_id={"rows": partner}, device_id_type=pl.DeviceIdType.MESH)

    sends = []

    def go(copy):
        copy.start()
        sends.append(copy)

    def far_arrived(ref, name):
        to_far(ref, ref, name).wait_recv()

    def partner_arrived(ref, name):
        to_partner(ref, ref, name).wait_recv()

    def t_rows(owner, k):
        return t_all.at[span(owner * NB + k * TR, TR), :]

    def c2_rows(owner):
        return c2_all.at[span(owner * MB, MB), :]

    def c2_pieces(owner, other, which):
        return (
            c2_all.at[span(owner * MB + 128, 128), span(other * MB, 128)],
            c2_all.at[span(owner * MB + which * 128, 128), span(other * MB + which * 128, 128)],
            c2_all.at[span(owner * MB, 128), span(owner * MB, MB)],
            c2_all.at[span(owner * MB + 128, 128), span(owner * MB + 128, 128)])

    def y_rows(owner):
        return y_all.at[span(owner * MB, MB), :]

    def x_rows(owner):
        return x_all.at[span(owner * NB, NB), :]

    def x_half(owner, k):
        return x_all.at[span(owner * NB + k * CH, CH), :]

    def c1_quads(base, other, which):
        return (c1_rows.at[base + HALF:base + NB, span(other * NB, HALF)],
                c1_rows.at[span(base + which * HALF, HALF), span(other * NB + which * HALF, HALF)])

    def c1_strip(base, owner, k):
        return c1_rows.at[base + k * 128:base + (k + 1) * 128, pl.ds(hint(owner * NB + k * 128, 128), NB - k * 128)]

    mark("cast_y")
    loads["y"].wait()
    y_all[span(me * MB, MB), :] = kern[:MB, :D].astype(BF16)
    loads["p"].wait()
    go(to_far(p_all.at[me], p_all.at[me], "p"))
    go(to_partner(p_all.at[me], p_all.at[me], "p"))
    go(to_far(y_rows(me), y_rows(me), "y"))
    go(to_partner(y_rows(me), y_rows(me), "y"))
    mark("cast_t")
    loads["t"].wait()
    for k in range(T_CHUNKS):
        t_all[span(me * NB + k * TR, TR), :] = t_st[k * TR:(k + 1) * TR, :].astype(BF16)
    for k in range(T_CHUNKS):
        go(to_far(t_rows(me, k), t_rows(me, k), ("t", k)))
    for k in range(T_CHUNKS):
        go(to_partner(t_rows(me, k), t_rows(me, k), ("t", k)))
    mark("cast_rest")
    for name in ("c2", "x", "left", "right", "q"):
        loads[name].wait()
    c2_all[span(me * MB, MB), :] = kern[MB + NB:2 * MB + NB, :].astype(BF16)
    x_all[span(me * NB, NB), :] = kern[MB:MB + NB, :D].astype(BF16)
    c1_rows[:NB, :M] = g_all[:NB, :].astype(BF16)
    c1_rows[:NB, M:] = g_all[NB:2 * NB, :].astype(BF16)
    for k, piece in enumerate(c2_pieces(me, partner, core)):
        go(to_far(piece, piece, ("c2", k)))
    for k, (src, dst) in enumerate(zip(c1_quads(0, partner, core), c1_quads(NB, partner, core))):
        go(to_far(src, dst, ("c1 quad", k)))
    for k in range(4):
        go(to_far(c1_strip(0, me, k), c1_strip(NB, me, k), ("c1 strip", k)))
    for k in range(2):
        go(to_far(x_half(me, k), x_half(me, k), ("x", k)))
    go(to_partner(c2_rows(me), c2_rows(me), "c2"))
    go(to_partner(x_rows(me), x_rows(me), "x"))
    go(to_partner(c1_rows.at[:NB, span(far_partner * NB, NB)], c1_side, "c1"))

    def mirror(src, src_row, src_col, dst, dst_row, dst_col, size):
        for i in range(size // LANES):
            for j in range(size // LANES):
                tile = src[span(src_row + i * LANES, LANES), span(src_col + j * LANES, LANES)]
                dst[span(dst_row + j * LANES, LANES), span(dst_col + i * LANES, LANES)] = (
                    tile.astype(F32).T.astype(BF16))

    mark("mirrors")
    mirror(c1_rows, 0, far * NB, c1_rows, NB, me * NB, NB)
    partner_arrived(c1_side, "c1")
    mirror(c1_side, 0, 0, c1_rows, NB, partner * NB, NB)
    partner_arrived(c2_rows(partner), "c2")
    mirror(c2_all, chip * 2 * MB, (1 - chip) * 2 * MB, c2_all, (1 - chip) * 2 * MB, chip * 2 * MB, 2 * MB)
    partner_arrived(y_rows(partner), "y")
    partner_arrived(p_all.at[partner], "p")
    partner_arrived(x_rows(partner), "x")

    def forward(ref, name):
        far_arrived(ref, name)
        go(to_partner(ref, ref, ("far " + name[0], name[1]) if isinstance(name, tuple) else "far " + name))

    def gram(owner):
        for n in range(4):
            g = lax.dot_general(x_all[span(owner * NB, NB), :], y_all[n * 256:(n + 1) * 256, :],
                                (((1,), (1,)), ((), ())), preferred_element_type=F32)
            g_all[span(owner * NB, NB), n * 256:(n + 1) * 256] = (2.0 * ALPHA) * g

    def grams(first, second):
        def one(i, carry):
            gram(first + i * (second - first))
            return carry
        lax.fori_loop(0, 2, one, 0)

    mark("wait_y")
    forward(y_rows(far), "y")
    forward(p_all.at[far], "p")
    partner_arrived(y_rows(far_partner), "far y")
    partner_arrived(p_all.at[far_partner], "far p")
    mark("p_b_gram")
    for owner in range(4):
        for i in range(NB // LANES):
            block = jnp.broadcast_to(p_all[owner, i:i + 1, :], (LANES, LANES))
            p_b[owner * NB + i * LANES:owner * NB + (i + 1) * LANES, :] = block.T
    grams(me, partner)
    mark("wait_t")
    for k in range(T_CHUNKS):
        partner_arrived(t_rows(partner, k), ("t", k))
    for k in range(T_CHUNKS):
        forward(t_rows(far, k), ("t", k))
    for k in range(T_CHUNKS):
        partner_arrived(t_rows(far_partner, k), ("far t", k))

    scale = LOG2E / eps_ref[0, 0]

    def a_rows(a_all, local, base, rows=CH):
        for n in range(4):
            a_all[span(base, rows), n * 256:(n + 1) * 256] = jnp.dot(
                c1_rows[span(local, rows), :], t_all[:, n * 256:(n + 1) * 256], preferred_element_type=F32).astype(BF16)

    def scores(a_all, base, raw):
        for n in range(4):
            b = jnp.dot(a_all[span(base, CH), :], c2_all[:, n * 256:(n + 1) * 256], preferred_element_type=F32)
            t_st[raw:raw + CH, n * 256:(n + 1) * 256] = g_all[span(base, CH), n * 256:(n + 1) * 256] + (2.0 * (1.0 - ALPHA)) * b

    def products(a_all, base):
        for n in range(4):
            b = jnp.dot(a_all[span(base, CH), :], c2_all[:, n * 256:(n + 1) * 256], preferred_element_type=F32)
            g_all[span(base, CH), n * 256:(n + 1) * 256] = (2.0 * (1.0 - ALPHA)) * b

    def late_scores(base, raw):
        for n in range(4):
            g = (2.0 * ALPHA) * lax.dot_general(x_all[span(base, CH), :], y_all[n * 256:(n + 1) * 256, :],
                                                (((1,), (1,)), ((), ())), preferred_element_type=F32)
            t_st[raw:raw + CH, n * 256:(n + 1) * 256] = g + g_all[span(base, CH), n * 256:(n + 1) * 256]
            g_all[span(base, CH), n * 256:(n + 1) * 256] = g

    def form(base, raw):
        acc = [acc_ref[:, col(j)] for j in range(COLS)]
        lead = 64
        group = FORM_GROUP
        shape = (group // 8, 8, LANES)
        for row in range(-2 * lead, CH, group):
            top = row + 2 * lead
            if top < CH:
                peak = tree(jnp.maximum, [t_st[raw + top:raw + top + group, col(j)] for j in range(COLS)])
                peak_b[raw + top:raw + top + group, :] = jnp.broadcast_to(jnp.max(peak, axis=1, keepdims=True), (group, LANES))
            mid = row + lead
            if 0 <= mid < CH:
                here = pl.ds(hint(base + mid, group), group)
                peak = peak_b[raw + mid:raw + mid + group, :]
                vals = [jnp.exp2((t_st[raw + mid:raw + mid + group, col(j)] - peak) * scale) for j in range(COLS)]
                for j in range(COLS):
                    kern[here, col(j)] = vals[j]
                    t_st[raw + mid:raw + mid + group, col(j)] = vals[j]
                total = jnp.sum(tree(jnp.add, vals), axis=1, keepdims=True)
                first_b[raw + mid:raw + mid + group, :] = p_b[here, :] / total
            if row >= 0:
                u = first_b[raw + row:raw + row + group, :].reshape(shape)
                acc = [acc[j] + jnp.sum(t_st[raw + row:raw + row + group, col(j)].reshape(shape) * u, axis=0)
                       for j in range(COLS)]
        for j in range(COLS):
            acc_ref[:, col(j)] = acc[j]

    def b_rows(a_all, bases, ready=None):
        raws = (raw0, raw1)
        for i, base in enumerate(bases):
            if ready and ready[i]:
                ready[i]()
            if i:
                form(bases[i - 1], raws[(i - 1) % 2])
            scores(a_all, base, raws[i % 2])
        form(bases[-1], raws[(len(bases) - 1) % 2])

    def a_slice(a_all, base):
        return a_all.at[span(base, CH), :]

    def my_base(i):
        return jnp.where(i < 2, me * NB + i * CH, far * NB + (i - 2) * CH)

    def their_base(i):
        return jnp.where(i < 2, partner * NB + i * CH, far_partner * NB + (i - 2) * CH)

    mine = [my_base(i) for i in range(4)]
    theirs = [their_base(i) for i in range(4)]

    def share(a_all, name, start, stop):
        slot = SIDE.names[(name, 0)]

        def piece(i):
            ref = a_slice(a_all, my_base(i))
            return pltpu.make_async_remote_copy(
                src_ref=ref, dst_ref=ref, send_sem=side_send.at[slot + i], recv_sem=side_recv.at[slot + i],
                device_id={"rows": partner}, device_id_type=pl.DeviceIdType.MESH)

        def step(i, carry):
            a_rows(a_all, i * CH, my_base(i))
            piece(i).start()
            return carry
        if stop - start == 1:
            step(start, 0)
        else:
            lax.fori_loop(start, stop, step, 0)
        for i in range(start, stop):
            sends.append(piece(i))

    def b_groups(a_all, count, arrived):
        def group(g, carry):
            @pl.when(g == 1)
            def _():
                arrived()
            b_rows(a_all, [jnp.where(g == 0, mine[i], theirs[i]) for i in range(count)])
            return carry
        lax.fori_loop(0, 2, group, 0)

    acc_ref[...] = jnp.zeros_like(acc_ref)
    mark("a_own")
    share(a1_all, "a1", 0, 2)
    mark("wait_c2")
    for k, piece in enumerate(c2_pieces(far, far_partner, core)):
        forward(piece, ("c2", k))
    for k, piece in enumerate(c2_pieces(far_partner, far, 1 - core)):
        partner_arrived(piece, ("far c2", k))
    mark("c2_mirror")
    first = (1 - chip) * 2 * MB
    second = first + MB
    for base in (first, second):
        mirror(c2_all, base, base + 128, c2_all, base + 128, base, 128)
    mirror(c2_all, second + 128, first, c2_all, first, second + 128, 128)
    mirror(c2_all, second + 128, first + 128, c2_all, first + 128, second + 128, 128)
    mirror(c2_all, first, second, c2_all, second, first, 128)
    mirror(c2_all, first + 128, second, c2_all, second, first + 128, 128)
    mark("b_own")

    def a1_arrived():
        for i in range(2):
            partner_arrived(a_slice(a1_all, theirs[i]), ("a1", i))
    b_groups(a1_all, 2, a1_arrived)
    mark("wait_quads")
    for k, piece in enumerate(c1_quads(NB, far_partner, core)):
        far_arrived(piece, ("c1 quad", k))
        go(to_partner(piece, quad_side.at[k * HALF:(k + 1) * HALF, :], ("c1 quad", k)))
    for k in range(2):
        partner_arrived(quad_side.at[k * HALF:(k + 1) * HALF, :], ("c1 quad", k))
    mark("quad_mirror")
    mirror(quad_side, 0, 0, c1_rows, NB, far_partner * NB + HALF, HALF)
    mirror(quad_side, HALF, 0, c1_rows, NB + (1 - core) * HALF, far_partner * NB + (1 - core) * HALF, HALF)
    mark("a_early")

    def a_early(i, carry):
        rows = span(NB + i * CH, CH)
        for n in range(4):
            cols = slice(n * 256, (n + 1) * 256)
            kern[span(far * NB + i * CH, CH), cols] = (
                jnp.dot(c1_rows[rows, span(chip * 2 * NB, 2 * NB)], t_all[span(chip * 2 * NB, 2 * NB), cols],
                        preferred_element_type=F32)
                + jnp.dot(c1_rows[rows, span(far_partner * NB, NB)], t_all[span(far_partner * NB, NB), cols],
                          preferred_element_type=F32))
        return carry
    lax.fori_loop(0, 2, a_early, 0)

    def a_late(i):
        base = mine[2 + i]
        for n in range(4):
            cols = slice(n * 256, (n + 1) * 256)
            a1_all[span(base, CH), cols] = (
                kern[span(base, CH), cols]
                + jnp.dot(c1_rows[NB + i * CH:NB + (i + 1) * CH, span(far * NB, NB)], t_all[span(far * NB, NB), cols],
                          preferred_element_type=F32)).astype(BF16)
        go(to_partner(a_slice(a1_all, base), a_slice(a1_all, base), ("a1", 2 + i)))

    for i in range(2):
        mark("wait_strips%d" % i)
        for k in (2 * i, 2 * i + 1):
            far_arrived(c1_strip(NB, far, k), ("c1 strip", k))
            for below in range(k + 1, 4):
                mirror(c1_rows, NB + k * 128, far * NB + below * 128, c1_rows, NB + below * 128, far * NB + k * 128, 128)
        mark("a_far%d" % i)
        a_late(i)
        mark("products%d" % i)
        products(a1_all, mine[2 + i])
    mark("products_theirs")
    for i in range(2):
        partner_arrived(a_slice(a1_all, theirs[2 + i]), ("a1", 2 + i))
        products(a1_all, theirs[2 + i])
    mark("late")
    for half in range(2):
        forward(x_half(far, half), ("x", half))
        late_scores(mine[2 + half], raw0)
        form(mine[2 + half], raw0)
        partner_arrived(x_half(far_partner, half), ("far x", half))
        late_scores(theirs[2 + half], raw1)
        form(theirs[2 + half], raw1)
    store_col_scale([acc_ref[:, col(j)] for j in range(COLS)], v_ref, q_ref)
    mark("sweeps")
    sweeps(SWEEPS - 1, kern, p_b, u_b, v_ref, q_ref, 32)

    mark("next_plan")
    for copy in sends:
        copy.wait_send()
    sends.clear()

    def next_plan(i, carry):
        row = hint(i * 64, 64)
        for j, t in scaled_rows(kern, u_b, v_ref, row, 64):
            t_all[pl.ds(row, 64), col(j)] = t.astype(BF16)
        return carry
    lax.fori_loop(0, N // 64, next_plan, 0)

    acc_ref[...] = jnp.zeros_like(acc_ref)
    mark("a_2")
    first_slot = SIDE.names[("a2", 0)]

    def a2_piece(i):
        ref = a2_all.at[span(jnp.where(i == 0, me, far) * NB, NB), :]
        return pltpu.make_async_remote_copy(
            src_ref=ref, dst_ref=ref, send_sem=side_send.at[first_slot + i], recv_sem=side_recv.at[first_slot + i],
            device_id={"rows": partner}, device_id_type=pl.DeviceIdType.MESH)

    def a2_step(i, carry):
        a_rows(a2_all, i * NB, jnp.where(i == 0, me, far) * NB, NB)
        a2_piece(i).start()
        return carry
    lax.fori_loop(0, 2, a2_step, 0)
    sends.extend((a2_piece(0), a2_piece(1)))
    mark("b_2")

    def a2_arrived():
        for i in range(2):
            a2_piece(i).wait_recv()
    b_groups(a2_all, 4, a2_arrived)
    store_col_scale([acc_ref[:, col(j)] for j in range(COLS)], v_ref, q_ref)
    mark("sweeps")
    sweeps(SWEEPS - 1, kern, p_b, u_b, v_ref, q_ref, 16)

    mark("result")

    def result(i, carry):
        row = hint(i * 64, 64)
        for j, t in scaled_rows(kern, u_b, v_ref, hint(me * NB + row, 64), 64):
            out_ref[pl.ds(row, 64), col(j)] = t
        return carry
    lax.fori_loop(0, NB // 64, result, 0)
    for copy in sends:
        copy.wait_send()
    mark(None)


def solution(mesh):
    vmem = pl.BlockSpec(memory_space=pltpu.VMEM)
    hbm = pl.BlockSpec(memory_space=pl.ANY)
    smem = pl.BlockSpec(memory_space=pltpu.SMEM)

    def local_fgw(cost_src, cost_tgt, plan_init, mass_src, mass_tgt, feat_src, feat_tgt, epsilon):
        return pl.pallas_call(
            kernel,
            out_shape=pltpu.VMEM((NB, M), F32),
            in_specs=[hbm] * 7 + [smem],
            out_specs=vmem,
            scratch_shapes=[
                pltpu.VMEM((1, M), F32),
                pltpu.VMEM((NB, M), F32),
                pltpu.VMEM((N, M), BF16),
                pltpu.VMEM((2 * NB, N), BF16),
                pltpu.VMEM((NB, NB), BF16),
                pltpu.VMEM((2 * HALF, HALF), BF16),
                pltpu.VMEM((M, M), BF16),
                pltpu.VMEM((M, D), BF16),
                pltpu.VMEM((N, D), BF16),
                pltpu.VMEM((N, M), F32),
                pltpu.VMEM((N, M), BF16),
                pltpu.VMEM((N, M), BF16),
                pltpu.VMEM((N, M), F32),
                pltpu.VMEM((4, NB // LANES, LANES), F32),
                pltpu.VMEM((N, LANES), F32),
                pltpu.VMEM((N, LANES), F32),
                pltpu.VMEM((2 * CH, LANES), F32),
                pltpu.VMEM((2 * CH, LANES), F32),
                pltpu.VMEM((8, M), F32),
                pltpu.VMEM((8, M), F32),
                pltpu.SemaphoreType.DMA((8,)),
                pltpu.SemaphoreType.DMA((len(LINK.names),)),
                pltpu.SemaphoreType.DMA((len(LINK.names),)),
                pltpu.SemaphoreType.DMA((len(SIDE.names),)),
                pltpu.SemaphoreType.DMA((len(SIDE.names),)),
            ],
            compiler_params=pltpu.CompilerParams(
                collective_id=0, has_side_effects=True, vmem_limit_bytes=54000 * 1024),
        )(*(pltpu.with_memory_space_constraint(x, pltpu.HBM) for x in (
            cost_src, cost_tgt, plan_init, mass_src.reshape(NB // LANES, LANES), mass_tgt.reshape(1, M),
            feat_src, feat_tgt)), epsilon.reshape(1, 1))

    row_spec = P(('pairs', 'rows'), None)
    vec_spec = P(('pairs', 'rows'))
    in_specs = (row_spec, row_spec, row_spec, vec_spec, P('pairs'), row_spec, row_spec, P())
    return jax.shard_map(local_fgw, mesh=mesh, in_specs=in_specs, out_specs=row_spec, check_vma=False)
```

```python
import jax
import jax.numpy as jnp
from jax import lax
from jax.experimental import pallas as pl
from jax.experimental.pallas import tpu as pltpu
from jax.sharding import PartitionSpec as P

ALPHA = 0.5
OUTER_STEPS = 2
SWEEPS = 10
LOG2E = 1.4426950408889634

N = 2048
M = 1024
D = 256
NB = 512
MB = 256
F32 = jnp.float32
BF16 = jnp.bfloat16
LANES = 128
COLS = M // LANES

T_CHUNKS = 2
TR = NB // T_CHUNKS
CH = 256
HALF = NB // 2
FORM_GROUP = 32


class Slots:
    def __init__(self):
        self.names = {}

    def __call__(self, name):
        return self.names.setdefault(name, len(self.names))


LINK = Slots()
SIDE = Slots()
for k in range(T_CHUNKS):
    LINK(("t", k)), SIDE(("t", k)), SIDE(("far t", k))
for k in range(4):
    LINK(("c2", k)), SIDE(("far c2", k)), LINK(("c1 strip", k))
for k in range(4):
    SIDE(("a1", k))
for k in range(2):
    SIDE(("a2", k))
for k in range(2):
    LINK(("c1 quad", k)), SIDE(("c1 quad", k))
for k in range(2):
    LINK(("x", k)), SIDE(("far x", k))
for name in ("y", "p"):
    LINK(name), SIDE(name), SIDE("far " + name)
SIDE("c2"), SIDE("c1"), SIDE("x")


def hint(value, multiple):
    return value if isinstance(value, int) else pl.multiple_of(value, multiple)


def span(start, size):
    return pl.ds(hint(start, size), size)


def col(j):
    return slice(j * LANES, (j + 1) * LANES)


def tree(op, parts):
    while len(parts) > 1:
        parts = [op(parts[i], parts[i + 1]) for i in range(0, len(parts), 2)]
    return parts[0]


def store_col_scale(acc, v_ref, q_ref):
    for j in range(COLS):
        col_sum = jnp.sum(acc[j], axis=0, keepdims=True)
        v_ref[:, col(j)] = jnp.broadcast_to(q_ref[:, col(j)] / col_sum, (8, LANES))


def sweeps(count, kern, plan_b, u_b, v_ref, q_ref, group):
    lead = 128
    shape = (group // 8, 8, LANES)

    def sweep(_, carry):
        v = [v_ref[:, col(j)][None] for j in range(COLS)]

        def tile(row, j):
            return kern[row:row + group, col(j)].reshape(shape)

        acc = [jnp.zeros((8, LANES), F32) for _ in range(COLS)]
        for row in range(-lead, N, group):
            top = row + lead
            if top < N:
                total = tree(jnp.add, [tile(top, j) * v[j] for j in range(COLS)])
                u = plan_b[top:top + group, :].reshape(shape) / jnp.sum(total, axis=2, keepdims=True)
                u_b[top:top + group, :] = u.reshape(group, LANES)
            if row >= 0:
                u = u_b[row:row + group, :].reshape(shape)
                acc = [acc[j] + jnp.sum(tile(row, j) * u, axis=0) for j in range(COLS)]
        store_col_scale(acc, v_ref, q_ref)
        return carry

    lax.fori_loop(0, count, sweep, 0)


def scaled_rows(kern, u_b, v_ref, row, count):
    u = u_b[pl.ds(row, count), :].reshape(count // 8, 8, LANES)
    for j in range(COLS):
        k = kern[pl.ds(row, count), col(j)].reshape(count // 8, 8, LANES)
        yield j, (u * k * v_ref[:, col(j)][None]).reshape(count, LANES)


def kernel(c1_hbm, c2_hbm, t0_hbm, p_hbm, q_hbm, x_hbm, y_hbm, eps_ref, out_ref,
           q_ref, t_st, t_all, c1_rows, c1_side, quad_side, c2_all, y_all, x_all, g_all, a1_all, a2_all,
           kern, p_all, p_b, u_b, peak_b, first_b, acc_ref, v_ref,
           load_sem, link_send, link_recv, side_send, side_recv):
    raw0, raw1 = 0, CH
    me = lax.axis_index("rows")
    chip = me // 2
    core = me % 2
    partner = chip * 2 + (1 - core)
    far = (1 - chip) * 2 + core
    far_partner = (1 - chip) * 2 + (1 - core)

    y_st, x_st, c2_st = kern.at[:MB, :D], kern.at[MB:MB + NB, :D], kern.at[MB + NB:2 * MB + NB, :]
    loads = {}
    for i, (name, src, dst) in enumerate((
            ("y", y_hbm, y_st), ("p", p_hbm, p_all.at[me]), ("t", t0_hbm, t_st), ("c2", c2_hbm, c2_st), ("x", x_hbm, x_st),
            ("left", c1_hbm.at[:, :M], g_all.at[:NB]), ("right", c1_hbm.at[:, M:], g_all.at[NB:2 * NB]), ("q", q_hbm, q_ref))):
        loads[name] = pltpu.make_async_copy(src, dst, load_sem.at[i])
        loads[name].start()

    barrier = pltpu.get_barrier_semaphore()
    for peer in (partner, far):
        pl.semaphore_signal(barrier, inc=1, device_id={"rows": peer}, device_id_type=pl.DeviceIdType.MESH)
    pl.semaphore_wait(barrier, 2)

    def to_far(src, dst, name):
        slot = LINK.names[name]
        return pltpu.make_async_remote_copy(
            src_ref=src, dst_ref=dst, send_sem=link_send.at[slot], recv_sem=link_recv.at[slot],
            device_id={"rows": far}, device_id_type=pl.DeviceIdType.MESH)

    def to_partner(src, dst, name):
        slot = SIDE.names[name]
        return pltpu.make_async_remote_copy(
            src_ref=src, dst_ref=dst, send_sem=side_send.at[slot], recv_sem=side_recv.at[slot],
            device_id={"rows": partner}, device_id_type=pl.DeviceIdType.MESH)

    sends = []

    def go(copy):
        copy.start()
        sends.append(copy)

    def far_arrived(ref, name):
        to_far(ref, ref, name).wait_recv()

    def partner_arrived(ref, name):
        to_partner(ref, ref, name).wait_recv()

    def t_rows(owner, k):
        return t_all.at[span(owner * NB + k * TR, TR), :]

    def c2_rows(owner):
        return c2_all.at[span(owner * MB, MB), :]

    def c2_pieces(owner, other, which):
        return (
            c2_all.at[span(owner * MB + 128, 128), span(other * MB, 128)],
            c2_all.at[span(owner * MB + which * 128, 128), span(other * MB + which * 128, 128)],
            c2_all.at[span(owner * MB, 128), span(owner * MB, MB)],
            c2_all.at[span(owner * MB + 128, 128), span(owner * MB + 128, 128)])

    def y_rows(owner):
        return y_all.at[span(owner * MB, MB), :]

    def x_rows(owner):
        return x_all.at[span(owner * NB, NB), :]

    def x_half(owner, k):
        return x_all.at[span(owner * NB + k * CH, CH), :]

    def c1_quads(base, other, which):
        return (c1_rows.at[base + HALF:base + NB, span(other * NB, HALF)],
                c1_rows.at[span(base + which * HALF, HALF), span(other * NB + which * HALF, HALF)])

    def c1_strip(base, owner, k):
        return c1_rows.at[base + k * 128:base + (k + 1) * 128, pl.ds(hint(owner * NB + k * 128, 128), NB - k * 128)]

    loads["y"].wait()
    y_all[span(me * MB, MB), :] = kern[:MB, :D].astype(BF16)
    loads["p"].wait()
    go(to_far(p_all.at[me], p_all.at[me], "p"))
    go(to_partner(p_all.at[me], p_all.at[me], "p"))
    go(to_far(y_rows(me), y_rows(me), "y"))
    go(to_partner(y_rows(me), y_rows(me), "y"))
    loads["t"].wait()
    for k in range(T_CHUNKS):
        t_all[span(me * NB + k * TR, TR), :] = t_st[k * TR:(k + 1) * TR, :].astype(BF16)
    for k in range(T_CHUNKS):
        go(to_far(t_rows(me, k), t_rows(me, k), ("t", k)))
    for k in range(T_CHUNKS):
        go(to_partner(t_rows(me, k), t_rows(me, k), ("t", k)))
    for name in ("c2", "x", "left", "right", "q"):
        loads[name].wait()
    c2_all[span(me * MB, MB), :] = kern[MB + NB:2 * MB + NB, :].astype(BF16)
    x_all[span(me * NB, NB), :] = kern[MB:MB + NB, :D].astype(BF16)
    c1_rows[:NB, :M] = g_all[:NB, :].astype(BF16)
    c1_rows[:NB, M:] = g_all[NB:2 * NB, :].astype(BF16)
    for k, piece in enumerate(c2_pieces(me, partner, core)):
        go(to_far(piece, piece, ("c2", k)))
    for k, (src, dst) in enumerate(zip(c1_quads(0, partner, core), c1_quads(NB, partner, core))):
        go(to_far(src, dst, ("c1 quad", k)))
    for k in range(4):
        go(to_far(c1_strip(0, me, k), c1_strip(NB, me, k), ("c1 strip", k)))
    for k in range(2):
        go(to_far(x_half(me, k), x_half(me, k), ("x", k)))
    go(to_partner(c2_rows(me), c2_rows(me), "c2"))
    go(to_partner(x_rows(me), x_rows(me), "x"))
    go(to_partner(c1_rows.at[:NB, span(far_partner * NB, NB)], c1_side, "c1"))

    def mirror(src, src_row, src_col, dst, dst_row, dst_col, size):
        for i in range(size // LANES):
            for j in range(size // LANES):
                tile = src[span(src_row + i * LANES, LANES), span(src_col + j * LANES, LANES)]
                dst[span(dst_row + j * LANES, LANES), span(dst_col + i * LANES, LANES)] = (
                    tile.astype(F32).T.astype(BF16))

    mirror(c1_rows, 0, far * NB, c1_rows, NB, me * NB, NB)
    partner_arrived(c1_side, "c1")
    mirror(c1_side, 0, 0, c1_rows, NB, partner * NB, NB)
    partner_arrived(c2_rows(partner), "c2")
    mirror(c2_all, chip * 2 * MB, (1 - chip) * 2 * MB, c2_all, (1 - chip) * 2 * MB, chip * 2 * MB, 2 * MB)
    partner_arrived(y_rows(partner), "y")
    partner_arrived(p_all.at[partner], "p")
    partner_arrived(x_rows(partner), "x")

    def forward(ref, name):
        far_arrived(ref, name)
        go(to_partner(ref, ref, ("far " + name[0], name[1]) if isinstance(name, tuple) else "far " + name))

    def gram(owner):
        for n in range(4):
            g = lax.dot_general(x_all[span(owner * NB, NB), :], y_all[n * 256:(n + 1) * 256, :],
                                (((1,), (1,)), ((), ())), preferred_element_type=F32)
            g_all[span(owner * NB, NB), n * 256:(n + 1) * 256] = (2.0 * ALPHA) * g

    def grams(first, second):
        def one(i, carry):
            gram(first + i * (second - first))
            return carry
        lax.fori_loop(0, 2, one, 0)

    forward(y_rows(far), "y")
    forward(p_all.at[far], "p")
    partner_arrived(y_rows(far_partner), "far y")
    partner_arrived(p_all.at[far_partner], "far p")
    for owner in range(4):
        for i in range(NB // LANES):
            block = jnp.broadcast_to(p_all[owner, i:i + 1, :], (LANES, LANES))
            p_b[owner * NB + i * LANES:owner * NB + (i + 1) * LANES, :] = block.T
    grams(me, partner)
    for k in range(T_CHUNKS):
        partner_arrived(t_rows(partner, k), ("t", k))
    for k in range(T_CHUNKS):
        forward(t_rows(far, k), ("t", k))
    for k in range(T_CHUNKS):
        partner_arrived(t_rows(far_partner, k), ("far t", k))

    scale = LOG2E / eps_ref[0, 0]

    def a_rows(a_all, local, base, rows=CH):
        for n in range(4):
            a_all[span(base, rows), n * 256:(n + 1) * 256] = jnp.dot(
                c1_rows[span(local, rows), :], t_all[:, n * 256:(n + 1) * 256], preferred_element_type=F32).astype(BF16)

    def scores(a_all, base, raw):
        for n in range(4):
            b = jnp.dot(a_all[span(base, CH), :], c2_all[:, n * 256:(n + 1) * 256], preferred_element_type=F32)
            t_st[raw:raw + CH, n * 256:(n + 1) * 256] = g_all[span(base, CH), n * 256:(n + 1) * 256] + (2.0 * (1.0 - ALPHA)) * b

    def products(a_all, base):
        for n in range(4):
            b = jnp.dot(a_all[span(base, CH), :], c2_all[:, n * 256:(n + 1) * 256], preferred_element_type=F32)
            g_all[span(base, CH), n * 256:(n + 1) * 256] = (2.0 * (1.0 - ALPHA)) * b

    def late_scores(base, raw):
        for n in range(4):
            g = (2.0 * ALPHA) * lax.dot_general(x_all[span(base, CH), :], y_all[n * 256:(n + 1) * 256, :],
                                                (((1,), (1,)), ((), ())), preferred_element_type=F32)
            t_st[raw:raw + CH, n * 256:(n + 1) * 256] = g + g_all[span(base, CH), n * 256:(n + 1) * 256]
            g_all[span(base, CH), n * 256:(n + 1) * 256] = g

    def form(base, raw):
        acc = [acc_ref[:, col(j)] for j in range(COLS)]
        lead = 64
        group = FORM_GROUP
        shape = (group // 8, 8, LANES)
        for row in range(-2 * lead, CH, group):
            top = row + 2 * lead
            if top < CH:
                peak = tree(jnp.maximum, [t_st[raw + top:raw + top + group, col(j)] for j in range(COLS)])
                peak_b[raw + top:raw + top + group, :] = jnp.broadcast_to(jnp.max(peak, axis=1, keepdims=True), (group, LANES))
            mid = row + lead
            if 0 <= mid < CH:
                here = pl.ds(hint(base + mid, group), group)
                peak = peak_b[raw + mid:raw + mid + group, :]
                vals = [jnp.exp2((t_st[raw + mid:raw + mid + group, col(j)] - peak) * scale) for j in range(COLS)]
                for j in range(COLS):
                    kern[here, col(j)] = vals[j]
                    t_st[raw + mid:raw + mid + group, col(j)] = vals[j]
                total = jnp.sum(tree(jnp.add, vals), axis=1, keepdims=True)
                first_b[raw + mid:raw + mid + group, :] = p_b[here, :] / total
            if row >= 0:
                u = first_b[raw + row:raw + row + group, :].reshape(shape)
                acc = [acc[j] + jnp.sum(t_st[raw + row:raw + row + group, col(j)].reshape(shape) * u, axis=0)
                       for j in range(COLS)]
        for j in range(COLS):
            acc_ref[:, col(j)] = acc[j]

    def b_rows(a_all, bases, ready=None):
        raws = (raw0, raw1)
        for i, base in enumerate(bases):
            if ready and ready[i]:
                ready[i]()
            if i:
                form(bases[i - 1], raws[(i - 1) % 2])
            scores(a_all, base, raws[i % 2])
        form(bases[-1], raws[(len(bases) - 1) % 2])

    def a_slice(a_all, base):
        return a_all.at[span(base, CH), :]

    def my_base(i):
        return jnp.where(i < 2, me * NB + i * CH, far * NB + (i - 2) * CH)

    def their_base(i):
        return jnp.where(i < 2, partner * NB + i * CH, far_partner * NB + (i - 2) * CH)

    mine = [my_base(i) for i in range(4)]
    theirs = [their_base(i) for i in range(4)]

    def share(a_all, name, start, stop):
        slot = SIDE.names[(name, 0)]

        def piece(i):
            ref = a_slice(a_all, my_base(i))
            return pltpu.make_async_remote_copy(
                src_ref=ref, dst_ref=ref, send_sem=side_send.at[slot + i], recv_sem=side_recv.at[slot + i],
                device_id={"rows": partner}, device_id_type=pl.DeviceIdType.MESH)

        def step(i, carry):
            a_rows(a_all, i * CH, my_base(i))
            piece(i).start()
            return carry
        if stop - start == 1:
            step(start, 0)
        else:
            lax.fori_loop(start, stop, step, 0)
        for i in range(start, stop):
            sends.append(piece(i))

    def b_groups(a_all, count, arrived):
        def group(g, carry):
            @pl.when(g == 1)
            def _():
                arrived()
            b_rows(a_all, [jnp.where(g == 0, mine[i], theirs[i]) for i in range(count)])
            return carry
        lax.fori_loop(0, 2, group, 0)

    acc_ref[...] = jnp.zeros_like(acc_ref)
    share(a1_all, "a1", 0, 2)
    for k, piece in enumerate(c2_pieces(far, far_partner, core)):
        forward(piece, ("c2", k))
    for k, piece in enumerate(c2_pieces(far_partner, far, 1 - core)):
        partner_arrived(piece, ("far c2", k))
    first = (1 - chip) * 2 * MB
    second = first + MB
    for base in (first, second):
        mirror(c2_all, base, base + 128, c2_all, base + 128, base, 128)
    mirror(c2_all, second + 128, first, c2_all, first, second + 128, 128)
    mirror(c2_all, second + 128, first + 128, c2_all, first + 128, second + 128, 128)
    mirror(c2_all, first, second, c2_all, second, first, 128)
    mirror(c2_all, first + 128, second, c2_all, second, first + 128, 128)

    def a1_arrived():
        for i in range(2):
            partner_arrived(a_slice(a1_all, theirs[i]), ("a1", i))
    b_groups(a1_all, 2, a1_arrived)
    for k, piece in enumerate(c1_quads(NB, far_partner, core)):
        far_arrived(piece, ("c1 quad", k))
        go(to_partner(piece, quad_side.at[k * HALF:(k + 1) * HALF, :], ("c1 quad", k)))
    for k in range(2):
        partner_arrived(quad_side.at[k * HALF:(k + 1) * HALF, :], ("c1 quad", k))
    mirror(quad_side, 0, 0, c1_rows, NB, far_partner * NB + HALF, HALF)
    mirror(quad_side, HALF, 0, c1_rows, NB + (1 - core) * HALF, far_partner * NB + (1 - core) * HALF, HALF)

    def a_early(i, carry):
        rows = span(NB + i * CH, CH)
        for n in range(4):
            cols = slice(n * 256, (n + 1) * 256)
            kern[span(far * NB + i * CH, CH), cols] = (
                jnp.dot(c1_rows[rows, span(chip * 2 * NB, 2 * NB)], t_all[span(chip * 2 * NB, 2 * NB), cols],
                        preferred_element_type=F32)
                + jnp.dot(c1_rows[rows, span(far_partner * NB, NB)], t_all[span(far_partner * NB, NB), cols],
                          preferred_element_type=F32))
        return carry
    lax.fori_loop(0, 2, a_early, 0)

    def a_late(i):
        base = mine[2 + i]
        for n in range(4):
            cols = slice(n * 256, (n + 1) * 256)
            a1_all[span(base, CH), cols] = (
                kern[span(base, CH), cols]
                + jnp.dot(c1_rows[NB + i * CH:NB + (i + 1) * CH, span(far * NB, NB)], t_all[span(far * NB, NB), cols],
                          preferred_element_type=F32)).astype(BF16)
        go(to_partner(a_slice(a1_all, base), a_slice(a1_all, base), ("a1", 2 + i)))

    for i in range(2):
        for k in (2 * i, 2 * i + 1):
            far_arrived(c1_strip(NB, far, k), ("c1 strip", k))
            for below in range(k + 1, 4):
                mirror(c1_rows, NB + k * 128, far * NB + below * 128, c1_rows, NB + below * 128, far * NB + k * 128, 128)
        a_late(i)
        products(a1_all, mine[2 + i])
    for i in range(2):
        partner_arrived(a_slice(a1_all, theirs[2 + i]), ("a1", 2 + i))
        products(a1_all, theirs[2 + i])
    for half in range(2):
        forward(x_half(far, half), ("x", half))
        late_scores(mine[2 + half], raw0)
        form(mine[2 + half], raw0)
        partner_arrived(x_half(far_partner, half), ("far x", half))
        late_scores(theirs[2 + half], raw1)
        form(theirs[2 + half], raw1)
    store_col_scale([acc_ref[:, col(j)] for j in range(COLS)], v_ref, q_ref)
    sweeps(SWEEPS - 1, kern, p_b, u_b, v_ref, q_ref, 32)

    for copy in sends:
        copy.wait_send()
    sends.clear()

    def next_plan(i, carry):
        row = hint(i * 128, 128)
        for j, t in scaled_rows(kern, u_b, v_ref, row, 128):
            t_all[pl.ds(row, 128), col(j)] = t.astype(BF16)
        return carry
    lax.fori_loop(0, N // 128, next_plan, 0)

    acc_ref[...] = jnp.zeros_like(acc_ref)
    first_slot = SIDE.names[("a2", 0)]

    def a2_piece(i):
        ref = a2_all.at[span(jnp.where(i == 0, me, far) * NB, NB), :]
        return pltpu.make_async_remote_copy(
            src_ref=ref, dst_ref=ref, send_sem=side_send.at[first_slot + i], recv_sem=side_recv.at[first_slot + i],
            device_id={"rows": partner}, device_id_type=pl.DeviceIdType.MESH)

    def a2_step(i, carry):
        a_rows(a2_all, i * NB, jnp.where(i == 0, me, far) * NB, NB)
        a2_piece(i).start()
        return carry
    lax.fori_loop(0, 2, a2_step, 0)
    sends.extend((a2_piece(0), a2_piece(1)))

    def a2_arrived():
        for i in range(2):
            a2_piece(i).wait_recv()
    b_groups(a2_all, 4, a2_arrived)
    store_col_scale([acc_ref[:, col(j)] for j in range(COLS)], v_ref, q_ref)
    sweeps(SWEEPS - 1, kern, p_b, u_b, v_ref, q_ref, 16)


    def result(i, carry):
        row = hint(i * 64, 64)
        for j, t in scaled_rows(kern, u_b, v_ref, hint(me * NB + row, 64), 64):
            out_ref[pl.ds(row, 64), col(j)] = t
        return carry
    lax.fori_loop(0, NB // 64, result, 0)
    for copy in sends:
        copy.wait_send()


def solution(mesh):
    vmem = pl.BlockSpec(memory_space=pltpu.VMEM)
    hbm = pl.BlockSpec(memory_space=pl.ANY)
    smem = pl.BlockSpec(memory_space=pltpu.SMEM)

    def local_fgw(cost_src, cost_tgt, plan_init, mass_src, mass_tgt, feat_src, feat_tgt, epsilon):
        return pl.pallas_call(
            kernel,
            out_shape=pltpu.VMEM((NB, M), F32),
            in_specs=[hbm] * 7 + [smem],
            out_specs=vmem,
            scratch_shapes=[
                pltpu.VMEM((1, M), F32),
                pltpu.VMEM((NB, M), F32),
                pltpu.VMEM((N, M), BF16),
                pltpu.VMEM((2 * NB, N), BF16),
                pltpu.VMEM((NB, NB), BF16),
                pltpu.VMEM((2 * HALF, HALF), BF16),
                pltpu.VMEM((M, M), BF16),
                pltpu.VMEM((M, D), BF16),
                pltpu.VMEM((N, D), BF16),
                pltpu.VMEM((N, M), F32),
                pltpu.VMEM((N, M), BF16),
                pltpu.VMEM((N, M), BF16),
                pltpu.VMEM((N, M), F32),
                pltpu.VMEM((4, NB // LANES, LANES), F32),
                pltpu.VMEM((N, LANES), F32),
                pltpu.VMEM((N, LANES), F32),
                pltpu.VMEM((2 * CH, LANES), F32),
                pltpu.VMEM((2 * CH, LANES), F32),
                pltpu.VMEM((8, M), F32),
                pltpu.VMEM((8, M), F32),
                pltpu.SemaphoreType.DMA((8,)),
                pltpu.SemaphoreType.DMA((len(LINK.names),)),
                pltpu.SemaphoreType.DMA((len(LINK.names),)),
                pltpu.SemaphoreType.DMA((len(SIDE.names),)),
                pltpu.SemaphoreType.DMA((len(SIDE.names),)),
            ],
            compiler_params=pltpu.CompilerParams(
                collective_id=0, has_side_effects=True, vmem_limit_bytes=54000 * 1024),
        )(*(pltpu.with_memory_space_constraint(x, pltpu.HBM) for x in (
            cost_src, cost_tgt, plan_init, mass_src.reshape(NB // LANES, LANES), mass_tgt.reshape(1, M),
            feat_src, feat_tgt)), epsilon.reshape(1, 1))

    row_spec = P(('pairs', 'rows'), None)
    vec_spec = P(('pairs', 'rows'))
    in_specs = (row_spec, row_spec, row_spec, vec_spec, P('pairs'), row_spec, row_spec, P())
    return jax.shard_map(local_fgw, mesh=mesh, in_specs=in_specs, out_specs=row_spec, check_vma=False)
```
